8 devices in a mesh: dp: 2 (over z, y), sp: 4 (over x, core).
Axes of the slice: x: 2, y: 2, z: 1, core: 2. Of those that a mesh axis runs over, the one named last changes fastest.
Arguments:
- hidden: bfloat16 [2, 4096, 1024], P('dp', 'sp')
- positions: int32 [2, 4096], P('dp', 'sp')
- grad_out: bfloat16 [2, 4096, 1024], P('dp', 'sp')
- gain_attn: bfloat16 [1024], P(('dp', 'sp'))
- gain_mlp: bfloat16 [1024], P(('dp', 'sp'))
- w_query: bfloat16 [1024, 2048], P(('dp', 'sp'))
- w_key: bfloat16 [1024, 1024], P(('dp', 'sp'))
- w_value: bfloat16 [1024, 1024], P(('dp', 'sp'))
- w_out: bfloat16 [2048, 1024], P(('dp', 'sp'))
- w_gate: bfloat16 [1024, 3072], P(('dp', 'sp'))
- w_up: bfloat16 [1024, 3072], P(('dp', 'sp'))
- w_down: bfloat16 [3072, 1024], P(('dp', 'sp'))
Outputs:
- output 1: bfloat16 [2, 4096, 1024], P('dp', 'sp')
- output 2: bfloat16 [2, 4096, 1024], P('dp', 'sp')
- output 3: float32 [1024], P(('dp', 'sp'))
- output 4: float32 [1024], P(('dp', 'sp'))
- output 5: float32 [1024, 2048], P(('dp', 'sp'))
- output 6: float32 [1024, 1024], P(('dp', 'sp'))
- output 7: float32 [1024, 1024], P(('dp', 'sp'))
- output 8: float32 [2048, 1024], P(('dp', 'sp'))
- output 9: float32 [1024, 3072], P(('dp', 'sp'))
- output 10: float32 [1024, 3072], P(('dp', 'sp'))
- output 11: float32 [3072, 1024], P(('dp', 'sp'))
All inputs are finite; a program needn't handle non-finite values.
Results may differ from the reference program's by a relative error of at most 0.0154287.
Values are sent between devices in bfloat16 or wider.
A program may use at most 1 GiB of HBM per device.

```python
import math
import jax
import jax.numpy as jnp
from jax import lax

BATCH = 2
SEQ = 4096
DIM = 1024
HEADS = 16
KV_HEADS = 8
FFN = 3072
HEAD_DIM = 128
ROPE_BASE = 10000.0
NORM_EPS = 1e-5
Q_PER_KV = HEADS // KV_HEADS


def setup_inputs(seed: int = 0) -> dict:
    rand_keys = jax.random.split(jax.random.key(seed), 13)
    qk_boost = (0.65 * math.log(SEQ)) ** 0.25

    def draw_normal(key_idx, arr_shape, spread):
        return (jax.random.normal(rand_keys[key_idx], arr_shape, jnp.float32) * spread).astype(jnp.bfloat16)

    def draw_gain(key_idx):
        return (1.0 + 0.3 * jax.random.normal(rand_keys[key_idx], (DIM,), jnp.float32)).astype(jnp.bfloat16)

    steps_up = jax.random.randint(rand_keys[1], (BATCH, SEQ), 1, 4)
    start_pos = jax.random.randint(rand_keys[2], (BATCH, 1), 0, SEQ)
    return {
        'hidden': draw_normal(0, (BATCH, SEQ, DIM), 1.0),
        'positions': (start_pos + jnp.cumsum(steps_up, axis=1)).astype(jnp.int32),
        'grad_out': draw_normal(3, (BATCH, SEQ, DIM), 1.0),
        'gain_attn': draw_gain(4),
        'gain_mlp': draw_gain(5),
        'w_query': draw_normal(6, (DIM, HEADS * HEAD_DIM), qk_boost / math.sqrt(DIM)),
        'w_key': draw_normal(7, (DIM, KV_HEADS * HEAD_DIM), qk_boost / math.sqrt(DIM)),
        'w_value': draw_normal(8, (DIM, KV_HEADS * HEAD_DIM), 1.0 / math.sqrt(DIM)),
        'w_out': draw_normal(9, (HEADS * HEAD_DIM, DIM), 1.0 / math.sqrt(HEADS * HEAD_DIM)),
        'w_gate': draw_normal(10, (DIM, FFN), 1.0 / math.sqrt(DIM)),
        'w_up': draw_normal(11, (DIM, FFN), 1.0 / math.sqrt(DIM)),
        'w_down': draw_normal(12, (FFN, DIM), 1.0 / math.sqrt(FFN)),
    }


def rope_tables(pos_ids):
    inv_freq = ROPE_BASE ** (-(jnp.arange(HEAD_DIM // 2, dtype=jnp.float32) * (2.0 / HEAD_DIM)))
    angles = pos_ids.astype(jnp.float32)[..., None] * inv_freq
    return jnp.cos(angles), jnp.sin(angles)


def apply_rope(values, cos_tab, sin_tab):
    half_dim = values.shape[-1] // 2
    low_half = values[..., :half_dim]
    high_half = values[..., half_dim:]
    cos_wide = cos_tab[..., None, :]
    sin_wide = sin_tab[..., None, :]
    return jnp.concatenate([low_half * cos_wide - high_half * sin_wide, high_half * cos_wide + low_half * sin_wide], axis=-1)


def rope_grad(grads_in, cos_tab, sin_tab):
    half_dim = grads_in.shape[-1] // 2
    low_half = grads_in[..., :half_dim]
    high_half = grads_in[..., half_dim:]
    cos_wide = cos_tab[..., None, :]
    sin_wide = sin_tab[..., None, :]
    return jnp.concatenate([low_half * cos_wide + high_half * sin_wide, high_half * cos_wide - low_half * sin_wide], axis=-1)


def rms_norm(values, gain_vec):
    vals32 = values.astype(jnp.float32)
    inv_rms = lax.rsqrt(jnp.mean(vals32 * vals32, axis=-1, keepdims=True) + NORM_EPS)
    normed = vals32 * inv_rms
    return (normed * gain_vec.astype(jnp.float32)).astype(jnp.bfloat16), normed, inv_rms


def rms_norm_grad(d_out, normed, inv_rms, gain_vec):
    d_normed = d_out * gain_vec.astype(jnp.float32)
    grad_gain = jnp.sum(d_out * normed, axis=0)
    grad_in = inv_rms * (d_normed - normed * jnp.mean(d_normed * normed, axis=-1, keepdims=True))
    return grad_in, grad_gain


def head_probs(q_one, k_one):
    scores = jnp.einsum('qgd,kd->gqk', q_one.astype(jnp.float32), k_one.astype(jnp.float32)) * (HEAD_DIM ** -0.5)
    causal = jnp.arange(SEQ)[:, None] >= jnp.arange(SEQ)[None, :]
    scores = jnp.where(causal, scores, -jnp.inf)
    row_max = jnp.max(scores, axis=-1, keepdims=True)
    exp_scores = jnp.exp(scores - row_max)
    return exp_scores / jnp.sum(exp_scores, axis=-1, keepdims=True)


def attention_forward(q_heads, k_heads, v_heads):
    q_major = q_heads.reshape(SEQ, KV_HEADS, Q_PER_KV, HEAD_DIM).transpose(1, 0, 2, 3)

    def one_head(operands):
        q_one, k_one, v_one = operands
        probs_bf = head_probs(q_one, k_one).astype(jnp.bfloat16)
        return jnp.einsum('gqk,kd->qgd', probs_bf.astype(jnp.float32), v_one.astype(jnp.float32))

    per_head = lax.map(one_head, (q_major, k_heads.transpose(1, 0, 2), v_heads.transpose(1, 0, 2)))
    return per_head.transpose(1, 0, 2, 3).astype(jnp.bfloat16).reshape(SEQ, HEADS * HEAD_DIM)


def attention_backward(q_heads, k_heads, v_heads, d_heads):
    q_major = q_heads.reshape(SEQ, KV_HEADS, Q_PER_KV, HEAD_DIM).transpose(1, 0, 2, 3)
    d_major = d_heads.reshape(SEQ, KV_HEADS, Q_PER_KV, HEAD_DIM).transpose(1, 0, 2, 3)

    def one_head(operands):
        q_one, k_one, v_one, d_one = operands
        attn_probs = head_probs(q_one, k_one)
        probs32 = attn_probs.astype(jnp.bfloat16).astype(jnp.float32)
        d_f32 = d_one.astype(jnp.float32)
        d_probs = jnp.einsum('qgd,kd->gqk', d_f32, v_one.astype(jnp.float32))
        grad_v = jnp.einsum('gqk,qgd->kd', probs32, d_f32)
        row_dot = jnp.sum(attn_probs * d_probs, axis=-1, keepdims=True)
        d_scores = (attn_probs * (d_probs - row_dot) * (HEAD_DIM ** -0.5)).astype(jnp.bfloat16).astype(jnp.float32)
        grad_q = jnp.einsum('gqk,kd->qgd', d_scores, k_one.astype(jnp.float32))
        grad_k = jnp.einsum('gqk,qgd->kd', d_scores, q_one.astype(jnp.float32))
        return grad_q.astype(jnp.bfloat16), grad_k.astype(jnp.bfloat16), grad_v.astype(jnp.bfloat16)

    grad_q, grad_k, grad_v = lax.map(one_head, (q_major, k_heads.transpose(1, 0, 2), v_heads.transpose(1, 0, 2), d_major))
    return grad_q.transpose(1, 0, 2, 3).reshape(SEQ, HEADS, HEAD_DIM), grad_k.transpose(1, 0, 2), grad_v.transpose(1, 0, 2)


def sequence_step(tokens, pos_ids, d_layer, gain_attn, gain_mlp, w_query, w_key, w_value, w_out, w_gate, w_up, w_down):
    cos_tab, sin_tab = rope_tables(pos_ids)
    u_attn, normed1, inv_rms1 = rms_norm(tokens, gain_attn)
    q_heads = apply_rope(jnp.dot(u_attn, w_query, preferred_element_type=jnp.float32).reshape(SEQ, HEADS, HEAD_DIM), cos_tab, sin_tab).astype(jnp.bfloat16)
    k_heads = apply_rope(jnp.dot(u_attn, w_key, preferred_element_type=jnp.float32).reshape(SEQ, KV_HEADS, HEAD_DIM), cos_tab, sin_tab).astype(jnp.bfloat16)
    v_heads = jnp.dot(u_attn, w_value, preferred_element_type=jnp.float32).astype(jnp.bfloat16).reshape(SEQ, KV_HEADS, HEAD_DIM)
    attn_out = attention_forward(q_heads, k_heads, v_heads)
    residual = (tokens.astype(jnp.float32) + jnp.dot(attn_out, w_out, preferred_element_type=jnp.float32)).astype(jnp.bfloat16)
    u_mlp, normed2, inv_rms2 = rms_norm(residual, gain_mlp)
    gate_pre = jnp.dot(u_mlp, w_gate, preferred_element_type=jnp.float32)
    up_pre = jnp.dot(u_mlp, w_up, preferred_element_type=jnp.float32)
    sig_gate = jax.nn.sigmoid(gate_pre)
    silu_gate = gate_pre * sig_gate
    mlp_act = (silu_gate * up_pre).astype(jnp.bfloat16)
    layer_out = (residual.astype(jnp.float32) + jnp.dot(mlp_act, w_down, preferred_element_type=jnp.float32)).astype(jnp.bfloat16)

    grad_w_down = jnp.dot(mlp_act.T, d_layer, preferred_element_type=jnp.float32)
    d_act = jnp.dot(d_layer, w_down.T, preferred_element_type=jnp.float32)
    d_gate = (d_act * up_pre * sig_gate * (1.0 + gate_pre * (1.0 - sig_gate))).astype(jnp.bfloat16)
    d_up = (d_act * silu_gate).astype(jnp.bfloat16)
    grad_w_gate = jnp.dot(u_mlp.T, d_gate, preferred_element_type=jnp.float32)
    grad_w_up = jnp.dot(u_mlp.T, d_up, preferred_element_type=jnp.float32)
    d_umlp = jnp.dot(d_gate, w_gate.T, preferred_element_type=jnp.float32) + jnp.dot(d_up, w_up.T, preferred_element_type=jnp.float32)
    d_res_norm, grad_gain_mlp = rms_norm_grad(d_umlp, normed2, inv_rms2, gain_mlp)
    d_resid = d_layer.astype(jnp.float32) + d_res_norm
    d_resid_bf = d_resid.astype(jnp.bfloat16)
    grad_w_out = jnp.dot(attn_out.T, d_resid_bf, preferred_element_type=jnp.float32)
    d_attn = jnp.dot(d_resid_bf, w_out.T, preferred_element_type=jnp.float32).astype(jnp.bfloat16).reshape(SEQ, HEADS, HEAD_DIM)
    grad_q, grad_k, grad_v = attention_backward(q_heads, k_heads, v_heads, d_attn)
    dq_pre = rope_grad(grad_q.astype(jnp.float32), cos_tab, sin_tab).astype(jnp.bfloat16).reshape(SEQ, HEADS * HEAD_DIM)
    dk_pre = rope_grad(grad_k.astype(jnp.float32), cos_tab, sin_tab).astype(jnp.bfloat16).reshape(SEQ, KV_HEADS * HEAD_DIM)
    dv_flat = grad_v.reshape(SEQ, KV_HEADS * HEAD_DIM)
    grad_w_query = jnp.dot(u_attn.T, dq_pre, preferred_element_type=jnp.float32)
    grad_w_key = jnp.dot(u_attn.T, dk_pre, preferred_element_type=jnp.float32)
    grad_w_value = jnp.dot(u_attn.T, dv_flat, preferred_element_type=jnp.float32)
    d_uattn = (jnp.dot(dq_pre, w_query.T, preferred_element_type=jnp.float32)
               + jnp.dot(dk_pre, w_key.T, preferred_element_type=jnp.float32)
               + jnp.dot(dv_flat, w_value.T, preferred_element_type=jnp.float32))
    d_tok_norm, grad_gain_attn = rms_norm_grad(d_uattn, normed1, inv_rms1, gain_attn)
    grad_hidden = (d_resid + d_tok_norm).astype(jnp.bfloat16)
    seq_grads = (grad_gain_attn, grad_gain_mlp, grad_w_query, grad_w_key, grad_w_value, grad_w_out, grad_w_gate, grad_w_up, grad_w_down)
    return layer_out, grad_hidden, seq_grads


def reference(hidden, positions, grad_out, gain_attn, gain_mlp, w_query, w_key, w_value, w_out, w_gate, w_up, w_down):
    weights = (gain_attn, gain_mlp, w_query, w_key, w_value, w_out, w_gate, w_up, w_down)
    zero_grads = tuple(jnp.zeros(weight.shape, jnp.float32) for weight in weights)

    def scan_body(grad_sums, seq_in):
        tokens, pos_ids, d_layer = seq_in
        layer_out, grad_hidden, seq_grads = sequence_step(tokens, pos_ids, d_layer, *weights)
        new_sums = tuple(acc_sum + seq_grad for acc_sum, seq_grad in zip(grad_sums, seq_grads))
        return new_sums, (layer_out, grad_hidden)

    grad_sums, outs_pair = lax.scan(scan_body, zero_grads, (hidden, positions, grad_out))
    return (outs_pair[0], outs_pair[1], grad_sums[0], grad_sums[1], grad_sums[2], grad_sums[3], grad_sums[4], grad_sums[5], grad_sums[6], grad_sums[7], grad_sums[8])
```

```python
import functools
import math

import jax
import jax.numpy as jnp
from jax import lax
from jax.experimental import pallas as pl
from jax.experimental.pallas import tpu as pltpu
from jax.sharding import PartitionSpec as P

HEAD_DIM = 128
ROPE_BASE = 10000.0
NORM_EPS = 1e-5
ATTN_SCALE = HEAD_DIM ** -0.5
LOG2E = math.log2(math.e)
SCALE2 = ATTN_SCALE * LOG2E
ALL_AXES = ('dp', 'sp')
BLK = 512
SEQ = 4096
TOK = 1024
DIM = 1024
NEG = -1e30
VMEM_LIMIT = 60 * 1024 * 1024


def dot_nt(left, right):
    return lax.dot_general(left, right, (((1,), (1,)), ((), ())), preferred_element_type=jnp.float32)


def dot_nn(left, right):
    return lax.dot_general(left, right, (((1,), (0,)), ((), ())), preferred_element_type=jnp.float32)


def dot_tn(left, right):
    return lax.dot_general(left, right, (((0,), (0,)), ((), ())), preferred_element_type=jnp.float32)


def qkv_kernel(x_ref, g_ref, w_ref, cos_ref, sin_ref, u_ref, q0_ref, k0_ref, v0_ref, q1_ref, k1_ref, v1_ref):
    x32 = x_ref[...].astype(jnp.float32)
    inv_rms = lax.rsqrt(jnp.mean(x32 * x32, axis=-1, keepdims=True) + NORM_EPS)
    u = (x32 * inv_rms * g_ref[...].astype(jnp.float32)).astype(jnp.bfloat16)
    u_ref[...] = u
    cos, sin = cos_ref[...], sin_ref[...]

    def rope(t):
        return (t * cos + pltpu.roll(t, 64, 1) * sin).astype(jnp.bfloat16)

    for g, (q_ref, k_ref, v_ref) in enumerate(((q0_ref, k0_ref, v0_ref), (q1_ref, k1_ref, v1_ref))):
        y = dot_nn(u, w_ref[:, g * 512:(g + 1) * 512])
        q_ref[:, 0:128] = rope(y[:, 0:128])
        q_ref[:, 128:256] = rope(y[:, 128:256])
        k_ref[...] = rope(y[:, 256:384])
        v_ref[...] = y[:, 384:512].astype(jnp.bfloat16)


def qkv_call(x_all, gain, w_own, cos, sin):
    row = lambda width: pl.BlockSpec((BLK, width), lambda i: (i, 0))
    fixed = lambda shape: pl.BlockSpec(shape, lambda i: (0, 0))
    out = lambda width: jax.ShapeDtypeStruct((SEQ, width), jnp.bfloat16)
    return pl.pallas_call(
        qkv_kernel,
        grid=(SEQ // BLK,),
        in_specs=[row(DIM), fixed((1, DIM)), fixed((DIM, 1024)), row(128), row(128)],
        out_specs=[row(DIM), row(256), row(128), row(128), row(256), row(128), row(128)],
        out_shape=[out(DIM), out(256), out(128), out(128), out(256), out(128), out(128)],
        compiler_params=pltpu.CompilerParams(vmem_limit_bytes=VMEM_LIMIT, dimension_semantics=('arbitrary',)),
        cost_estimate=pl.CostEstimate(flops=2 * SEQ * DIM * 1024, bytes_accessed=40 << 20, transcendentals=0),
        name='qkv',
    )(x_all, gain, w_own, cos, sin)


def fwd_kernel(q_ref, k_ref, v_ref, o_ref, lse_ref, acc_ref):
    i = pl.program_id(0)
    qs = [q_ref[:, h * 128:(h + 1) * 128] for h in range(2)]

    def step(j, carry, masked):
        start = pl.multiple_of(j * BLK, BLK)
        k = k_ref[pl.ds(start, BLK), :]
        v = v_ref[pl.ds(start, BLK), :]
        out = []
        for h in range(2):
            m, l = carry[h]
            s = dot_nt(qs[h], k)
            if masked:
                rows = lax.broadcasted_iota(jnp.int32, (BLK, BLK), 0)
                cols = lax.broadcasted_iota(jnp.int32, (BLK, BLK), 1)
                s = jnp.where(rows >= cols, s, NEG)
            m_new = jnp.maximum(m, jnp.max(s, axis=1, keepdims=True))
            p = jnp.exp2(s * SCALE2 - m_new * SCALE2)
            alpha = jnp.exp2((m - m_new) * SCALE2)
            l_new = alpha * l + ((p[:, 0:128] + p[:, 128:256]) + (p[:, 256:384] + p[:, 384:512]))
            pv = dot_nn(p.astype(jnp.bfloat16), v)
            acc_ref[h] = acc_ref[h] * alpha + pv
            out.append((m_new, l_new))
        return tuple(out)

    acc_ref[...] = jnp.zeros_like(acc_ref)
    init = tuple((jnp.full((BLK, 1), NEG, jnp.float32), jnp.zeros((BLK, 128), jnp.float32)) for _ in range(2))
    carry = lax.fori_loop(0, i, lambda j, c: step(j, c, False), init)
    carry = step(i, carry, True)
    for h in range(2):
        m, l = carry[h]
        total = jnp.sum(l, axis=1, keepdims=True)
        o_ref[0, :, h * 128:(h + 1) * 128] = (acc_ref[h] / total).astype(jnp.bfloat16)
        lse = jnp.broadcast_to(m * SCALE2 + jnp.log2(total), (BLK, 128))
        lse_ref[h] = lse.T[0:8, :]


def fwd_call(q, k, v):
    fixed = pl.BlockSpec((SEQ, 128), lambda i: (0, 0))
    per = TOK // BLK
    return pl.pallas_call(
        fwd_kernel,
        grid=(SEQ // BLK,),
        in_specs=[pl.BlockSpec((BLK, 256), lambda i: (i, 0)), fixed, fixed],
        out_specs=[pl.BlockSpec((1, BLK, 256), lambda i: (i // per, i % per, 0)), pl.BlockSpec((2, 8, BLK), lambda i: (0, 0, i))],
        out_shape=[jax.ShapeDtypeStruct((SEQ // TOK, TOK, 256), jnp.bfloat16), jax.ShapeDtypeStruct((2, 8, SEQ), jnp.float32)],
        scratch_shapes=[pltpu.VMEM((2, BLK, 128), jnp.float32)],
        compiler_params=pltpu.CompilerParams(vmem_limit_bytes=VMEM_LIMIT, dimension_semantics=('arbitrary',)),
        cost_estimate=pl.CostEstimate(flops=30 * 10 ** 9, bytes_accessed=8 << 20, transcendentals=1 << 24),
        name='attn_fwd',
    )(q, k, v)


def bwd_kernel(q_ref, k_ref, v_ref, o_ref, do_ref, lse_ref, cos_ref, sin_ref, out_ref, dq_acc, dk_acc, dv_acc, delta):
    j = pl.program_id(0)
    n_blk = SEQ // BLK

    @pl.when(j == 0)
    def _():
        dq_acc[...] = jnp.zeros_like(dq_acc)

        def rows(i, _):
            start = pl.multiple_of(i * BLK, BLK)
            prod = o_ref[pl.ds(start, BLK), :].astype(jnp.float32) * do_ref[pl.ds(start, BLK), :].astype(jnp.float32)
            for h in range(2):
                tot = jnp.sum(prod[:, h * 128:(h + 1) * 128], axis=1, keepdims=True)
                delta[h, :, pl.ds(start, BLK)] = jnp.broadcast_to(tot, (BLK, 128)).T[0:8, :]
            return 0

        lax.fori_loop(0, n_blk, rows, 0)

    k = k_ref[...]
    v = v_ref[...]
    dk_acc[...] = jnp.zeros_like(dk_acc)
    dv_acc[...] = jnp.zeros_like(dv_acc)

    def step(i, masked):
        start = pl.multiple_of(i * BLK, BLK)
        rows = pl.ds(start, BLK)
        for h in range(2):
            cols = slice(h * 128, (h + 1) * 128)
            q = q_ref[rows, cols]
            do = do_ref[rows, cols]
            s = dot_nt(k, q)
            p = jnp.exp2(s * SCALE2 - lse_ref[h, 0:1, rows])
            if masked:
                kv_idx = lax.broadcasted_iota(jnp.int32, (BLK, BLK), 0)
                q_idx = lax.broadcasted_iota(jnp.int32, (BLK, BLK), 1)
                p = jnp.where(q_idx >= kv_idx, p, 0.0)
            dp = dot_nt(v, do)
            dv_acc[...] += dot_nn(p.astype(jnp.bfloat16), do)
            ds = (p * (dp - delta[h, 0:1, rows]) * ATTN_SCALE).astype(jnp.bfloat16)
            dk_acc[...] += dot_nn(ds, q)
            dq_acc[rows, cols] += dot_tn(ds, k)

    step(j, True)

    def body(i, _):
        step(i, False)
        return 0

    lax.fori_loop(j + 1, n_blk, body, 0)

    cos, sin = cos_ref[...], sin_ref[...]

    def rope_back(t):
        t = t.astype(jnp.bfloat16).astype(jnp.float32)
        return (t * cos - pltpu.roll(t, 64, 1) * sin).astype(jnp.bfloat16)

    mine = pl.ds(pl.multiple_of(j * BLK, BLK), BLK)
    for h in range(2):
        out_ref[0, :, h * 128:(h + 1) * 128] = rope_back(dq_acc[mine, h * 128:(h + 1) * 128])
    out_ref[0, :, 256:384] = rope_back(dk_acc[...])
    out_ref[0, :, 384:512] = dv_acc[...].astype(jnp.bfloat16)


def bwd_call(q, k, v, o, do, lse, cos, sin):
    whole = lambda width: pl.BlockSpec((SEQ, width), lambda j: (0, 0))
    block = pl.BlockSpec((BLK, 128), lambda j: (j, 0))
    per = TOK // BLK
    return pl.pallas_call(
        bwd_kernel,
        grid=(SEQ // BLK,),
        in_specs=[whole(256), block, block, whole(256), whole(256), pl.BlockSpec((2, 8, SEQ), lambda j: (0, 0, 0)), block, block],
        out_specs=pl.BlockSpec((1, BLK, 512), lambda j: (j // per, j % per, 0)),
        out_shape=jax.ShapeDtypeStruct((SEQ // TOK, TOK, 512), jnp.bfloat16),
        scratch_shapes=[
            pltpu.VMEM((SEQ, 256), jnp.float32),
            pltpu.VMEM((BLK, 128), jnp.float32),
            pltpu.VMEM((BLK, 128), jnp.float32),
            pltpu.VMEM((2, 8, SEQ), jnp.float32),
        ],
        compiler_params=pltpu.CompilerParams(vmem_limit_bytes=VMEM_LIMIT, dimension_semantics=('arbitrary',)),
        cost_estimate=pl.CostEstimate(flops=65 * 10 ** 9, bytes_accessed=16 << 20, transcendentals=1 << 24),
        name='attn_bwd',
    )(q, k, v, o, do, lse, cos, sin)


def gather_full(shard):
    return lax.all_gather(shard, ALL_AXES, axis=0, tiled=True)


def gather_seq(shard):
    return lax.all_gather(shard, 'sp', axis=0, tiled=True)


def scatter_sum(partial_sum):
    return lax.psum_scatter(partial_sum, ALL_AXES, scatter_dimension=0, tiled=True)


def swap_seq(parts):
    return lax.all_to_all(parts, 'sp', 0, 0, tiled=True)


def swap_all(parts):
    return lax.all_to_all(parts, ALL_AXES, 0, 0, tiled=True)


def rms_norm(values, gain_vec):
    vals32 = values.astype(jnp.float32)
    inv_rms = lax.rsqrt(jnp.mean(vals32 * vals32, axis=-1, keepdims=True) + NORM_EPS)
    normed = vals32 * inv_rms
    return (normed * gain_vec.astype(jnp.float32)).astype(jnp.bfloat16), normed, inv_rms


def rms_norm_grad(d_out, normed, inv_rms, gain_vec):
    d_normed = d_out * gain_vec.astype(jnp.float32)
    grad_gain = jnp.sum(d_out * normed, axis=0)
    grad_in = inv_rms * (d_normed - normed * jnp.mean(d_normed * normed, axis=-1, keepdims=True))
    return grad_in, grad_gain


def layer_step(hidden, positions, grad_out, gain_attn, gain_mlp, w_query, w_key, w_value, w_out, w_gate, w_up, w_down):
    tokens = hidden[0]
    d_layer = grad_out[0]
    dp = lax.axis_index('dp')
    sp = lax.axis_index('sp')
    f32, bf16 = jnp.float32, jnp.bfloat16

    w_arr = jnp.concatenate(
        [w_query.reshape(128, 2, 4, 256), w_key.reshape(128, 2, 4, 128), w_value.reshape(128, 2, 4, 128)], axis=3)
    w_send = jnp.transpose(w_arr, (2, 0, 1, 3)).reshape(4, 128, 1024)
    x_all = gather_seq(tokens)
    w_own = swap_all(jnp.concatenate([w_send, w_send], axis=0)).reshape(DIM, 1024)
    gains = lax.all_gather(jnp.stack([gain_attn, gain_mlp]), ALL_AXES, axis=1, tiled=True)
    gain1, gain2 = gains[0], gains[1]
    pos_all = gather_seq(positions[0])
    wo_full = gather_full(w_out)
    wg_full = gather_full(w_gate)
    wu_full = gather_full(w_up)
    wd_full = gather_full(w_down)
    w_all = gather_full(w_arr.reshape(128, 4096))

    inv_freq = ROPE_BASE ** (-(jnp.arange(HEAD_DIM // 2, dtype=f32) * (2.0 / HEAD_DIM)))
    angles = pos_all.astype(f32)[:, None] * inv_freq
    cos_half, sin_half = jnp.cos(angles), jnp.sin(angles)
    cos = jnp.concatenate([cos_half, cos_half], axis=1)
    sin = jnp.concatenate([-sin_half, sin_half], axis=1)

    u_all, q0, k0, v0, q1, k1, v1 = qkv_call(x_all, gain1[None], w_own, cos, sin)
    o0, lse0 = fwd_call(q0, k0, v0)
    got0 = swap_seq(o0)
    o1, lse1 = fwd_call(q1, k1, v1)
    got1 = swap_seq(o1)
    attn0 = jnp.transpose(got0, (1, 0, 2)).reshape(TOK, 1024)
    attn1 = jnp.transpose(got1, (1, 0, 2)).reshape(TOK, 1024)
    proj = dot_nn(attn0, wo_full[:1024]) + dot_nn(attn1, wo_full[1024:])
    residual = (tokens.astype(f32) + proj).astype(bf16)

    u_mlp, normed2, inv_rms2 = rms_norm(residual, gain2)
    gate_pre = dot_nn(u_mlp, wg_full)
    up_pre = dot_nn(u_mlp, wu_full)
    sig_gate = jax.nn.sigmoid(gate_pre)
    silu_gate = gate_pre * sig_gate
    mlp_act = (silu_gate * up_pre).astype(bf16)
    layer_out = (residual.astype(f32) + dot_nn(mlp_act, wd_full)).astype(bf16)

    d_act = dot_nt(d_layer, wd_full)
    d_gate = (d_act * up_pre * sig_gate * (1.0 + gate_pre * (1.0 - sig_gate))).astype(bf16)
    d_up = (d_act * silu_gate).astype(bf16)
    d_umlp = dot_nt(d_gate, wg_full) + dot_nt(d_up, wu_full)
    d_res_norm, d_gain2 = rms_norm_grad(d_umlp, normed2, inv_rms2, gain2)
    d_resid = d_layer.astype(f32) + d_res_norm
    dh_all = gather_seq(d_resid.astype(bf16))
    grad_w_down = scatter_sum(dot_tn(mlp_act, d_layer))
    grad_w_gate = scatter_sum(dot_tn(u_mlp, d_gate))
    grad_w_up = scatter_sum(dot_tn(u_mlp, d_up))

    wo_blocks = wo_full.reshape(2, 4, 256, 1024)
    wo_own = lax.dynamic_slice(wo_blocks, (0, sp, 0, 0), (2, 1, 256, 1024))
    o_own = (o0.reshape(SEQ, 256), o1.reshape(SEQ, 256))
    do0 = dot_nt(dh_all, wo_own[0, 0]).astype(bf16)
    do1 = dot_nt(dh_all, wo_own[1, 0]).astype(bf16)
    d0 = bwd_call(q0, k0, v0, o_own[0], do0, lse0, cos, sin)
    back0 = swap_seq(d0)
    dw0 = swap_all(dot_tn(u_all, d0.reshape(SEQ, 512)).reshape(8, 128, 512))
    d1 = bwd_call(q1, k1, v1, o_own[1], do1, lse1, cos, sin)
    back1 = swap_seq(d1)
    dw1 = swap_all(dot_tn(u_all, d1.reshape(SEQ, 512)).reshape(8, 128, 512))

    dwo = jnp.stack([dot_tn(o_own[0], dh_all), dot_tn(o_own[1], dh_all)])
    dwo_send = lax.dynamic_index_in_dim(dwo, 1 - dp, 0, keepdims=False)
    dwo_keep = lax.dynamic_index_in_dim(dwo, dp, 0, keepdims=False)
    grad_w_out = dwo_keep + lax.ppermute(dwo_send, 'dp', [(0, 1), (1, 0)])

    sums = [(t[:4] + t[4:]) for t in (dw0, dw1)]
    cat = lambda lo, hi: jnp.concatenate([jnp.transpose(t[:, :, lo:hi], (1, 0, 2)).reshape(128, -1) for t in sums], axis=1)
    grad_w_query, grad_w_key, grad_w_value = cat(0, 256), cat(256, 384), cat(384, 512)

    flat = lambda t: jnp.transpose(t, (1, 0, 2)).reshape(TOK, 2048)
    d_uattn = dot_nt(flat(back0), w_all[:, :2048]) + dot_nt(flat(back1), w_all[:, 2048:])
    _, normed1, inv_rms1 = rms_norm(tokens, gain1)
    d_tok_norm, d_gain1 = rms_norm_grad(d_uattn, normed1, inv_rms1, gain1)
    grad_hidden = (d_resid + d_tok_norm).astype(bf16)

    gain_parts = jnp.stack([d_gain1.reshape(8, 128), d_gain2.reshape(8, 128)], axis=1)
    gain_sums = jnp.sum(swap_all(gain_parts), axis=0)
    return (layer_out[None], grad_hidden[None], gain_sums[0], gain_sums[1], grad_w_query, grad_w_key, grad_w_value,
            grad_w_out, grad_w_gate, grad_w_up, grad_w_down)


def solution(mesh):
    act_spec = P('dp', 'sp', None)
    pos_spec = P('dp', 'sp')
    vec_spec = P(ALL_AXES)
    mat_spec = P(ALL_AXES, None)
    in_specs = (act_spec, pos_spec, act_spec, vec_spec, vec_spec) + (mat_spec,) * 7
    out_specs = (act_spec, act_spec, vec_spec, vec_spec) + (mat_spec,) * 7
    return jax.shard_map(layer_step, mesh=mesh, in_specs=in_specs, out_specs=out_specs, check_vma=False)
```

```python
import math

import jax
import jax.numpy as jnp
from jax import lax
from jax.experimental import pallas as pl
from jax.experimental.pallas import tpu as pltpu
from jax.sharding import PartitionSpec as P


HEAD_DIM = 128
ROPE_BASE = 10000.0
NORM_EPS = 1e-5
ATTN_SCALE = HEAD_DIM ** -0.5
LOG2E = math.log2(math.e)
SCALE2 = ATTN_SCALE * LOG2E
ALL_AXES = ('dp', 'sp')
BLK = 512
QSUB = 256
SEQ = 4096
TOK = 1024
DIM = 1024
HALF = 1536
SEND = 144
CORE_GROUPS = [[0, 2, 4, 6], [1, 3, 5, 7]]
PAIR = 256
TINY = 10 ** 8
SP = 4
PAIRS = 2
GRP = 512
OWN = 384
NEG = -1e30
VMEM_LIMIT = 60 * 1024 * 1024


def dot_nt(left, right):
    return lax.dot_general(left, right, (((1,), (1,)), ((), ())), preferred_element_type=jnp.float32)


def dot_nn(left, right):
    return lax.dot_general(left, right, (((1,), (0,)), ((), ())), preferred_element_type=jnp.float32)


def dot_tn(left, right):
    return lax.dot_general(left, right, (((0,), (0,)), ((), ())), preferred_element_type=jnp.float32)


def params(**kw):
    return pltpu.CompilerParams(vmem_limit_bytes=VMEM_LIMIT, dimension_semantics=('arbitrary',), **kw)


def cost(flops, mib):
    return pl.CostEstimate(flops=flops, bytes_accessed=mib << 20, transcendentals=0)


def pack_kernel(core_ref, wq_ref, wk_ref, wv_ref, w1_ref, w3_ref, g1_ref, g2_ref, all_ref, send_ref, a1_ref, b1_ref, a3_ref, b3_ref):
    for g in range(PAIRS):
        for n in range(SP):
            m = g * 4 + n
            piece = jnp.concatenate([wq_ref[:, m * PAIR:(m + 1) * PAIR], wk_ref[:, m * HEAD_DIM:(m + 1) * HEAD_DIM], wv_ref[:, m * HEAD_DIM:(m + 1) * HEAD_DIM]], axis=1)
            all_ref[:, m * GRP:(m + 1) * GRP] = piece
            send_ref[n * SEND:n * SEND + HEAD_DIM, g * GRP:(g + 1) * GRP] = piece
    tail = jnp.concatenate([g1_ref[...], g2_ref[...], jnp.zeros((1, DIM - PAIR), jnp.bfloat16)], axis=1)
    for n in range(SP):
        send_ref[n * SEND + HEAD_DIM:(n + 1) * SEND, :] = jnp.broadcast_to(tail, (SEND - HEAD_DIM, DIM))
    core = core_ref[0]
    for ref, own_ref, other_ref in ((w1_ref, a1_ref, b1_ref), (w3_ref, a3_ref, b3_ref)):
        for n in range(SP):
            cols = slice(n * OWN, (n + 1) * OWN)
            own_ref[:, cols] = ref[:, pl.ds(pl.multiple_of((n * 2 + core) * OWN, HEAD_DIM), OWN)]
            other_ref[:, cols] = ref[:, pl.ds(pl.multiple_of((n * 2 + 1 - core) * OWN, HEAD_DIM), OWN)]


def pack_call(core_arr, *weights):
    out = lambda *shape: jax.ShapeDtypeStruct(shape, jnp.bfloat16)
    return pl.pallas_call(
        pack_kernel,
        in_specs=[pl.BlockSpec(memory_space=pltpu.SMEM)] + [pl.BlockSpec(memory_space=pltpu.VMEM)] * 7,
        out_shape=[out(HEAD_DIM, SEQ), out(4 * SEND, DIM)] + [out(HEAD_DIM, HALF)] * 4,
        cost_estimate=cost(TINY, 6),
        name='pack',
    )(core_arr, *weights)


def join_kernel(pos_ref, *refs):
    count = len(refs) // 3
    for n in range(count):
        own_ref, got_ref, out_ref = refs[2 * n], refs[2 * n + 1], refs[2 * count + n]
        rows = own_ref.shape[0]
        out_ref[pl.ds(pl.multiple_of(pos_ref[0] * rows, HEAD_DIM), rows), :] = own_ref[...]
        out_ref[pl.ds(pl.multiple_of((1 - pos_ref[0]) * rows, HEAD_DIM), rows), :] = got_ref[...]


def join_call(pos_arr, *pairs):
    flat = [t for pair in pairs for t in pair]
    return pl.pallas_call(
        join_kernel,
        in_specs=[pl.BlockSpec(memory_space=pltpu.SMEM)] + [pl.BlockSpec(memory_space=pltpu.VMEM)] * len(flat),
        out_shape=[jax.ShapeDtypeStruct((2 * a.shape[0], a.shape[1]), a.dtype) for a, _ in pairs],
        cost_estimate=cost(TINY, 4),
        name='join',
    )(pos_arr, *flat)


def join_qkv_kernel(dp_ref, own_ref, got_ref, w_ref, g1_ref, g2_ref):
    for ref, part in ((own_ref, dp_ref[0]), (got_ref, 1 - dp_ref[0])):
        for n in range(SP):
            rows = pl.ds(pl.multiple_of((part * 4 + n) * HEAD_DIM, HEAD_DIM), HEAD_DIM)
            w_ref[rows, :] = ref[n * SEND:n * SEND + HEAD_DIM, :]
            tail = ref[n * SEND + HEAD_DIM:(n + 1) * SEND, 0:PAIR]
            g1_ref[:, rows] = tail[:, 0:HEAD_DIM]
            g2_ref[:, rows] = tail[:, HEAD_DIM:PAIR]


def join_qkv_call(dp_arr, own, got):
    out = lambda rows: jax.ShapeDtypeStruct((rows, DIM), jnp.bfloat16)
    return pl.pallas_call(
        join_qkv_kernel,
        in_specs=[pl.BlockSpec(memory_space=pltpu.SMEM)] + [pl.BlockSpec(memory_space=pltpu.VMEM)] * 2,
        out_shape=[out(DIM), out(SEND - HEAD_DIM), out(SEND - HEAD_DIM)],
        cost_estimate=cost(TINY, 4),
        name='join_qkv',
    )(dp_arr, own, got)


def unpack_qkv_kernel(p0_ref, p1_ref, wq_ref, wk_ref, wv_ref):
    for g, ref in enumerate((p0_ref, p1_ref)):
        for n in range(SP):
            m = g * 4 + n
            total = ref[n] + ref[4 + n]
            wq_ref[:, m * PAIR:(m + 1) * PAIR] = total[:, 0:PAIR]
            wk_ref[:, m * HEAD_DIM:(m + 1) * HEAD_DIM] = total[:, PAIR:OWN]
            wv_ref[:, m * HEAD_DIM:(m + 1) * HEAD_DIM] = total[:, OWN:GRP]


def unpack_qkv_call(p0, p1):
    out = lambda cols: jax.ShapeDtypeStruct((HEAD_DIM, cols), jnp.float32)
    return pl.pallas_call(unpack_qkv_kernel, out_shape=[out(2048), out(DIM), out(DIM)], cost_estimate=cost(TINY, 6), name='unpack_qkv')(p0, p1)


def unpack_cols_kernel(core_ref, own_ref, got_ref, gate_ref, up_ref):
    core = core_ref[0]
    mine = own_ref[pl.ds(pl.multiple_of(core * HEAD_DIM, HEAD_DIM), HEAD_DIM), :]
    for w, ref in enumerate((gate_ref, up_ref)):
        for n in range(SP):
            cols = slice(w * HALF + n * OWN, w * HALF + (n + 1) * OWN)
            ref[:, pl.ds(pl.multiple_of((n * 2 + core) * OWN, HEAD_DIM), OWN)] = mine[:, cols]
            ref[:, pl.ds(pl.multiple_of((n * 2 + 1 - core) * OWN, HEAD_DIM), OWN)] = got_ref[:, cols]


def unpack_cols_call(core_arr, own, got):
    return pl.pallas_call(
        unpack_cols_kernel,
        in_specs=[pl.BlockSpec(memory_space=pltpu.SMEM)] + [pl.BlockSpec(memory_space=pltpu.VMEM)] * 2,
        out_shape=[jax.ShapeDtypeStruct((HEAD_DIM, 2 * HALF), jnp.float32)] * 2,
        cost_estimate=cost(TINY, 4),
        name='unpack_cols',
    )(core_arr, own, got)


def qkv_kernel(sp_ref, xa_ref, xb_ref, g_ref, w_ref, cos_ref, sin_ref, *rest):
    u_ref, q0_ref, k0_ref, v0_ref, q1_ref, k1_ref, v1_ref, x_scr = rest[-8:]
    i = pl.program_id(0)

    @pl.when(i < 2)
    def _():
        x_scr[...] = xa_ref[...]

    @pl.when(i >= 2)
    def _():
        x_scr[...] = xb_ref[...]

    x32 = x_scr[...].astype(jnp.float32)
    inv_rms = lax.rsqrt(jnp.mean(x32 * x32, axis=-1, keepdims=True) + NORM_EPS)
    u = (x32 * inv_rms * g_ref[...].astype(jnp.float32)).astype(jnp.bfloat16)
    u_ref[...] = u
    cos, sin = cos_ref[...], sin_ref[...]

    def rope(t):
        return (t * cos + pltpu.roll(t, 64, 1) * sin).astype(jnp.bfloat16)

    for g, (q_ref, k_ref, v_ref) in enumerate(((q0_ref, k0_ref, v0_ref), (q1_ref, k1_ref, v1_ref))):
        y = dot_nn(u, w_ref[:, g * GRP:(g + 1) * GRP])
        q_ref[:, 0:HEAD_DIM] = rope(y[:, 0:HEAD_DIM])
        q_ref[:, HEAD_DIM:PAIR] = rope(y[:, HEAD_DIM:PAIR])
        k_ref[...] = rope(y[:, PAIR:OWN])
        v_ref[...] = y[:, OWN:GRP].astype(jnp.bfloat16)


def qkv_call(sp_arr, xa, xb, first, gain, w_own, cos, sin, prev):
    place = lambda width: pl.BlockSpec((BLK, width), lambda i, s: ((s[0] ^ (first + i // 2)) * 2 + i % 2, 0))
    local = lambda width: pl.BlockSpec((BLK, width), lambda i, s: (first * 2 + i, 0))
    fixed = lambda shape: pl.BlockSpec(shape, lambda i, s: (0, 0))
    out = lambda width: jax.ShapeDtypeStruct((SEQ, width), jnp.bfloat16)
    xa_spec = pl.BlockSpec((BLK, DIM), lambda i, s: (jnp.minimum(i, 1), 0))
    xb_spec = pl.BlockSpec((BLK, DIM), lambda i, s: (jnp.maximum(i - 2, 0), 0))
    widths = (DIM, PAIR, HEAD_DIM, HEAD_DIM, PAIR, HEAD_DIM, HEAD_DIM)
    return pl.pallas_call(
        qkv_kernel,
        grid_spec=pltpu.PrefetchScalarGridSpec(
            num_scalar_prefetch=1,
            grid=(4,),
            in_specs=[xa_spec, xb_spec, fixed((1, DIM)), fixed((DIM, DIM)), local(HEAD_DIM), local(HEAD_DIM)]
            + [pl.BlockSpec(memory_space=pl.ANY)] * len(prev),
            out_specs=[local(DIM)] + [place(w) for w in widths[1:]],
            scratch_shapes=[pltpu.VMEM((BLK, DIM), jnp.bfloat16)],
        ),
        out_shape=[out(w) for w in widths],
        input_output_aliases={7 + n: n for n in range(len(prev))},
        compiler_params=params(),
        cost_estimate=cost(2 * 2048 * DIM * DIM, 20),
        name='qkv',
    )(sp_arr, xa, xb, gain, w_own, cos, sin, *prev)


def fwd_kernel(q_ref, k_ref, v_ref, o_ref, lse_ref, acc_ref, q_scr):
    i = pl.program_id(0)
    for h in range(PAIRS):
        q_scr[h * BLK:(h + 1) * BLK, :] = q_ref[:, h * HEAD_DIM:(h + 1) * HEAD_DIM]

    chunks = [(h, n) for h in range(PAIRS) for n in range(BLK // QSUB)]

    def step(j, carry, masked):
        start = pl.multiple_of(j * BLK, BLK)
        k = k_ref[pl.ds(start, BLK), :]
        v = v_ref[pl.ds(start, BLK), :]

        def scores(c):
            h, n = chunks[c]
            s = dot_nt(k, q_scr[h * BLK + n * QSUB:h * BLK + (n + 1) * QSUB, :])
            if masked:
                kv_idx = lax.broadcasted_iota(jnp.int32, (BLK, QSUB), 0)
                q_idx = lax.broadcasted_iota(jnp.int32, (BLK, QSUB), 1) + n * QSUB
                s = jnp.where(q_idx >= kv_idx, s, NEG)
            return s

        out = []
        s_next = scores(0)
        for c in range(len(chunks)):
            s = s_next
            if c + 1 < len(chunks):
                s_next = scores(c + 1)
            m, l = carry[c]
            m_new = jnp.maximum(m, jnp.max(s, axis=0, keepdims=True))
            p = jnp.exp2(s * SCALE2 - m_new * SCALE2)
            alpha = jnp.exp2((m - m_new) * SCALE2)
            l_new = alpha * l + jnp.sum(p, axis=0, keepdims=True)
            acc_ref[c] = acc_ref[c] * alpha + dot_tn(v, p.astype(jnp.bfloat16))
            out.append((m_new, l_new))
        return tuple(out)

    acc_ref[...] = jnp.zeros_like(acc_ref)
    init = tuple((jnp.full((1, QSUB), NEG, jnp.float32), jnp.zeros((1, QSUB), jnp.float32)) for _ in chunks)
    carry = lax.fori_loop(0, i, lambda j, c: step(j, c, False), init)
    carry = step(i, carry, True)
    for c, (h, n) in enumerate(chunks):
        m, l = carry[c]
        rows = slice(n * QSUB, (n + 1) * QSUB)
        o_ref[0, rows, h * HEAD_DIM:(h + 1) * HEAD_DIM] = (acc_ref[c] / l).T.astype(jnp.bfloat16)
        lse_ref[h, :, rows] = jnp.broadcast_to(m * SCALE2 + jnp.log2(l), (8, QSUB))


def fwd_call(q, k, v):
    fixed = pl.BlockSpec((SEQ, HEAD_DIM), lambda i: (0, 0))
    per = TOK // BLK
    return pl.pallas_call(
        fwd_kernel,
        grid=(SEQ // BLK,),
        in_specs=[pl.BlockSpec((BLK, PAIR), lambda i: (i, 0)), fixed, fixed],
        out_specs=[pl.BlockSpec((1, BLK, PAIR), lambda i: (i // per, i % per, 0)), pl.BlockSpec((2, 8, BLK), lambda i: (0, 0, i))],
        out_shape=[jax.ShapeDtypeStruct((SEQ // TOK, TOK, PAIR), jnp.bfloat16), jax.ShapeDtypeStruct((2, 8, SEQ), jnp.float32)],
        scratch_shapes=[pltpu.VMEM((2 * BLK // QSUB, HEAD_DIM, QSUB), jnp.float32), pltpu.VMEM((2 * BLK, HEAD_DIM), jnp.bfloat16)],
        compiler_params=params(),
        cost_estimate=cost(24 * 10 ** 9, 8),
        name='attn_fwd',
    )(q, k, v)


def bwd_kernel(sp_ref, q_ref, k_ref, v_ref, o_ref, do_ref, lse_ref, cos_ref, sin_ref, out0_ref, out1_ref, out2_ref, out3_ref, dq_acc, dk_acc, dv_acc, delta):
    j = pl.program_id(0)
    n_blk = SEQ // BLK

    @pl.when(j == 0)
    def _():
        dq_acc[...] = jnp.zeros_like(dq_acc)

        def rows(i, _):
            start = pl.multiple_of(i * BLK, BLK)
            prod = o_ref[pl.ds(start, BLK), :].astype(jnp.float32) * do_ref[pl.ds(start, BLK), :].astype(jnp.float32)
            for h in range(PAIRS):
                tot = jnp.sum(prod[:, h * HEAD_DIM:(h + 1) * HEAD_DIM], axis=1, keepdims=True)
                delta[h, :, pl.ds(start, BLK)] = jnp.broadcast_to(tot, (BLK, HEAD_DIM)).T[0:8, :]
            return 0

        lax.fori_loop(0, n_blk, rows, 0)

    k = k_ref[...]
    v = v_ref[...]
    dk_acc[...] = jnp.zeros_like(dk_acc)
    dv_acc[...] = jnp.zeros_like(dv_acc)

    def step(i, masked):
        start = pl.multiple_of(i * BLK, BLK)
        rows = pl.ds(start, BLK)
        for h in range(PAIRS):
            cols = slice(h * HEAD_DIM, (h + 1) * HEAD_DIM)
            q = q_ref[rows, cols]
            do = do_ref[rows, cols]
            s = dot_nt(k, q)
            p = jnp.exp2(s * SCALE2 - lse_ref[h, 0:1, rows])
            if masked:
                kv_idx = lax.broadcasted_iota(jnp.int32, (BLK, BLK), 0)
                q_idx = lax.broadcasted_iota(jnp.int32, (BLK, BLK), 1)
                p = jnp.where(q_idx >= kv_idx, p, 0.0)
            dp = dot_nt(v, do)
            dv_acc[...] += dot_nn(p.astype(jnp.bfloat16), do)
            ds = (p * (dp - delta[h, 0:1, rows]) * ATTN_SCALE).astype(jnp.bfloat16)
            dk_acc[...] += dot_nn(ds, q)
            dq_acc[rows, cols] += dot_tn(ds, k)

    step(j, True)

    def body(i, _):
        step(i, False)
        return 0

    lax.fori_loop(j + 1, n_blk, body, 0)

    cos, sin = cos_ref[...], sin_ref[...]

    def rope_back(t):
        t = t.astype(jnp.bfloat16).astype(jnp.float32)
        return (t * cos - pltpu.roll(t, 64, 1) * sin).astype(jnp.bfloat16)

    mine = pl.ds(pl.multiple_of(j * BLK, BLK), BLK)
    result = jnp.concatenate(
        [rope_back(dq_acc[mine, h * HEAD_DIM:(h + 1) * HEAD_DIM]) for h in range(PAIRS)] + [rope_back(dk_acc[...]), dv_acc[...].astype(jnp.bfloat16)], axis=1)
    for n, ref in enumerate((out0_ref, out1_ref, out2_ref, out3_ref)):
        @pl.when((j * BLK // TOK) ^ sp_ref[0] == n)
        def _(ref=ref):
            ref[...] = result


def bwd_call(sp_arr, q, k, v, o, do, lse, cos, sin):
    whole = lambda width: pl.BlockSpec((SEQ, width), lambda j, s: (0, 0))
    block = pl.BlockSpec((BLK, HEAD_DIM), lambda j, s: (j, 0))
    per = TOK // BLK
    table = pl.BlockSpec((BLK, HEAD_DIM), lambda j, s: (((j // per) ^ s[0]) * per + j % per, 0))
    piece = lambda n: pl.BlockSpec((BLK, GRP), lambda j, s: (jnp.clip(j - per * (s[0] ^ n), 0, per - 1), 0))
    return pl.pallas_call(
        bwd_kernel,
        grid_spec=pltpu.PrefetchScalarGridSpec(
            num_scalar_prefetch=1,
            grid=(SEQ // BLK,),
            in_specs=[whole(PAIR), block, block, whole(PAIR), whole(PAIR), pl.BlockSpec((2, 8, SEQ), lambda j, s: (0, 0, 0)), table, table],
            out_specs=[piece(n) for n in range(SP)],
            scratch_shapes=[
                pltpu.VMEM((SEQ, PAIR), jnp.float32),
                pltpu.VMEM((BLK, HEAD_DIM), jnp.float32),
                pltpu.VMEM((BLK, HEAD_DIM), jnp.float32),
                pltpu.VMEM((2, 8, SEQ), jnp.float32),
            ],
        ),
        out_shape=[jax.ShapeDtypeStruct((TOK, GRP), jnp.bfloat16)] * 4,
        compiler_params=params(),
        cost_estimate=cost(60 * 10 ** 9, 16),
        name='attn_bwd',
    )(sp_arr, q, k, v, o, do, lse, cos, sin)


def oproj_kernel(a0_ref, a1_ref, w_ref, x_ref, g_ref, h_ref, u_ref):
    total = x_ref[...].astype(jnp.float32)
    for g, a_ref in enumerate((a0_ref, a1_ref)):
        a = jnp.concatenate([a_ref[s] for s in range(SP)], axis=1)
        total += dot_nn(a, w_ref[g * DIM:(g + 1) * DIM, :])
    h = total.astype(jnp.bfloat16)
    h_ref[...] = h
    h32 = h.astype(jnp.float32)
    inv_rms = lax.rsqrt(jnp.mean(h32 * h32, axis=-1, keepdims=True) + NORM_EPS)
    u_ref[...] = (h32 * inv_rms * g_ref[...].astype(jnp.float32)).astype(jnp.bfloat16)


def oproj_call(a0, a1, wo, x, gain):
    blk = PAIR
    row = pl.BlockSpec((blk, DIM), lambda i: (i, 0))
    part = pl.BlockSpec((4, blk, PAIR), lambda i: (0, i, 0))
    return pl.pallas_call(
        oproj_kernel,
        grid=(TOK // blk,),
        in_specs=[part, part, pl.BlockSpec((2048, DIM), lambda i: (0, 0)), row, pl.BlockSpec((1, DIM), lambda i: (0, 0))],
        out_specs=[row, row],
        out_shape=[jax.ShapeDtypeStruct((TOK, DIM), jnp.bfloat16)] * 2,
        compiler_params=params(),
        cost_estimate=cost(2 * TOK * DIM * 2048, 14),
        name='oproj',
    )(a0, a1, wo, x, gain)


def mlp_kernel(u_ref, dy_ref, w1_ref, w3_ref, w2_ref, z_ref, da_ref, dc_ref, y_ref, d_ref):
    u, dy = u_ref[...], dy_ref[...]
    for n in range(HALF // GRP):
        cols = slice(n * GRP, (n + 1) * GRP)
        gate = dot_nn(u, w1_ref[:, cols])
        up = dot_nn(u, w3_ref[:, cols])
        e = dot_nt(dy, w2_ref[cols, :])
        sig = 1.0 / (1.0 + jnp.exp(-gate))
        silu = gate * sig
        z_ref[:, cols] = (silu * up).astype(jnp.bfloat16)
        da_ref[:, cols] = (e * up * sig * (1.0 + gate * (1.0 - sig))).astype(jnp.bfloat16)
        dc_ref[:, cols] = (e * silu).astype(jnp.bfloat16)
    d_ref[...] = dot_nt(da_ref[...], w1_ref[...]) + dot_nt(dc_ref[...], w3_ref[...])
    y_ref[...] = dot_nn(z_ref[...], w2_ref[...])


def mlp_call(u, dy, w1, w3, w2):
    blk = PAIR
    row = lambda width: pl.BlockSpec((blk, width), lambda i: (i, 0))
    fixed = lambda shape: pl.BlockSpec(shape, lambda i: (0, 0))
    return pl.pallas_call(
        mlp_kernel,
        grid=(TOK // blk,),
        in_specs=[row(DIM), row(DIM), fixed((DIM, HALF)), fixed((DIM, HALF)), fixed((HALF, DIM))],
        out_specs=[row(HALF), row(HALF), row(HALF), row(DIM), row(DIM)],
        out_shape=[jax.ShapeDtypeStruct((TOK, HALF), jnp.bfloat16)] * 3 + [jax.ShapeDtypeStruct((TOK, DIM), jnp.float32)] * 2,
        compiler_params=params(),
        cost_estimate=cost(12 * TOK * DIM * HALF, 30),
        name='mlp',
    )(u, dy, w1, w3, w2)


def dw_kernel(la_ref, lb_ref, *refs):
    rights, out_ref = refs[:-1], refs[-1]
    for n in range(len(rights) // 2):
        ra_ref, rb_ref = rights[2 * n], rights[2 * n + 1]
        cols = ra_ref.shape[1]
        out_ref[:, n * cols:(n + 1) * cols] = dot_tn(la_ref[...], ra_ref[...]) + dot_tn(lb_ref[...], rb_ref[...])


def dw_call(la, lb, *rights):
    rows, cols = la.shape[1] // 4, rights[0].shape[1]
    total = cols * len(rights) // 2
    left = pl.BlockSpec((TOK, rows), lambda b: (0, b))
    right = pl.BlockSpec((TOK, cols), lambda b: (0, 0))
    return pl.pallas_call(
        dw_kernel,
        grid=(4,),
        in_specs=[left, left] + [right] * len(rights),
        out_specs=pl.BlockSpec((rows, total), lambda b: (b, 0)),
        out_shape=jax.ShapeDtypeStruct((4 * rows, total), jnp.float32),
        compiler_params=params(),
        cost_estimate=cost(4 * TOK * rows * 4 * total, 20),
        name='dw',
    )(la, lb, *rights)


def dw_qkv_kernel(u_ref, *refs):
    out_ref = refs[-1]
    total = dot_tn(u_ref[0:TOK, :], refs[0][...])
    for n in range(1, 4):
        total += dot_tn(u_ref[n * TOK:(n + 1) * TOK, :], refs[n][...])
    out_ref[...] = total


def dw_qkv_call(u, pieces):
    return pl.pallas_call(
        dw_qkv_kernel,
        grid=(4,),
        in_specs=[pl.BlockSpec((SEQ, PAIR), lambda b: (0, b))] + [pl.BlockSpec((TOK, GRP), lambda b: (0, 0))] * 4,
        out_specs=pl.BlockSpec((PAIR, GRP), lambda b: (b, 0)),
        out_shape=jax.ShapeDtypeStruct((DIM, GRP), jnp.float32),
        compiler_params=params(),
        cost_estimate=cost(2 * SEQ * DIM * GRP, 14),
        name='dw_qkv',
    )(u, *pieces)


def dout_kernel(sp_ref, h0_ref, h1_ref, h2_ref, h3_ref, o0_ref, o1_ref, wa_ref, wb_ref, d0_ref, d1_ref, dwo_ref, scr):
    i = pl.program_id(0)
    for n, ref in enumerate((h0_ref, h1_ref, h2_ref, h3_ref)):
        @pl.when(i // 2 == n)
        def _(ref=ref):
            scr[...] = ref[...]
    dh = scr[...]
    d0_ref[...] = dot_nt(dh, wa_ref[...]).astype(jnp.bfloat16)
    d1_ref[...] = dot_nt(dh, wb_ref[...]).astype(jnp.bfloat16)

    @pl.when(i == 0)
    def _():
        dwo_ref[...] = jnp.zeros_like(dwo_ref)

    dwo_ref[0] += dot_tn(o0_ref[0], dh)
    dwo_ref[1] += dot_tn(o1_ref[0], dh)


def dout_call(sp_arr, dhs, o0, o1, wo):
    src = lambda n: pl.BlockSpec((BLK, DIM), lambda i, s: (jnp.clip(i - 2 * n, 0, 1), 0))
    o_spec = pl.BlockSpec((1, BLK, PAIR), lambda i, s: (s[0] ^ (i // 2), i % 2, 0))
    d_spec = pl.BlockSpec((BLK, PAIR), lambda i, s: ((s[0] ^ (i // 2)) * 2 + i % 2, 0))
    out = jax.ShapeDtypeStruct((SEQ, PAIR), jnp.bfloat16)
    return pl.pallas_call(
        dout_kernel,
        grid_spec=pltpu.PrefetchScalarGridSpec(
            num_scalar_prefetch=1,
            grid=(SEQ // BLK,),
            in_specs=[src(0), src(1), src(2), src(3), o_spec, o_spec,
                      pl.BlockSpec((PAIR, DIM), lambda i, s: (s[0], 0)), pl.BlockSpec((PAIR, DIM), lambda i, s: (4 + s[0], 0))],
            out_specs=[d_spec, d_spec, pl.BlockSpec((2, PAIR, DIM), lambda i, s: (0, 0, 0))],
            scratch_shapes=[pltpu.VMEM((BLK, DIM), jnp.bfloat16)],
        ),
        out_shape=[out, out, jax.ShapeDtypeStruct((2, PAIR, DIM), jnp.float32)],
        compiler_params=params(),
        cost_estimate=cost(4 * SEQ * DIM * GRP, 20),
        name='dout',
    )(sp_arr, *dhs, o0, o1, wo, wo)


def dx_kernel(sp_ref, *refs):
    pieces, (w_ref, x_ref, dr_ref, g_ref, dx_ref, dg_ref) = refs[:8], refs[8:]
    i = pl.program_id(0)
    d_u = jnp.zeros(dr_ref.shape, jnp.float32)
    for n in range(8):
        cols = pl.ds(pl.multiple_of(((n // 4) * 4 + (sp_ref[0] ^ (n % 4))) * GRP, GRP), GRP)
        piece = pieces[n][...]
        d_u += dot_nt(piece, w_ref[:, cols])
    x32 = x_ref[...].astype(jnp.float32)
    inv_rms = lax.rsqrt(jnp.mean(x32 * x32, axis=-1, keepdims=True) + NORM_EPS)
    normed = x32 * inv_rms
    d_normed = d_u * g_ref[...].astype(jnp.float32)
    grad_in = inv_rms * (d_normed - normed * jnp.mean(d_normed * normed, axis=-1, keepdims=True))
    dx_ref[...] = (dr_ref[...] + grad_in).astype(jnp.bfloat16)

    @pl.when(i == 0)
    def _():
        dg_ref[...] = jnp.zeros_like(dg_ref)

    dg_ref[...] += jnp.sum(d_u * normed, axis=0, keepdims=True)


def dx_call(sp_arr, pieces, w_all, x, d_resid, gain):
    blk = PAIR
    row = lambda width: pl.BlockSpec((blk, width), lambda i, s: (i, 0))
    one = pl.BlockSpec((1, DIM), lambda i, s: (0, 0))
    return pl.pallas_call(
        dx_kernel,
        grid_spec=pltpu.PrefetchScalarGridSpec(
            num_scalar_prefetch=1,
            grid=(TOK // blk,),
            in_specs=[row(GRP)] * 8 + [pl.BlockSpec((DIM, SEQ), lambda i, s: (0, 0)), row(DIM), row(DIM), one],
            out_specs=[row(DIM), one],
        ),
        out_shape=[jax.ShapeDtypeStruct((TOK, DIM), jnp.bfloat16), jax.ShapeDtypeStruct((1, DIM), jnp.float32)],
        compiler_params=params(),
        cost_estimate=cost(2 * TOK * DIM * SEQ, 24),
        name='dx',
    )(sp_arr, *pieces, w_all, x, d_resid, gain)


def gather_full(shard):
    return lax.all_gather(shard, ALL_AXES, axis=0, tiled=True)


def gather_core(shard):
    return lax.all_gather(shard, ALL_AXES, axis=0, tiled=True, axis_index_groups=CORE_GROUPS)


def swap_seq(parts):
    return lax.all_to_all(parts, 'sp', 0, 0, tiled=True)


def swap_all(parts):
    return lax.all_to_all(parts, ALL_AXES, 0, 0, tiled=True)


def from_sp(value, bits):
    return lax.ppermute(value, 'sp', [(s, s ^ bits) for s in range(SP)])


def from_dp(value):
    return lax.ppermute(value, 'dp', [(0, 1), (1, 0)])


def gather_chip_then_core(value):
    far = from_sp(value, 2)
    return value, from_sp(value, 1), far, from_sp(far, 1)


def reduce_chips(part):
    return lax.psum_scatter(part, ALL_AXES, scatter_dimension=0, tiled=True, axis_index_groups=CORE_GROUPS)


def layer_step(hidden, positions, grad_out, gain_attn, gain_mlp, w_query, w_key, w_value, w_out, w_gate, w_up, w_down):
    tokens = hidden[0]
    d_layer = grad_out[0]
    dp = lax.axis_index('dp')
    sp = lax.axis_index('sp')
    core = sp % 2
    f32, bf16 = jnp.float32, jnp.bfloat16
    sp_arr, dp_arr, core_arr = (t.astype(jnp.int32)[None] for t in (sp, dp, core))

    xs = gather_chip_then_core(tokens)
    w_cols, w_send, a1, b1, a3, b3 = pack_call(core_arr, w_query, w_key, w_value, w_gate, w_up, gain_attn[None], gain_mlp[None])
    w_mine = swap_seq(w_send)
    w_own, gain1, gain2 = join_qkv_call(dp_arr, w_mine, from_dp(w_mine))
    gain1, gain2 = gain1[0:1], gain2[0:1]
    pos = gather_chip_then_core(positions[0].reshape(8, HEAD_DIM))
    pos_all = jnp.concatenate(pos).reshape(SEQ)
    w1_rows, w3_rows = join_call(core_arr, (a1, from_sp(b1, 1)), (a3, from_sp(b3, 1)))
    wo_full = gather_full(w_out)
    w2 = gather_core(w_down)
    w1, w3 = gather_core(w1_rows), gather_core(w3_rows)
    w_all = gather_full(w_cols)
    dy_pair = from_sp(d_layer, 1)

    lane = jnp.arange(HEAD_DIM)
    half = HEAD_DIM // 2
    inv_freq = ROPE_BASE ** (-((lane % half).astype(f32) * (2.0 / HEAD_DIM)))
    angles = pos_all.astype(f32)[:, None] * inv_freq
    cos = jnp.cos(angles)
    sin = jnp.sin(angles) * jnp.where(lane < half, -1.0, 1.0)

    near = qkv_call(sp_arr, xs[0], xs[1], 0, gain1, w_own, cos, sin, ())
    u_all, q0, k0, v0, q1, k1, v1 = qkv_call(sp_arr, xs[2], xs[3], 2, gain1, w_own, cos, sin, near)
    o0, lse0 = fwd_call(q0, k0, v0)
    got0 = swap_seq(o0)
    o1, lse1 = fwd_call(q1, k1, v1)
    got1 = swap_seq(o1)
    residual, u_mlp = oproj_call(got0, got1, wo_full, tokens, gain2)

    u_pair = from_sp(u_mlp, 1)
    z_a, da_a, dc_a, y_a, d_a = mlp_call(u_mlp, d_layer, w1, w3, w2)
    z_b, da_b, dc_b, y_b, d_b = mlp_call(u_pair, dy_pair, w1, w3, w2)
    d_umlp = d_a + from_sp(d_b, 1)
    h32 = residual.astype(f32)
    layer_out = (h32 + (y_a + from_sp(y_b, 1))).astype(bf16)
    inv_rms2 = lax.rsqrt(jnp.mean(h32 * h32, axis=-1, keepdims=True) + NORM_EPS)
    normed2 = h32 * inv_rms2
    d_normed2 = d_umlp * gain2.astype(f32)
    d_gain2 = jnp.sum(d_umlp * normed2, axis=0)
    d_resid = d_layer.astype(f32) + inv_rms2 * (d_normed2 - normed2 * jnp.mean(d_normed2 * normed2, axis=-1, keepdims=True))
    dhs = gather_chip_then_core(d_resid.astype(bf16))
    grad_w_down = reduce_chips(dw_call(z_a, z_b, d_layer, dy_pair))

    part = reduce_chips(dw_call(u_mlp, u_pair, da_a, da_b, dc_a, dc_b))

    do0, do1, dwo = dout_call(sp_arr, dhs, o0, o1, wo_full)
    o_seq = (o0.reshape(SEQ, PAIR), o1.reshape(SEQ, PAIR))
    d0 = bwd_call(sp_arr, q0, k0, v0, o_seq[0], do0, lse0, cos, sin)
    back0 = [d0[0]] + [from_sp(d0[n], n) for n in (2, 3, 1)]
    part0 = dw_qkv_call(u_all, d0).reshape(8, HEAD_DIM, GRP)
    dw0 = swap_all(part0)
    d1 = bwd_call(sp_arr, q1, k1, v1, o_seq[1], do1, lse1, cos, sin)
    back1 = [d1[0]] + [from_sp(d1[n], n) for n in (2, 3, 1)]
    part1 = dw_qkv_call(u_all, d1).reshape(8, HEAD_DIM, GRP)
    part1, _ = lax.optimization_barrier((part1, dw0))
    dw1 = swap_all(part1)
    pieces = [t[n] for t in (back0, back1) for n in (0, 3, 1, 2)]

    grad_w_out = lax.dynamic_index_in_dim(dwo, dp, 0, keepdims=False) + from_dp(lax.dynamic_index_in_dim(dwo, 1 - dp, 0, keepdims=False))
    grad_w_query, grad_w_key, grad_w_value = unpack_qkv_call(dw0, dw1)

    grad_hidden, d_gain1 = dx_call(sp_arr, pieces, w_all, tokens, d_resid, gain1)
    part, _ = lax.optimization_barrier((part, d_gain1))
    send = lax.dynamic_slice(part, ((1 - core) * HEAD_DIM, 0), (HEAD_DIM, 2 * HALF))
    grad_w_gate, grad_w_up = unpack_cols_call(core_arr, part, from_sp(send, 1))
    gain_parts = jnp.stack([d_gain1.reshape(8, HEAD_DIM), d_gain2.reshape(8, HEAD_DIM)], axis=1)
    gain_parts, _ = lax.optimization_barrier((gain_parts, dw1))
    gain_sums = jnp.sum(swap_all(gain_parts), axis=0)
    return (layer_out[None], grad_hidden[None], gain_sums[0], gain_sums[1], grad_w_query, grad_w_key, grad_w_value,
            grad_w_out, grad_w_gate, grad_w_up, grad_w_down)


def solution(mesh):
    act_spec = P('dp', 'sp', None)
    pos_spec = P('dp', 'sp')
    vec_spec = P(ALL_AXES)
    mat_spec = P(ALL_AXES, None)
    in_specs = (act_spec, pos_spec, act_spec, vec_spec, vec_spec) + (mat_spec,) * 7
    out_specs = (act_spec, act_spec, vec_spec, vec_spec) + (mat_spec,) * 7

    return jax.shard_map(layer_step, mesh=mesh, in_specs=in_specs, out_specs=out_specs, check_vma=False)
```

```python
import math

import jax
import jax.numpy as jnp
from jax import lax
from jax.experimental import pallas as pl
from jax.experimental.pallas import tpu as pltpu
from jax.sharding import PartitionSpec as P


HEAD_DIM = 128
ROPE_BASE = 10000.0
NORM_EPS = 1e-5
ATTN_SCALE = HEAD_DIM ** -0.5
LOG2E = math.log2(math.e)
SCALE2 = ATTN_SCALE * LOG2E
ALL_AXES = ('dp', 'sp')
BLK = 512
QSUB = 256
SEQ = 4096
TOK = 1024
DIM = 1024
HALF = 1536
SEND = 144
CORE_GROUPS = [[0, 2, 4, 6], [1, 3, 5, 7]]
PAIR = 256
TINY = 10 ** 8
SP = 4
PAIRS = 2
GRP = 512
OWN = 384
NEG = -1e30
VMEM_LIMIT = 60 * 1024 * 1024


def dot_nt(left, right):
    return lax.dot_general(left, right, (((1,), (1,)), ((), ())), preferred_element_type=jnp.float32)


def dot_nn(left, right):
    return lax.dot_general(left, right, (((1,), (0,)), ((), ())), preferred_element_type=jnp.float32)


def dot_tn(left, right):
    return lax.dot_general(left, right, (((0,), (0,)), ((), ())), preferred_element_type=jnp.float32)


def fixed(shape):
    return pl.BlockSpec(shape, lambda *_: tuple(0 for _ in shape))


def params(**kw):
    return pltpu.CompilerParams(vmem_limit_bytes=VMEM_LIMIT, dimension_semantics=('arbitrary',), **kw)


def cost(flops, mib):
    return pl.CostEstimate(flops=flops, bytes_accessed=mib << 20, transcendentals=0)


def pack_kernel(core_ref, wq_ref, wk_ref, wv_ref, w1_ref, w3_ref, g1_ref, g2_ref, all_ref, send_ref, a1_ref, b1_ref, a3_ref, b3_ref):
    for g in range(PAIRS):
        for n in range(SP):
            m = g * 4 + n
            piece = jnp.concatenate([wq_ref[:, m * PAIR:(m + 1) * PAIR], wk_ref[:, m * HEAD_DIM:(m + 1) * HEAD_DIM], wv_ref[:, m * HEAD_DIM:(m + 1) * HEAD_DIM]], axis=1)
            all_ref[:, m * GRP:(m + 1) * GRP] = piece
            send_ref[n * SEND:n * SEND + HEAD_DIM, g * GRP:(g + 1) * GRP] = piece
    tail = jnp.concatenate([g1_ref[...], g2_ref[...], jnp.zeros((1, DIM - PAIR), jnp.bfloat16)], axis=1)
    for n in range(SP):
        send_ref[n * SEND + HEAD_DIM:(n + 1) * SEND, :] = jnp.broadcast_to(tail, (SEND - HEAD_DIM, DIM))
    core = core_ref[0]
    for ref, own_ref, other_ref in ((w1_ref, a1_ref, b1_ref), (w3_ref, a3_ref, b3_ref)):
        for n in range(SP):
            cols = slice(n * OWN, (n + 1) * OWN)
            own_ref[:, cols] = ref[:, pl.ds(pl.multiple_of((n * 2 + core) * OWN, HEAD_DIM), OWN)]
            other_ref[:, cols] = ref[:, pl.ds(pl.multiple_of((n * 2 + 1 - core) * OWN, HEAD_DIM), OWN)]


def pack_call(core_arr, *weights):
    out = lambda *shape: jax.ShapeDtypeStruct(shape, jnp.bfloat16)
    return pl.pallas_call(
        pack_kernel,
        in_specs=[pl.BlockSpec(memory_space=pltpu.SMEM)] + [pl.BlockSpec(memory_space=pltpu.VMEM)] * 7,
        out_shape=[out(HEAD_DIM, SEQ), out(4 * SEND, DIM)] + [out(HEAD_DIM, HALF)] * 4,
        cost_estimate=cost(TINY, 6),
        name='pack',
    )(core_arr, *weights)


def join_kernel(pos_ref, *refs):
    count = len(refs) // 3
    for n in range(count):
        own_ref, got_ref, out_ref = refs[2 * n], refs[2 * n + 1], refs[2 * count + n]
        rows = own_ref.shape[0]
        out_ref[pl.ds(pl.multiple_of(pos_ref[0] * rows, HEAD_DIM), rows), :] = own_ref[...]
        out_ref[pl.ds(pl.multiple_of((1 - pos_ref[0]) * rows, HEAD_DIM), rows), :] = got_ref[...]


def join_call(pos_arr, *pairs):
    flat = [t for pair in pairs for t in pair]
    return pl.pallas_call(
        join_kernel,
        in_specs=[pl.BlockSpec(memory_space=pltpu.SMEM)] + [pl.BlockSpec(memory_space=pltpu.VMEM)] * len(flat),
        out_shape=[jax.ShapeDtypeStruct((2 * a.shape[0], a.shape[1]), a.dtype) for a, _ in pairs],
        cost_estimate=cost(TINY, 4),
        name='join',
    )(pos_arr, *flat)


def join_qkv_kernel(dp_ref, own_ref, got_ref, w_ref, g1_ref, g2_ref):
    for ref, part in ((own_ref, dp_ref[0]), (got_ref, 1 - dp_ref[0])):
        for n in range(SP):
            rows = pl.ds(pl.multiple_of((part * 4 + n) * HEAD_DIM, HEAD_DIM), HEAD_DIM)
            w_ref[rows, :] = ref[n * SEND:n * SEND + HEAD_DIM, :]
            tail = ref[n * SEND + HEAD_DIM:(n + 1) * SEND, 0:PAIR]
            g1_ref[:, rows] = tail[:, 0:HEAD_DIM]
            g2_ref[:, rows] = tail[:, HEAD_DIM:PAIR]


def join_qkv_call(dp_arr, own, got):
    out = lambda rows: jax.ShapeDtypeStruct((rows, DIM), jnp.bfloat16)
    return pl.pallas_call(
        join_qkv_kernel,
        in_specs=[pl.BlockSpec(memory_space=pltpu.SMEM)] + [pl.BlockSpec(memory_space=pltpu.VMEM)] * 2,
        out_shape=[out(DIM), out(SEND - HEAD_DIM), out(SEND - HEAD_DIM)],
        cost_estimate=cost(TINY, 4),
        name='join_qkv',
    )(dp_arr, own, got)


def unpack_qkv_kernel(p0_ref, p1_ref, wq_ref, wk_ref, wv_ref):
    for g, ref in enumerate((p0_ref, p1_ref)):
        for n in range(SP):
            m = g * 4 + n
            total = ref[n] + ref[4 + n]
            wq_ref[:, m * PAIR:(m + 1) * PAIR] = total[:, 0:PAIR]
            wk_ref[:, m * HEAD_DIM:(m + 1) * HEAD_DIM] = total[:, PAIR:OWN]
            wv_ref[:, m * HEAD_DIM:(m + 1) * HEAD_DIM] = total[:, OWN:GRP]


def unpack_qkv_call(p0, p1):
    out = lambda cols: jax.ShapeDtypeStruct((HEAD_DIM, cols), jnp.float32)
    return pl.pallas_call(unpack_qkv_kernel, out_shape=[out(2048), out(DIM), out(DIM)], cost_estimate=cost(TINY, 6), name='unpack_qkv')(p0, p1)


def unpack_cols_kernel(core_ref, own_ref, got_ref, gate_ref, up_ref):
    core = core_ref[0]
    mine = own_ref[pl.ds(pl.multiple_of(core * HEAD_DIM, HEAD_DIM), HEAD_DIM), :]
    for w, ref in enumerate((gate_ref, up_ref)):
        for n in range(SP):
            cols = slice(w * HALF + n * OWN, w * HALF + (n + 1) * OWN)
            ref[:, pl.ds(pl.multiple_of((n * 2 + core) * OWN, HEAD_DIM), OWN)] = mine[:, cols]
            ref[:, pl.ds(pl.multiple_of((n * 2 + 1 - core) * OWN, HEAD_DIM), OWN)] = got_ref[:, cols]


def unpack_cols_call(core_arr, own, got):
    return pl.pallas_call(
        unpack_cols_kernel,
        in_specs=[pl.BlockSpec(memory_space=pltpu.SMEM)] + [pl.BlockSpec(memory_space=pltpu.VMEM)] * 2,
        out_shape=[jax.ShapeDtypeStruct((HEAD_DIM, 2 * HALF), jnp.float32)] * 2,
        cost_estimate=cost(TINY, 4),
        name='unpack_cols',
    )(core_arr, own, got)


def qkv_kernel(sp_ref, xa_ref, xb_ref, g_ref, w_ref, cos_ref, sin_ref, *rest):
    u_ref, q0_ref, k0_ref, v0_ref, q1_ref, k1_ref, v1_ref, x_scr = rest[-8:]
    i = pl.program_id(0)

    @pl.when(i < 2)
    def _():
        x_scr[...] = xa_ref[...]

    @pl.when(i >= 2)
    def _():
        x_scr[...] = xb_ref[...]

    x32 = x_scr[...].astype(jnp.float32)
    inv_rms = lax.rsqrt(jnp.mean(x32 * x32, axis=-1, keepdims=True) + NORM_EPS)
    u = (x32 * inv_rms * g_ref[...].astype(jnp.float32)).astype(jnp.bfloat16)
    u_ref[...] = u
    cos, sin = cos_ref[...], sin_ref[...]

    def rope(t):
        return (t * cos + pltpu.roll(t, 64, 1) * sin).astype(jnp.bfloat16)

    for g, (q_ref, k_ref, v_ref) in enumerate(((q0_ref, k0_ref, v0_ref), (q1_ref, k1_ref, v1_ref))):
        y = dot_nn(u, w_ref[:, g * GRP:(g + 1) * GRP])
        q_ref[:, 0:HEAD_DIM] = rope(y[:, 0:HEAD_DIM])
        q_ref[:, HEAD_DIM:PAIR] = rope(y[:, HEAD_DIM:PAIR])
        k_ref[...] = rope(y[:, PAIR:OWN])
        v_ref[...] = y[:, OWN:GRP].astype(jnp.bfloat16)


def qkv_call(sp_arr, xa, xb, first, gain, w_own, cos, sin, prev):
    place = lambda width: pl.BlockSpec((BLK, width), lambda i, s: ((s[0] ^ (first + i // 2)) * 2 + i % 2, 0))
    local = lambda width: pl.BlockSpec((BLK, width), lambda i, s: (first * 2 + i, 0))
    out = lambda width: jax.ShapeDtypeStruct((SEQ, width), jnp.bfloat16)
    xa_spec = pl.BlockSpec((BLK, DIM), lambda i, s: (jnp.minimum(i, 1), 0))
    xb_spec = pl.BlockSpec((BLK, DIM), lambda i, s: (jnp.maximum(i - 2, 0), 0))
    widths = (DIM, PAIR, HEAD_DIM, HEAD_DIM, PAIR, HEAD_DIM, HEAD_DIM)
    return pl.pallas_call(
        qkv_kernel,
        grid_spec=pltpu.PrefetchScalarGridSpec(
            num_scalar_prefetch=1,
            grid=(4,),
            in_specs=[xa_spec, xb_spec, fixed((1, DIM)), fixed((DIM, DIM)), local(HEAD_DIM), local(HEAD_DIM)]
            + [pl.BlockSpec(memory_space=pl.ANY)] * len(prev),
            out_specs=[local(DIM)] + [place(w) for w in widths[1:]],
            scratch_shapes=[pltpu.VMEM((BLK, DIM), jnp.bfloat16)],
        ),
        out_shape=[out(w) for w in widths],
        input_output_aliases={7 + n: n for n in range(len(prev))},
        compiler_params=params(),
        cost_estimate=cost(2 * 2048 * DIM * DIM, 20),
        name='qkv',
    )(sp_arr, xa, xb, gain, w_own, cos, sin, *prev)


def fwd_kernel(q_ref, k_ref, v_ref, o_ref, lse_ref, acc_ref, q_scr):
    i = pl.program_id(0)
    for h in range(PAIRS):
        q_scr[h * BLK:(h + 1) * BLK, :] = q_ref[:, h * HEAD_DIM:(h + 1) * HEAD_DIM]

    chunks = [(h, n) for h in range(PAIRS) for n in range(BLK // QSUB)]

    def step(j, carry, masked):
        start = pl.multiple_of(j * BLK, BLK)
        k = k_ref[pl.ds(start, BLK), :]
        v = v_ref[pl.ds(start, BLK), :]

        def scores(c):
            h, n = chunks[c]
            s = dot_nt(k, q_scr[h * BLK + n * QSUB:h * BLK + (n + 1) * QSUB, :])
            if masked:
                kv_idx = lax.broadcasted_iota(jnp.int32, (BLK, QSUB), 0)
                q_idx = lax.broadcasted_iota(jnp.int32, (BLK, QSUB), 1) + n * QSUB
                s = jnp.where(q_idx >= kv_idx, s, NEG)
            return s

        out = []
        s_next = scores(0)
        for c in range(len(chunks)):
            s = s_next
            if c + 1 < len(chunks):
                s_next = scores(c + 1)
            m, l = carry[c]
            m_new = jnp.maximum(m, jnp.max(s, axis=0, keepdims=True))
            p = jnp.exp2(s * SCALE2 - m_new * SCALE2)
            alpha = jnp.exp2((m - m_new) * SCALE2)
            l_new = alpha * l + jnp.sum(p, axis=0, keepdims=True)
            acc_ref[c] = acc_ref[c] * alpha + dot_tn(v, p.astype(jnp.bfloat16))
            out.append((m_new, l_new))
        return tuple(out)

    acc_ref[...] = jnp.zeros_like(acc_ref)
    init = tuple((jnp.full((1, QSUB), NEG, jnp.float32), jnp.zeros((1, QSUB), jnp.float32)) for _ in chunks)
    carry = lax.fori_loop(0, i, lambda j, c: step(j, c, False), init)
    carry = step(i, carry, True)
    for c, (h, n) in enumerate(chunks):
        m, l = carry[c]
        rows = slice(n * QSUB, (n + 1) * QSUB)
        o_ref[0, rows, h * HEAD_DIM:(h + 1) * HEAD_DIM] = (acc_ref[c] / l).T.astype(jnp.bfloat16)
        lse_ref[h, :, rows] = jnp.broadcast_to(m * SCALE2 + jnp.log2(l), (8, QSUB))


def fwd_call(q, k, v):
    whole = fixed((SEQ, HEAD_DIM))
    per = TOK // BLK
    return pl.pallas_call(
        fwd_kernel,
        grid=(SEQ // BLK,),
        in_specs=[pl.BlockSpec((BLK, PAIR), lambda i: (i, 0)), whole, whole],
        out_specs=[pl.BlockSpec((1, BLK, PAIR), lambda i: (i // per, i % per, 0)), pl.BlockSpec((2, 8, BLK), lambda i: (0, 0, i))],
        out_shape=[jax.ShapeDtypeStruct((SEQ // TOK, TOK, PAIR), jnp.bfloat16), jax.ShapeDtypeStruct((2, 8, SEQ), jnp.float32)],
        scratch_shapes=[pltpu.VMEM((2 * BLK // QSUB, HEAD_DIM, QSUB), jnp.float32), pltpu.VMEM((2 * BLK, HEAD_DIM), jnp.bfloat16)],
        compiler_params=params(),
        cost_estimate=cost(24 * 10 ** 9, 8),
        name='attn_fwd',
    )(q, k, v)


def bwd_kernel(sp_ref, q_ref, k_ref, v_ref, o_ref, do_ref, lse_ref, cos_ref, sin_ref, out0_ref, out1_ref, out2_ref, out3_ref, dq_acc, dk_acc, dv_acc, delta):
    j = pl.program_id(0)
    n_blk = SEQ // BLK

    @pl.when(j == 0)
    def _():
        dq_acc[...] = jnp.zeros_like(dq_acc)

        def rows(i, _):
            start = pl.multiple_of(i * BLK, BLK)
            prod = o_ref[pl.ds(start, BLK), :].astype(jnp.float32) * do_ref[pl.ds(start, BLK), :].astype(jnp.float32)
            for h in range(PAIRS):
                tot = jnp.sum(prod[:, h * HEAD_DIM:(h + 1) * HEAD_DIM], axis=1, keepdims=True)
                delta[h, :, pl.ds(start, BLK)] = jnp.broadcast_to(tot, (BLK, HEAD_DIM)).T[0:8, :]
            return 0

        lax.fori_loop(0, n_blk, rows, 0)

    k = k_ref[...]
    v = v_ref[...]
    dk_acc[...] = jnp.zeros_like(dk_acc)
    dv_acc[...] = jnp.zeros_like(dv_acc)

    def step(i, masked):
        start = pl.multiple_of(i * BLK, BLK)
        rows = pl.ds(start, BLK)
        for h in range(PAIRS):
            cols = slice(h * HEAD_DIM, (h + 1) * HEAD_DIM)
            q = q_ref[rows, cols]
            do = do_ref[rows, cols]
            s = dot_nt(k, q)
            p = jnp.exp2(s * SCALE2 - lse_ref[h, 0:1, rows])
            if masked:
                kv_idx = lax.broadcasted_iota(jnp.int32, (BLK, BLK), 0)
                q_idx = lax.broadcasted_iota(jnp.int32, (BLK, BLK), 1)
                p = jnp.where(q_idx >= kv_idx, p, 0.0)
            dp = dot_nt(v, do)
            dv_acc[...] += dot_nn(p.astype(jnp.bfloat16), do)
            ds = (p * (dp - delta[h, 0:1, rows]) * ATTN_SCALE).astype(jnp.bfloat16)
            dk_acc[...] += dot_nn(ds, q)
            dq_acc[rows, cols] += dot_tn(ds, k)

    step(j, True)

    def body(i, _):
        step(i, False)
        return 0

    lax.fori_loop(j + 1, n_blk, body, 0)

    cos, sin = cos_ref[...], sin_ref[...]

    def rope_back(t):
        t = t.astype(jnp.bfloat16).astype(jnp.float32)
        return (t * cos - pltpu.roll(t, 64, 1) * sin).astype(jnp.bfloat16)

    mine = pl.ds(pl.multiple_of(j * BLK, BLK), BLK)
    result = jnp.concatenate(
        [rope_back(dq_acc[mine, h * HEAD_DIM:(h + 1) * HEAD_DIM]) for h in range(PAIRS)] + [rope_back(dk_acc[...]), dv_acc[...].astype(jnp.bfloat16)], axis=1)
    for n, ref in enumerate((out0_ref, out1_ref, out2_ref, out3_ref)):
        @pl.when((j * BLK // TOK) ^ sp_ref[0] == n)
        def _(ref=ref):
            ref[...] = result


def bwd_call(sp_arr, q, k, v, o, do, lse, cos, sin):
    whole = lambda width: fixed((SEQ, width))
    block = pl.BlockSpec((BLK, HEAD_DIM), lambda j, s: (j, 0))
    per = TOK // BLK
    table = pl.BlockSpec((BLK, HEAD_DIM), lambda j, s: (((j // per) ^ s[0]) * per + j % per, 0))
    piece = lambda n: pl.BlockSpec((BLK, GRP), lambda j, s: (jnp.clip(j - per * (s[0] ^ n), 0, per - 1), 0))
    return pl.pallas_call(
        bwd_kernel,
        grid_spec=pltpu.PrefetchScalarGridSpec(
            num_scalar_prefetch=1,
            grid=(SEQ // BLK,),
            in_specs=[whole(PAIR), block, block, whole(PAIR), whole(PAIR), fixed((2, 8, SEQ)), table, table],
            out_specs=[piece(n) for n in range(SP)],
            scratch_shapes=[
                pltpu.VMEM((SEQ, PAIR), jnp.float32),
                pltpu.VMEM((BLK, HEAD_DIM), jnp.float32),
                pltpu.VMEM((BLK, HEAD_DIM), jnp.float32),
                pltpu.VMEM((2, 8, SEQ), jnp.float32),
            ],
        ),
        out_shape=[jax.ShapeDtypeStruct((TOK, GRP), jnp.bfloat16)] * 4,
        compiler_params=params(),
        cost_estimate=cost(60 * 10 ** 9, 16),
        name='attn_bwd',
    )(sp_arr, q, k, v, o, do, lse, cos, sin)


def oproj_kernel(a0_ref, a1_ref, w_ref, x_ref, g_ref, h_ref, u_ref):
    total = x_ref[...].astype(jnp.float32)
    for g, a_ref in enumerate((a0_ref, a1_ref)):
        a = jnp.concatenate([a_ref[s] for s in range(SP)], axis=1)
        total += dot_nn(a, w_ref[g * DIM:(g + 1) * DIM, :])
    h = total.astype(jnp.bfloat16)
    h_ref[...] = h
    h32 = h.astype(jnp.float32)
    inv_rms = lax.rsqrt(jnp.mean(h32 * h32, axis=-1, keepdims=True) + NORM_EPS)
    u_ref[...] = (h32 * inv_rms * g_ref[...].astype(jnp.float32)).astype(jnp.bfloat16)


def oproj_call(a0, a1, wo, x, gain):
    blk = PAIR
    row = pl.BlockSpec((blk, DIM), lambda i: (i, 0))
    part = pl.BlockSpec((4, blk, PAIR), lambda i: (0, i, 0))
    return pl.pallas_call(
        oproj_kernel,
        grid=(TOK // blk,),
        in_specs=[part, part, fixed((2048, DIM)), row, fixed((1, DIM))],
        out_specs=[row, row],
        out_shape=[jax.ShapeDtypeStruct((TOK, DIM), jnp.bfloat16)] * 2,
        compiler_params=params(),
        cost_estimate=cost(2 * TOK * DIM * 2048, 14),
        name='oproj',
    )(a0, a1, wo, x, gain)


def mlp_kernel(u_ref, dy_ref, w1_ref, w3_ref, w2_ref, z_ref, da_ref, dc_ref, y_ref, d_ref):
    u, dy = u_ref[...], dy_ref[...]
    for n in range(HALF // GRP):
        cols = slice(n * GRP, (n + 1) * GRP)
        gate = dot_nn(u, w1_ref[:, cols])
        up = dot_nn(u, w3_ref[:, cols])
        e = dot_nt(dy, w2_ref[cols, :])
        sig = 1.0 / (1.0 + jnp.exp(-gate))
        silu = gate * sig
        z_ref[:, cols] = (silu * up).astype(jnp.bfloat16)
        da_ref[:, cols] = (e * up * sig * (1.0 + gate * (1.0 - sig))).astype(jnp.bfloat16)
        dc_ref[:, cols] = (e * silu).astype(jnp.bfloat16)
    d_ref[...] = dot_nt(da_ref[...], w1_ref[...]) + dot_nt(dc_ref[...], w3_ref[...])
    y_ref[...] = dot_nn(z_ref[...], w2_ref[...])


def mlp_call(u, dy, w1, w3, w2):
    blk = PAIR
    row = lambda width: pl.BlockSpec((blk, width), lambda i: (i, 0))
    return pl.pallas_call(
        mlp_kernel,
        grid=(TOK // blk,),
        in_specs=[row(DIM), row(DIM), fixed((DIM, HALF)), fixed((DIM, HALF)), fixed((HALF, DIM))],
        out_specs=[row(HALF), row(HALF), row(HALF), row(DIM), row(DIM)],
        out_shape=[jax.ShapeDtypeStruct((TOK, HALF), jnp.bfloat16)] * 3 + [jax.ShapeDtypeStruct((TOK, DIM), jnp.float32)] * 2,
        compiler_params=params(),
        cost_estimate=cost(12 * TOK * DIM * HALF, 30),
        name='mlp',
    )(u, dy, w1, w3, w2)


def dw_kernel(la_ref, lb_ref, *refs):
    rights, out_ref = refs[:-1], refs[-1]
    for n in range(len(rights) // 2):
        ra_ref, rb_ref = rights[2 * n], rights[2 * n + 1]
        cols = ra_ref.shape[1]
        out_ref[:, n * cols:(n + 1) * cols] = dot_tn(la_ref[...], ra_ref[...]) + dot_tn(lb_ref[...], rb_ref[...])


def dw_call(la, lb, *rights):
    rows, cols = la.shape[1] // 4, rights[0].shape[1]
    total = cols * len(rights) // 2
    left = pl.BlockSpec((TOK, rows), lambda b: (0, b))
    right = fixed((TOK, cols))
    return pl.pallas_call(
        dw_kernel,
        grid=(4,),
        in_specs=[left, left] + [right] * len(rights),
        out_specs=pl.BlockSpec((rows, total), lambda b: (b, 0)),
        out_shape=jax.ShapeDtypeStruct((4 * rows, total), jnp.float32),
        compiler_params=params(),
        cost_estimate=cost(4 * TOK * rows * 4 * total, 20),
        name='dw',
    )(la, lb, *rights)


def dw_split_kernel(idx_ref, la_ref, lb_ref, ra_ref, rb_ref, send_ref, keep_ref):
    b = pl.program_id(0)
    total = dot_tn(la_ref[...], ra_ref[...]) + dot_tn(lb_ref[...], rb_ref[...])
    for n, ref in enumerate((send_ref, keep_ref)):
        @pl.when(b // PAIRS == n)
        def _(ref=ref):
            ref[0] = total


def dw_split_call(idx, la, lb, ra, rb):
    rows, cols = la.shape[1] // SP, ra.shape[1]
    left = pl.BlockSpec((TOK, rows), lambda b, s: (0, s[b]))
    right = fixed((TOK, cols))
    out = lambda n: pl.BlockSpec((1, rows, cols), lambda b, s: (jnp.clip(b - PAIRS * n, 0, 1), 0, 0))
    return pl.pallas_call(
        dw_split_kernel,
        grid_spec=pltpu.PrefetchScalarGridSpec(
            num_scalar_prefetch=1, grid=(SP,), in_specs=[left, left, right, right], out_specs=[out(0), out(1)]),
        out_shape=[jax.ShapeDtypeStruct((PAIRS, rows, cols), jnp.float32)] * PAIRS,
        compiler_params=params(),
        cost_estimate=cost(SP * TOK * rows * SP * cols, 20),
        name='dw_split',
    )(idx, la, lb, ra, rb)


def dw_qkv_kernel(u_ref, *refs):
    out_ref = refs[-1]
    total = dot_tn(u_ref[0:TOK, :], refs[0][...])
    for n in range(1, 4):
        total += dot_tn(u_ref[n * TOK:(n + 1) * TOK, :], refs[n][...])
    out_ref[...] = total


def dw_qkv_call(u, pieces):
    return pl.pallas_call(
        dw_qkv_kernel,
        grid=(4,),
        in_specs=[pl.BlockSpec((SEQ, PAIR), lambda b: (0, b))] + [fixed((TOK, GRP))] * 4,
        out_specs=pl.BlockSpec((PAIR, GRP), lambda b: (b, 0)),
        out_shape=jax.ShapeDtypeStruct((DIM, GRP), jnp.float32),
        compiler_params=params(),
        cost_estimate=cost(2 * SEQ * DIM * GRP, 14),
        name='dw_qkv',
    )(u, *pieces)


def dout_kernel(sp_ref, h0_ref, h1_ref, h2_ref, h3_ref, o0_ref, o1_ref, wa_ref, wb_ref, d0_ref, d1_ref, dwo_ref, scr):
    i = pl.program_id(0)
    for n, ref in enumerate((h0_ref, h1_ref, h2_ref, h3_ref)):
        @pl.when(i // 2 == n)
        def _(ref=ref):
            scr[...] = ref[...]
    dh = scr[...]
    d0_ref[...] = dot_nt(dh, wa_ref[...]).astype(jnp.bfloat16)
    d1_ref[...] = dot_nt(dh, wb_ref[...]).astype(jnp.bfloat16)

    @pl.when(i == 0)
    def _():
        dwo_ref[...] = jnp.zeros_like(dwo_ref)

    dwo_ref[0] += dot_tn(o0_ref[0], dh)
    dwo_ref[1] += dot_tn(o1_ref[0], dh)


def dout_call(sp_arr, dhs, o0, o1, wo):
    src = lambda n: pl.BlockSpec((BLK, DIM), lambda i, s: (jnp.clip(i - 2 * n, 0, 1), 0))
    o_spec = pl.BlockSpec((1, BLK, PAIR), lambda i, s: (s[0] ^ (i // 2), i % 2, 0))
    d_spec = pl.BlockSpec((BLK, PAIR), lambda i, s: ((s[0] ^ (i // 2)) * 2 + i % 2, 0))
    out = jax.ShapeDtypeStruct((SEQ, PAIR), jnp.bfloat16)
    return pl.pallas_call(
        dout_kernel,
        grid_spec=pltpu.PrefetchScalarGridSpec(
            num_scalar_prefetch=1,
            grid=(SEQ // BLK,),
            in_specs=[src(0), src(1), src(2), src(3), o_spec, o_spec,
                      pl.BlockSpec((PAIR, DIM), lambda i, s: (s[0], 0)), pl.BlockSpec((PAIR, DIM), lambda i, s: (4 + s[0], 0))],
            out_specs=[d_spec, d_spec, fixed((2, PAIR, DIM))],
            scratch_shapes=[pltpu.VMEM((BLK, DIM), jnp.bfloat16)],
        ),
        out_shape=[out, out, jax.ShapeDtypeStruct((2, PAIR, DIM), jnp.float32)],
        compiler_params=params(),
        cost_estimate=cost(4 * SEQ * DIM * GRP, 20),
        name='dout',
    )(sp_arr, *dhs, o0, o1, wo, wo)


def du_sum(sp_ref, pieces, w_ref):
    total = 0.0
    for n, piece in enumerate(pieces):
        cols = pl.ds(pl.multiple_of((sp_ref[0] ^ n) * GRP, GRP), GRP)
        total += dot_nt(piece[...], w_ref[:, cols])
    return total


def du_kernel(sp_ref, *refs):
    refs[-1][...] = du_sum(sp_ref, refs[:SP], refs[SP])


def dx_kernel(sp_ref, *refs):
    w_ref, du_ref, x_ref, dr_ref, g_ref, dx_ref, dg_ref = refs[SP:]
    d_u = du_ref[...] + du_sum(sp_ref, refs[:SP], w_ref)
    x32 = x_ref[...].astype(jnp.float32)
    inv_rms = lax.rsqrt(jnp.mean(x32 * x32, axis=-1, keepdims=True) + NORM_EPS)
    normed = x32 * inv_rms
    d_normed = d_u * g_ref[...].astype(jnp.float32)
    grad_in = inv_rms * (d_normed - normed * jnp.mean(d_normed * normed, axis=-1, keepdims=True))
    dx_ref[...] = (dr_ref[...] + grad_in).astype(jnp.bfloat16)

    @pl.when(pl.program_id(0) == 0)
    def _():
        dg_ref[...] = jnp.zeros_like(dg_ref)

    dg_ref[...] += jnp.sum(d_u * normed, axis=0, keepdims=True)


def dx_call(sp_arr, group, pieces, w_all, *rest):
    row = lambda width: pl.BlockSpec((PAIR, width), lambda i, s: (i, 0))
    one = fixed((1, DIM))
    du_shape = jax.ShapeDtypeStruct((TOK, DIM), jnp.float32)
    last = len(rest) > 0
    return pl.pallas_call(
        dx_kernel if last else du_kernel,
        grid_spec=pltpu.PrefetchScalarGridSpec(
            num_scalar_prefetch=1,
            grid=(TOK // PAIR,),
            in_specs=[row(GRP)] * SP + [pl.BlockSpec((DIM, SP * GRP), lambda i, s: (0, group))] + ([row(DIM)] * 3 + [one] if last else []),
            out_specs=[row(DIM), one] if last else row(DIM),
        ),
        out_shape=[jax.ShapeDtypeStruct((TOK, DIM), jnp.bfloat16), jax.ShapeDtypeStruct((1, DIM), jnp.float32)] if last else du_shape,
        compiler_params=params(),
        cost_estimate=cost(SP * TOK * DIM * DIM, 16),
        name='dx' if last else 'du',
    )(sp_arr, *pieces, w_all, *rest)


def gather_full(shard):
    return lax.all_gather(shard, ALL_AXES, axis=0, tiled=True)


def gather_core(shard):
    return lax.all_gather(shard, ALL_AXES, axis=0, tiled=True, axis_index_groups=CORE_GROUPS)


def swap_seq(parts):
    return lax.all_to_all(parts, 'sp', 0, 0, tiled=True)


def swap_all(parts):
    return lax.all_to_all(parts, ALL_AXES, 0, 0, tiled=True)


def from_sp(value, bits):
    return lax.ppermute(value, 'sp', [(s, s ^ bits) for s in range(SP)])


def from_dp(value):
    return lax.ppermute(value, 'dp', [(0, 1), (1, 0)])


def gather_chip_then_core(value):
    far = from_sp(value, 2)
    return value, from_sp(value, 1), far, from_sp(far, 1)


def reduce_chips(part):
    return lax.psum_scatter(part, ALL_AXES, scatter_dimension=0, tiled=True, axis_index_groups=CORE_GROUPS)


def layer_step(hidden, positions, grad_out, gain_attn, gain_mlp, w_query, w_key, w_value, w_out, w_gate, w_up, w_down):
    tokens = hidden[0]
    d_layer = grad_out[0]
    dp = lax.axis_index('dp')
    sp = lax.axis_index('sp')
    core = sp % 2
    f32, bf16 = jnp.float32, jnp.bfloat16
    sp_arr, dp_arr, core_arr = (t.astype(jnp.int32)[None] for t in (sp, dp, core))

    xs = gather_chip_then_core(tokens)
    w_cols, w_send, a1, b1, a3, b3 = pack_call(core_arr, w_query, w_key, w_value, w_gate, w_up, gain_attn[None], gain_mlp[None])
    w_mine = swap_seq(w_send)
    w_own, gain1, gain2 = join_qkv_call(dp_arr, w_mine, from_dp(w_mine))
    gain1, gain2 = gain1[0:1], gain2[0:1]
    pos = gather_chip_then_core(positions[0].reshape(8, HEAD_DIM))
    pos_all = jnp.concatenate(pos).reshape(SEQ)
    w1_rows, w3_rows = join_call(core_arr, (a1, from_sp(b1, 1)), (a3, from_sp(b3, 1)))
    wo_full = gather_full(w_out)
    w2 = gather_core(w_down)
    w1, w3 = gather_core(w1_rows), gather_core(w3_rows)
    w_all = gather_full(w_cols)
    dy_pair = from_sp(d_layer, 1)

    lane = jnp.arange(HEAD_DIM)
    half = HEAD_DIM // 2
    inv_freq = ROPE_BASE ** (-((lane % half).astype(f32) * (2.0 / HEAD_DIM)))
    angles = pos_all.astype(f32)[:, None] * inv_freq
    cos = jnp.cos(angles)
    sin = jnp.sin(angles) * jnp.where(lane < half, -1.0, 1.0)

    near = qkv_call(sp_arr, xs[0], xs[1], 0, gain1, w_own, cos, sin, ())
    u_all, q0, k0, v0, q1, k1, v1 = qkv_call(sp_arr, xs[2], xs[3], 2, gain1, w_own, cos, sin, near)
    o0, lse0 = fwd_call(q0, k0, v0)
    got0 = swap_seq(o0)
    o1, lse1 = fwd_call(q1, k1, v1)
    got1 = swap_seq(o1)
    residual, u_mlp = oproj_call(got0, got1, wo_full, tokens, gain2)

    u_pair = from_sp(u_mlp, 1)
    z_a, da_a, dc_a, y_a, d_a = mlp_call(u_mlp, d_layer, w1, w3, w2)
    z_b, da_b, dc_b, y_b, d_b = mlp_call(u_pair, dy_pair, w1, w3, w2)
    d_umlp = d_a + from_sp(d_b, 1)
    h32 = residual.astype(f32)
    layer_out = (h32 + (y_a + from_sp(y_b, 1))).astype(bf16)
    inv_rms2 = lax.rsqrt(jnp.mean(h32 * h32, axis=-1, keepdims=True) + NORM_EPS)
    normed2 = h32 * inv_rms2
    d_normed2 = d_umlp * gain2.astype(f32)
    d_gain2 = jnp.sum(d_umlp * normed2, axis=0)
    d_resid = d_layer.astype(f32) + inv_rms2 * (d_normed2 - normed2 * jnp.mean(d_normed2 * normed2, axis=-1, keepdims=True))
    dhs = gather_chip_then_core(d_resid.astype(bf16))
    chip = dp * PAIRS + sp // PAIRS
    order = jnp.stack([chip ^ 3, chip ^ 2, chip ^ 1, chip]).astype(jnp.int32)
    down_send, down_keep = dw_split_call(order, z_a, z_b, d_layer, dy_pair)
    down_got = from_dp(down_send)

    part = reduce_chips(dw_call(u_mlp, u_pair, da_a, da_b, dc_a, dc_b))

    do0, do1, dwo = dout_call(sp_arr, dhs, o0, o1, wo_full)
    down_far, down_near = down_keep[0] + down_got[0], down_keep[1] + down_got[1]
    down_last = from_sp(down_far, 2)
    o_seq = (o0.reshape(SEQ, PAIR), o1.reshape(SEQ, PAIR))
    d0 = bwd_call(sp_arr, q0, k0, v0, o_seq[0], do0, lse0, cos, sin)
    back0 = [d0[0]] + [from_sp(d0[n], n) for n in (1, 2, 3)]
    part0 = dw_qkv_call(u_all, d0).reshape(8, HEAD_DIM, GRP)
    dw0 = swap_all(part0)
    d1 = bwd_call(sp_arr, q1, k1, v1, o_seq[1], do1, lse1, cos, sin)
    back1 = [d1[0]] + [from_sp(d1[n], n) for n in (1, 2, 3)]
    part1 = dw_qkv_call(u_all, d1).reshape(8, HEAD_DIM, GRP)
    part1, _ = lax.optimization_barrier((part1, dw0))
    dw1 = swap_all(part1)
    grad_w_out = lax.dynamic_index_in_dim(dwo, dp, 0, keepdims=False) + from_dp(lax.dynamic_index_in_dim(dwo, 1 - dp, 0, keepdims=False))
    part, _ = lax.optimization_barrier((part, part1))
    send = lax.dynamic_slice(part, ((1 - core) * HEAD_DIM, 0), (HEAD_DIM, 2 * HALF))
    grad_w_gate, grad_w_up = unpack_cols_call(core_arr, part, from_sp(send, 1))
    grad_w_down = down_near + down_last
    du0 = dx_call(sp_arr, 0, back0, w_all)
    grad_hidden, d_gain1 = dx_call(sp_arr, 1, back1, w_all, du0, tokens, d_resid, gain1)
    grad_w_query, grad_w_key, grad_w_value = unpack_qkv_call(dw0, dw1)
    gain_parts = jnp.stack([d_gain1.reshape(8, HEAD_DIM), d_gain2.reshape(8, HEAD_DIM)], axis=1)
    gain_parts, _ = lax.optimization_barrier((gain_parts, dw1))
    gain_sums = jnp.sum(swap_all(gain_parts), axis=0)
    return (layer_out[None], grad_hidden[None], gain_sums[0], gain_sums[1], grad_w_query, grad_w_key, grad_w_value,
            grad_w_out, grad_w_gate, grad_w_up, grad_w_down)


def solution(mesh):
    act_spec = P('dp', 'sp', None)
    pos_spec = P('dp', 'sp')
    vec_spec = P(ALL_AXES)
    mat_spec = P(ALL_AXES, None)
    in_specs = (act_spec, pos_spec, act_spec, vec_spec, vec_spec) + (mat_spec,) * 7
    out_specs = (act_spec, act_spec, vec_spec, vec_spec) + (mat_spec,) * 7

    return jax.shard_map(layer_step, mesh=mesh, in_specs=in_specs, out_specs=out_specs, check_vma=False)
```

```python
import math

import jax
import jax.numpy as jnp
from jax import lax
from jax.experimental import pallas as pl
from jax.experimental.pallas import tpu as pltpu
from jax.sharding import PartitionSpec as P


HEAD_DIM = 128
ROPE_BASE = 10000.0
NORM_EPS = 1e-5
ATTN_SCALE = HEAD_DIM ** -0.5
LOG2E = math.log2(math.e)
SCALE2 = ATTN_SCALE * LOG2E
ALL_AXES = ('dp', 'sp')
BLK = 512
QSUB = 256
SEQ = 4096
TOK = 1024
DIM = 1024
HALF = 1536
SEND = 144
CORE_GROUPS = [[0, 2, 4, 6], [1, 3, 5, 7]]
PAIR = 256
TINY = 10 ** 8
SP = 4
PAIRS = 2
GRP = 512
OWN = 384
NEG = -1e30
VMEM_LIMIT = 60 * 1024 * 1024


def dot_nt(left, right):
    return lax.dot_general(left, right, (((1,), (1,)), ((), ())), preferred_element_type=jnp.float32)


def dot_nn(left, right):
    return lax.dot_general(left, right, (((1,), (0,)), ((), ())), preferred_element_type=jnp.float32)


def dot_tn(left, right):
    return lax.dot_general(left, right, (((0,), (0,)), ((), ())), preferred_element_type=jnp.float32)


def fixed(shape):
    return pl.BlockSpec(shape, lambda *_: tuple(0 for _ in shape))


def params(**kw):
    return pltpu.CompilerParams(vmem_limit_bytes=VMEM_LIMIT, dimension_semantics=('arbitrary',), **kw)


def cost(flops, mib):
    return pl.CostEstimate(flops=flops, bytes_accessed=mib << 20, transcendentals=0)


def pack_kernel(core_ref, wq_ref, wk_ref, wv_ref, w1_ref, w3_ref, g1_ref, g2_ref, all_ref, send_ref, a1_ref, b1_ref, a3_ref, b3_ref):
    for g in range(PAIRS):
        for n in range(SP):
            m = g * 4 + n
            piece = jnp.concatenate([wq_ref[:, m * PAIR:(m + 1) * PAIR], wk_ref[:, m * HEAD_DIM:(m + 1) * HEAD_DIM], wv_ref[:, m * HEAD_DIM:(m + 1) * HEAD_DIM]], axis=1)
            all_ref[:, m * GRP:(m + 1) * GRP] = piece
            send_ref[n * SEND:n * SEND + HEAD_DIM, g * GRP:(g + 1) * GRP] = piece
    tail = jnp.concatenate([g1_ref[...], g2_ref[...], jnp.zeros((1, DIM - PAIR), jnp.bfloat16)], axis=1)
    for n in range(SP):
        send_ref[n * SEND + HEAD_DIM:(n + 1) * SEND, :] = jnp.broadcast_to(tail, (SEND - HEAD_DIM, DIM))
    core = core_ref[0]
    for ref, own_ref, other_ref in ((w1_ref, a1_ref, b1_ref), (w3_ref, a3_ref, b3_ref)):
        for n in range(SP):
            cols = slice(n * OWN, (n + 1) * OWN)
            own_ref[:, cols] = ref[:, pl.ds(pl.multiple_of((n * 2 + core) * OWN, HEAD_DIM), OWN)]
            other_ref[:, cols] = ref[:, pl.ds(pl.multiple_of((n * 2 + 1 - core) * OWN, HEAD_DIM), OWN)]


def pack_call(core_arr, *weights):
    out = lambda *shape: jax.ShapeDtypeStruct(shape, jnp.bfloat16)
    return pl.pallas_call(
        pack_kernel,
        in_specs=[pl.BlockSpec(memory_space=pltpu.SMEM)] + [pl.BlockSpec(memory_space=pltpu.VMEM)] * 7,
        out_shape=[out(HEAD_DIM, SEQ), out(4 * SEND, DIM)] + [out(HEAD_DIM, HALF)] * 4,
        cost_estimate=cost(TINY, 6),
        name='pack',
    )(core_arr, *weights)


def join_kernel(pos_ref, *refs):
    count = len(refs) // 3
    for n in range(count):
        own_ref, got_ref, out_ref = refs[2 * n], refs[2 * n + 1], refs[2 * count + n]
        rows = own_ref.shape[0]
        out_ref[pl.ds(pl.multiple_of(pos_ref[0] * rows, HEAD_DIM), rows), :] = own_ref[...]
        out_ref[pl.ds(pl.multiple_of((1 - pos_ref[0]) * rows, HEAD_DIM), rows), :] = got_ref[...]


def join_call(pos_arr, *pairs):
    flat = [t for pair in pairs for t in pair]
    return pl.pallas_call(
        join_kernel,
        in_specs=[pl.BlockSpec(memory_space=pltpu.SMEM)] + [pl.BlockSpec(memory_space=pltpu.VMEM)] * len(flat),
        out_shape=[jax.ShapeDtypeStruct((2 * a.shape[0], a.shape[1]), a.dtype) for a, _ in pairs],
        cost_estimate=cost(TINY, 4),
        name='join',
    )(pos_arr, *flat)


def join_qkv_kernel(dp_ref, own_ref, got_ref, w_ref, g1_ref, g2_ref):
    for ref, part in ((own_ref, dp_ref[0]), (got_ref, 1 - dp_ref[0])):
        for n in range(SP):
            rows = pl.ds(pl.multiple_of((part * 4 + n) * HEAD_DIM, HEAD_DIM), HEAD_DIM)
            w_ref[rows, :] = ref[n * SEND:n * SEND + HEAD_DIM, :]
            tail = ref[n * SEND + HEAD_DIM:(n + 1) * SEND, 0:PAIR]
            g1_ref[:, rows] = tail[:, 0:HEAD_DIM]
            g2_ref[:, rows] = tail[:, HEAD_DIM:PAIR]


def join_qkv_call(dp_arr, own, got):
    out = lambda rows: jax.ShapeDtypeStruct((rows, DIM), jnp.bfloat16)
    return pl.pallas_call(
        join_qkv_kernel,
        in_specs=[pl.BlockSpec(memory_space=pltpu.SMEM)] + [pl.BlockSpec(memory_space=pltpu.VMEM)] * 2,
        out_shape=[out(DIM), out(SEND - HEAD_DIM), out(SEND - HEAD_DIM)],
        cost_estimate=cost(TINY, 4),
        name='join_qkv',
    )(dp_arr, own, got)


def unpack_qkv_kernel(p0_ref, p1_ref, wq_ref, wk_ref, wv_ref):
    for g, ref in enumerate((p0_ref, p1_ref)):
        for n in range(SP):
            m = g * 4 + n
            total = ref[n] + ref[4 + n]
            wq_ref[:, m * PAIR:(m + 1) * PAIR] = total[:, 0:PAIR]
            wk_ref[:, m * HEAD_DIM:(m + 1) * HEAD_DIM] = total[:, PAIR:OWN]
            wv_ref[:, m * HEAD_DIM:(m + 1) * HEAD_DIM] = total[:, OWN:GRP]


def unpack_qkv_call(p0, p1):
    out = lambda cols: jax.ShapeDtypeStruct((HEAD_DIM, cols), jnp.float32)
    return pl.pallas_call(unpack_qkv_kernel, out_shape=[out(2048), out(DIM), out(DIM)], cost_estimate=cost(TINY, 6), name='unpack_qkv')(p0, p1)


def unpack_cols_kernel(core_ref, own_ref, got_ref, gate_ref, up_ref):
    core = core_ref[0]
    mine = own_ref[pl.ds(pl.multiple_of(core * HEAD_DIM, HEAD_DIM), HEAD_DIM), :]
    for w, ref in enumerate((gate_ref, up_ref)):
        for n in range(SP):
            cols = slice(w * HALF + n * OWN, w * HALF + (n + 1) * OWN)
            ref[:, pl.ds(pl.multiple_of((n * 2 + core) * OWN, HEAD_DIM), OWN)] = mine[:, cols]
            ref[:, pl.ds(pl.multiple_of((n * 2 + 1 - core) * OWN, HEAD_DIM), OWN)] = got_ref[:, cols]


def unpack_cols_call(core_arr, own, got):
    return pl.pallas_call(
        unpack_cols_kernel,
        in_specs=[pl.BlockSpec(memory_space=pltpu.SMEM)] + [pl.BlockSpec(memory_space=pltpu.VMEM)] * 2,
        out_shape=[jax.ShapeDtypeStruct((HEAD_DIM, 2 * HALF), jnp.float32)] * 2,
        cost_estimate=cost(TINY, 4),
        name='unpack_cols',
    )(core_arr, own, got)


def qkv_kernel(sp_ref, xa_ref, xb_ref, g_ref, w_ref, cos_ref, sin_ref, *rest):
    u_ref, q0_ref, k0_ref, v0_ref, q1_ref, k1_ref, v1_ref, x_scr = rest[-8:]
    i = pl.program_id(0)

    @pl.when(i < 2)
    def _():
        x_scr[...] = xa_ref[...]

    @pl.when(i >= 2)
    def _():
        x_scr[...] = xb_ref[...]

    x32 = x_scr[...].astype(jnp.float32)
    inv_rms = lax.rsqrt(jnp.mean(x32 * x32, axis=-1, keepdims=True) + NORM_EPS)
    u = (x32 * inv_rms * g_ref[...].astype(jnp.float32)).astype(jnp.bfloat16)
    u_ref[...] = u
    cos, sin = cos_ref[...], sin_ref[...]

    def rope(t):
        return (t * cos + pltpu.roll(t, 64, 1) * sin).astype(jnp.bfloat16)

    for g, (q_ref, k_ref, v_ref) in enumerate(((q0_ref, k0_ref, v0_ref), (q1_ref, k1_ref, v1_ref))):
        y = dot_nn(u, w_ref[:, g * GRP:(g + 1) * GRP])
        q_ref[:, 0:HEAD_DIM] = rope(y[:, 0:HEAD_DIM])
        q_ref[:, HEAD_DIM:PAIR] = rope(y[:, HEAD_DIM:PAIR])
        k_ref[...] = rope(y[:, PAIR:OWN])
        v_ref[...] = y[:, OWN:GRP].astype(jnp.bfloat16)


def qkv_call(sp_arr, xa, xb, first, gain, w_own, cos, sin, prev):
    place = lambda width: pl.BlockSpec((BLK, width), lambda i, s: ((s[0] ^ (first + i // 2)) * 2 + i % 2, 0))
    local = lambda width: pl.BlockSpec((BLK, width), lambda i, s: (first * 2 + i, 0))
    out = lambda width: jax.ShapeDtypeStruct((SEQ, width), jnp.bfloat16)
    xa_spec = pl.BlockSpec((BLK, DIM), lambda i, s: (jnp.minimum(i, 1), 0))
    xb_spec = pl.BlockSpec((BLK, DIM), lambda i, s: (jnp.maximum(i - 2, 0), 0))
    widths = (DIM, PAIR, HEAD_DIM, HEAD_DIM, PAIR, HEAD_DIM, HEAD_DIM)
    return pl.pallas_call(
        qkv_kernel,
        grid_spec=pltpu.PrefetchScalarGridSpec(
            num_scalar_prefetch=1,
            grid=(4,),
            in_specs=[xa_spec, xb_spec, fixed((1, DIM)), fixed((DIM, DIM)), local(HEAD_DIM), local(HEAD_DIM)]
            + [pl.BlockSpec(memory_space=pl.ANY)] * len(prev),
            out_specs=[local(DIM)] + [place(w) for w in widths[1:]],
            scratch_shapes=[pltpu.VMEM((BLK, DIM), jnp.bfloat16)],
        ),
        out_shape=[out(w) for w in widths],
        input_output_aliases={7 + n: n for n in range(len(prev))},
        compiler_params=params(),
        cost_estimate=cost(2 * 2048 * DIM * DIM, 20),
        name='qkv',
    )(sp_arr, xa, xb, gain, w_own, cos, sin, *prev)


def fwd_kernel(q_ref, k_ref, v_ref, o_ref, lse_ref, acc_ref, q_scr):
    i = pl.program_id(0)
    for h in range(PAIRS):
        q_scr[h * BLK:(h + 1) * BLK, :] = q_ref[:, h * HEAD_DIM:(h + 1) * HEAD_DIM]

    chunks = [(h, n) for h in range(PAIRS) for n in range(BLK // QSUB)]

    def step(j, carry, masked):
        start = pl.multiple_of(j * BLK, BLK)
        k = k_ref[pl.ds(start, BLK), :]
        v = v_ref[pl.ds(start, BLK), :]

        def scores(c):
            h, n = chunks[c]
            s = dot_nt(k, q_scr[h * BLK + n * QSUB:h * BLK + (n + 1) * QSUB, :])
            if masked:
                kv_idx = lax.broadcasted_iota(jnp.int32, (BLK, QSUB), 0)
                q_idx = lax.broadcasted_iota(jnp.int32, (BLK, QSUB), 1) + n * QSUB
                s = jnp.where(q_idx >= kv_idx, s, NEG)
            return s

        out = []
        s_next = scores(0)
        for c in range(len(chunks)):
            s = s_next
            if c + 1 < len(chunks):
                s_next = scores(c + 1)
            m, l = carry[c]
            m_new = jnp.maximum(m, jnp.max(s, axis=0, keepdims=True))
            p = jnp.exp2(s * SCALE2 - m_new * SCALE2)
            alpha = jnp.exp2((m - m_new) * SCALE2)
            l_new = alpha * l + jnp.sum(p, axis=0, keepdims=True)
            acc_ref[c] = acc_ref[c] * alpha + dot_tn(v, p.astype(jnp.bfloat16))
            out.append((m_new, l_new))
        return tuple(out)

    acc_ref[...] = jnp.zeros_like(acc_ref)
    init = tuple((jnp.full((1, QSUB), NEG, jnp.float32), jnp.zeros((1, QSUB), jnp.float32)) for _ in chunks)
    carry = lax.fori_loop(0, i, lambda j, c: step(j, c, False), init)
    carry = step(i, carry, True)
    for c, (h, n) in enumerate(chunks):
        m, l = carry[c]
        rows = slice(n * QSUB, (n + 1) * QSUB)
        o_ref[0, rows, h * HEAD_DIM:(h + 1) * HEAD_DIM] = (acc_ref[c] / l).T.astype(jnp.bfloat16)
        lse_ref[h, :, rows] = jnp.broadcast_to(m * SCALE2 + jnp.log2(l), (8, QSUB))


def fwd_call(q, k, v):
    whole = fixed((SEQ, HEAD_DIM))
    per = TOK // BLK
    return pl.pallas_call(
        fwd_kernel,
        grid=(SEQ // BLK,),
        in_specs=[pl.BlockSpec((BLK, PAIR), lambda i: (i, 0)), whole, whole],
        out_specs=[pl.BlockSpec((1, BLK, PAIR), lambda i: (i // per, i % per, 0)), pl.BlockSpec((2, 8, BLK), lambda i: (0, 0, i))],
        out_shape=[jax.ShapeDtypeStruct((SEQ // TOK, TOK, PAIR), jnp.bfloat16), jax.ShapeDtypeStruct((2, 8, SEQ), jnp.float32)],
        scratch_shapes=[pltpu.VMEM((2 * BLK // QSUB, HEAD_DIM, QSUB), jnp.float32), pltpu.VMEM((2 * BLK, HEAD_DIM), jnp.bfloat16)],
        compiler_params=params(),
        cost_estimate=cost(24 * 10 ** 9, 8),
        name='attn_fwd',
    )(q, k, v)


def bwd_kernel(sp_ref, q_ref, k_ref, v_ref, o_ref, do_ref, lse_ref, cos_ref, sin_ref, out0_ref, out1_ref, out2_ref, out3_ref, dq_acc, dk_acc, dv_acc, delta):
    j = pl.program_id(0)
    n_blk = SEQ // BLK

    @pl.when(j == 0)
    def _():
        dq_acc[...] = jnp.zeros_like(dq_acc)

        def rows(i, _):
            start = pl.multiple_of(i * BLK, BLK)
            prod = o_ref[pl.ds(start, BLK), :].astype(jnp.float32) * do_ref[pl.ds(start, BLK), :].astype(jnp.float32)
            for h in range(PAIRS):
                tot = jnp.sum(prod[:, h * HEAD_DIM:(h + 1) * HEAD_DIM], axis=1, keepdims=True)
                delta[h, :, pl.ds(start, BLK)] = jnp.broadcast_to(tot, (BLK, HEAD_DIM)).T[0:8, :]
            return 0

        lax.fori_loop(0, n_blk, rows, 0)

    k = k_ref[...]
    v = v_ref[...]
    dk_acc[...] = jnp.zeros_like(dk_acc)
    dv_acc[...] = jnp.zeros_like(dv_acc)

    def step(i, masked):
        start = pl.multiple_of(i * BLK, BLK)
        rows = pl.ds(start, BLK)
        for h in range(PAIRS):
            cols = slice(h * HEAD_DIM, (h + 1) * HEAD_DIM)
            q = q_ref[rows, cols]
            do = do_ref[rows, cols]
            s = dot_nt(k, q)
            p = jnp.exp2(s * SCALE2 - lse_ref[h, 0:1, rows])
            if masked:
                kv_idx = lax.broadcasted_iota(jnp.int32, (BLK, BLK), 0)
                q_idx = lax.broadcasted_iota(jnp.int32, (BLK, BLK), 1)
                p = jnp.where(q_idx >= kv_idx, p, 0.0)
            dp = dot_nt(v, do)
            dv_acc[...] += dot_nn(p.astype(jnp.bfloat16), do)
            ds = (p * (dp - delta[h, 0:1, rows]) * ATTN_SCALE).astype(jnp.bfloat16)
            dk_acc[...] += dot_nn(ds, q)
            dq_acc[rows, cols] += dot_tn(ds, k)

    step(j, True)

    def body(i, _):
        step(i, False)
        return 0

    lax.fori_loop(j + 1, n_blk, body, 0)

    cos, sin = cos_ref[...], sin_ref[...]

    def rope_back(t):
        t = t.astype(jnp.bfloat16).astype(jnp.float32)
        return (t * cos - pltpu.roll(t, 64, 1) * sin).astype(jnp.bfloat16)

    mine = pl.ds(pl.multiple_of(j * BLK, BLK), BLK)
    result = jnp.concatenate(
        [rope_back(dq_acc[mine, h * HEAD_DIM:(h + 1) * HEAD_DIM]) for h in range(PAIRS)] + [rope_back(dk_acc[...]), dv_acc[...].astype(jnp.bfloat16)], axis=1)
    for n, ref in enumerate((out0_ref, out1_ref, out2_ref, out3_ref)):
        @pl.when((j * BLK // TOK) ^ sp_ref[0] == n)
        def _(ref=ref):
            ref[...] = result


def bwd_call(sp_arr, q, k, v, o, do, lse, cos, sin):
    whole = lambda width: fixed((SEQ, width))
    block = pl.BlockSpec((BLK, HEAD_DIM), lambda j, s: (j, 0))
    per = TOK // BLK
    table = pl.BlockSpec((BLK, HEAD_DIM), lambda j, s: (((j // per) ^ s[0]) * per + j % per, 0))
    piece = lambda n: pl.BlockSpec((BLK, GRP), lambda j, s: (jnp.clip(j - per * (s[0] ^ n), 0, per - 1), 0))
    return pl.pallas_call(
        bwd_kernel,
        grid_spec=pltpu.PrefetchScalarGridSpec(
            num_scalar_prefetch=1,
            grid=(SEQ // BLK,),
            in_specs=[whole(PAIR), block, block, whole(PAIR), whole(PAIR), fixed((2, 8, SEQ)), table, table],
            out_specs=[piece(n) for n in range(SP)],
            scratch_shapes=[
                pltpu.VMEM((SEQ, PAIR), jnp.float32),
                pltpu.VMEM((BLK, HEAD_DIM), jnp.float32),
                pltpu.VMEM((BLK, HEAD_DIM), jnp.float32),
                pltpu.VMEM((2, 8, SEQ), jnp.float32),
            ],
        ),
        out_shape=[jax.ShapeDtypeStruct((TOK, GRP), jnp.bfloat16)] * 4,
        compiler_params=params(),
        cost_estimate=cost(60 * 10 ** 9, 16),
        name='attn_bwd',
    )(sp_arr, q, k, v, o, do, lse, cos, sin)


def oproj_kernel(a0_ref, a1_ref, w_ref, x_ref, g_ref, h_ref, u_ref):
    total = x_ref[...].astype(jnp.float32)
    for g, a_ref in enumerate((a0_ref, a1_ref)):
        a = jnp.concatenate([a_ref[s] for s in range(SP)], axis=1)
        total += dot_nn(a, w_ref[g * DIM:(g + 1) * DIM, :])
    h = total.astype(jnp.bfloat16)
    h_ref[...] = h
    h32 = h.astype(jnp.float32)
    inv_rms = lax.rsqrt(jnp.mean(h32 * h32, axis=-1, keepdims=True) + NORM_EPS)
    u_ref[...] = (h32 * inv_rms * g_ref[...].astype(jnp.float32)).astype(jnp.bfloat16)


def oproj_call(a0, a1, wo, x, gain):
    blk = PAIR
    row = pl.BlockSpec((blk, DIM), lambda i: (i, 0))
    part = pl.BlockSpec((4, blk, PAIR), lambda i: (0, i, 0))
    return pl.pallas_call(
        oproj_kernel,
        grid=(TOK // blk,),
        in_specs=[part, part, fixed((2048, DIM)), row, fixed((1, DIM))],
        out_specs=[row, row],
        out_shape=[jax.ShapeDtypeStruct((TOK, DIM), jnp.bfloat16)] * 2,
        compiler_params=params(),
        cost_estimate=cost(2 * TOK * DIM * 2048, 14),
        name='oproj',
    )(a0, a1, wo, x, gain)


def mlp_kernel(chip_ref, u_ref, dy_ref, *refs):
    z_ref, da_ref, dc_ref, y_ref, d_ref, w1_ref, w3_ref, w2_ref = refs[3 * SP:]

    @pl.when(pl.program_id(0) == 0)
    def _():
        for w, ref in enumerate((w1_ref, w3_ref, w2_ref)):
            for n in range(SP):
                piece = refs[w * SP + n]
                rows = piece.shape[0]
                ref[pl.ds(pl.multiple_of((chip_ref[0] ^ n) * rows, HEAD_DIM), rows), :] = piece[...]

    u, dy = u_ref[...], dy_ref[...]
    for n in range(HALF // GRP):
        cols = slice(n * GRP, (n + 1) * GRP)
        gate = dot_nn(u, w1_ref[:, cols])
        up = dot_nn(u, w3_ref[:, cols])
        e = dot_nt(dy, w2_ref[cols, :])
        sig = 1.0 / (1.0 + jnp.exp(-gate))
        silu = gate * sig
        z_ref[:, cols] = (silu * up).astype(jnp.bfloat16)
        da_ref[:, cols] = (e * up * sig * (1.0 + gate * (1.0 - sig))).astype(jnp.bfloat16)
        dc_ref[:, cols] = (e * silu).astype(jnp.bfloat16)
    d_ref[...] = dot_nt(da_ref[...], w1_ref[...]) + dot_nt(dc_ref[...], w3_ref[...])
    y_ref[...] = dot_nn(z_ref[...], w2_ref[...])


def mlp_call(chip_arr, u, dy, w1, w3, w2):
    row = lambda width: pl.BlockSpec((PAIR, width), lambda i, s: (i, 0))
    pieces = [*w1, *w3, *w2]
    bf16, f32 = jnp.bfloat16, jnp.float32
    return pl.pallas_call(
        mlp_kernel,
        grid_spec=pltpu.PrefetchScalarGridSpec(
            num_scalar_prefetch=1,
            grid=(TOK // PAIR,),
            in_specs=[row(DIM), row(DIM)] + [fixed(t.shape) for t in pieces],
            out_specs=[row(HALF), row(HALF), row(HALF), row(DIM), row(DIM)],
            scratch_shapes=[pltpu.VMEM((DIM, HALF), bf16), pltpu.VMEM((DIM, HALF), bf16), pltpu.VMEM((HALF, DIM), bf16)],
        ),
        out_shape=[jax.ShapeDtypeStruct((TOK, HALF), bf16)] * 3 + [jax.ShapeDtypeStruct((TOK, DIM), f32)] * PAIRS,
        compiler_params=params(),
        cost_estimate=cost(12 * TOK * DIM * HALF, 30),
        name='mlp',
    )(chip_arr, u, dy, *pieces)


def dw_kernel(la_ref, lb_ref, *refs):
    rights, out_ref = refs[:-1], refs[-1]
    for n in range(len(rights) // 2):
        ra_ref, rb_ref = rights[2 * n], rights[2 * n + 1]
        cols = ra_ref.shape[1]
        out_ref[:, n * cols:(n + 1) * cols] = dot_tn(la_ref[...], ra_ref[...]) + dot_tn(lb_ref[...], rb_ref[...])


def dw_call(la, lb, *rights):
    rows, cols = la.shape[1] // 4, rights[0].shape[1]
    total = cols * len(rights) // 2
    left = pl.BlockSpec((TOK, rows), lambda b: (0, b))
    right = fixed((TOK, cols))
    return pl.pallas_call(
        dw_kernel,
        grid=(4,),
        in_specs=[left, left] + [right] * len(rights),
        out_specs=pl.BlockSpec((rows, total), lambda b: (b, 0)),
        out_shape=jax.ShapeDtypeStruct((4 * rows, total), jnp.float32),
        compiler_params=params(),
        cost_estimate=cost(4 * TOK * rows * 4 * total, 20),
        name='dw',
    )(la, lb, *rights)


def dw_split_kernel(idx_ref, la_ref, lb_ref, ra_ref, rb_ref, send_ref, keep_ref):
    b = pl.program_id(0)
    total = dot_tn(la_ref[...], ra_ref[...]) + dot_tn(lb_ref[...], rb_ref[...])
    for n, ref in enumerate((send_ref, keep_ref)):
        @pl.when(b // PAIRS == n)
        def _(ref=ref):
            ref[0] = total


def dw_split_call(idx, la, lb, ra, rb):
    rows, cols = la.shape[1] // SP, ra.shape[1]
    left = pl.BlockSpec((TOK, rows), lambda b, s: (0, s[b]))
    right = fixed((TOK, cols))
    out = lambda n: pl.BlockSpec((1, rows, cols), lambda b, s: (jnp.clip(b - PAIRS * n, 0, 1), 0, 0))
    return pl.pallas_call(
        dw_split_kernel,
        grid_spec=pltpu.PrefetchScalarGridSpec(
            num_scalar_prefetch=1, grid=(SP,), in_specs=[left, left, right, right], out_specs=[out(0), out(1)]),
        out_shape=[jax.ShapeDtypeStruct((PAIRS, rows, cols), jnp.float32)] * PAIRS,
        compiler_params=params(),
        cost_estimate=cost(SP * TOK * rows * SP * cols, 20),
        name='dw_split',
    )(idx, la, lb, ra, rb)


def dw_qkv_kernel(u_ref, *refs):
    out_ref = refs[-1]
    total = dot_tn(u_ref[0:TOK, :], refs[0][...])
    for n in range(1, 4):
        total += dot_tn(u_ref[n * TOK:(n + 1) * TOK, :], refs[n][...])
    out_ref[...] = total


def dw_qkv_call(u, pieces):
    return pl.pallas_call(
        dw_qkv_kernel,
        grid=(4,),
        in_specs=[pl.BlockSpec((SEQ, PAIR), lambda b: (0, b))] + [fixed((TOK, GRP))] * 4,
        out_specs=pl.BlockSpec((PAIR, GRP), lambda b: (b, 0)),
        out_shape=jax.ShapeDtypeStruct((DIM, GRP), jnp.float32),
        compiler_params=params(),
        cost_estimate=cost(2 * SEQ * DIM * GRP, 14),
        name='dw_qkv',
    )(u, *pieces)


def dout_kernel(sp_ref, h0_ref, h1_ref, h2_ref, h3_ref, o0_ref, o1_ref, wa_ref, wb_ref, d0_ref, d1_ref, dwo_ref, scr):
    i = pl.program_id(0)
    for n, ref in enumerate((h0_ref, h1_ref, h2_ref, h3_ref)):
        @pl.when(i // 2 == n)
        def _(ref=ref):
            scr[...] = ref[...]
    dh = scr[...]
    d0_ref[...] = dot_nt(dh, wa_ref[...]).astype(jnp.bfloat16)
    d1_ref[...] = dot_nt(dh, wb_ref[...]).astype(jnp.bfloat16)

    @pl.when(i == 0)
    def _():
        dwo_ref[...] = jnp.zeros_like(dwo_ref)

    dwo_ref[0] += dot_tn(o0_ref[0], dh)
    dwo_ref[1] += dot_tn(o1_ref[0], dh)


def dout_call(sp_arr, dhs, o0, o1, wo):
    src = lambda n: pl.BlockSpec((BLK, DIM), lambda i, s: (jnp.clip(i - 2 * n, 0, 1), 0))
    o_spec = pl.BlockSpec((1, BLK, PAIR), lambda i, s: (s[0] ^ (i // 2), i % 2, 0))
    d_spec = pl.BlockSpec((BLK, PAIR), lambda i, s: ((s[0] ^ (i // 2)) * 2 + i % 2, 0))
    out = jax.ShapeDtypeStruct((SEQ, PAIR), jnp.bfloat16)
    return pl.pallas_call(
        dout_kernel,
        grid_spec=pltpu.PrefetchScalarGridSpec(
            num_scalar_prefetch=1,
            grid=(SEQ // BLK,),
            in_specs=[src(0), src(1), src(2), src(3), o_spec, o_spec,
                      pl.BlockSpec((PAIR, DIM), lambda i, s: (s[0], 0)), pl.BlockSpec((PAIR, DIM), lambda i, s: (4 + s[0], 0))],
            out_specs=[d_spec, d_spec, fixed((2, PAIR, DIM))],
            scratch_shapes=[pltpu.VMEM((BLK, DIM), jnp.bfloat16)],
        ),
        out_shape=[out, out, jax.ShapeDtypeStruct((2, PAIR, DIM), jnp.float32)],
        compiler_params=params(),
        cost_estimate=cost(4 * SEQ * DIM * GRP, 20),
        name='dout',
    )(sp_arr, *dhs, o0, o1, wo, wo)


def du_sum(sp_ref, pieces, w_ref):
    total = 0.0
    for n, piece in enumerate(pieces):
        cols = pl.ds(pl.multiple_of((sp_ref[0] ^ n) * GRP, GRP), GRP)
        total += dot_nt(piece[...], w_ref[:, cols])
    return total


def du_kernel(sp_ref, *refs):
    refs[-1][...] = du_sum(sp_ref, refs[:SP], refs[SP])


def dx_kernel(sp_ref, *refs):
    w_ref, du_ref, x_ref, dr_ref, g_ref, dx_ref, dg_ref = refs[SP:]
    d_u = du_ref[...] + du_sum(sp_ref, refs[:SP], w_ref)
    x32 = x_ref[...].astype(jnp.float32)
    inv_rms = lax.rsqrt(jnp.mean(x32 * x32, axis=-1, keepdims=True) + NORM_EPS)
    normed = x32 * inv_rms
    d_normed = d_u * g_ref[...].astype(jnp.float32)
    grad_in = inv_rms * (d_normed - normed * jnp.mean(d_normed * normed, axis=-1, keepdims=True))
    dx_ref[...] = (dr_ref[...] + grad_in).astype(jnp.bfloat16)

    @pl.when(pl.program_id(0) == 0)
    def _():
        dg_ref[...] = jnp.zeros_like(dg_ref)

    dg_ref[...] += jnp.sum(d_u * normed, axis=0, keepdims=True)


def dx_call(sp_arr, group, pieces, w_all, *rest):
    row = lambda width: pl.BlockSpec((PAIR, width), lambda i, s: (i, 0))
    one = fixed((1, DIM))
    du_shape = jax.ShapeDtypeStruct((TOK, DIM), jnp.float32)
    last = len(rest) > 0
    return pl.pallas_call(
        dx_kernel if last else du_kernel,
        grid_spec=pltpu.PrefetchScalarGridSpec(
            num_scalar_prefetch=1,
            grid=(TOK // PAIR,),
            in_specs=[row(GRP)] * SP + [pl.BlockSpec((DIM, SP * GRP), lambda i, s: (0, group))] + ([row(DIM)] * 3 + [one] if last else []),
            out_specs=[row(DIM), one] if last else row(DIM),
        ),
        out_shape=[jax.ShapeDtypeStruct((TOK, DIM), jnp.bfloat16), jax.ShapeDtypeStruct((1, DIM), jnp.float32)] if last else du_shape,
        compiler_params=params(),
        cost_estimate=cost(SP * TOK * DIM * DIM, 16),
        name='dx' if last else 'du',
    )(sp_arr, *pieces, w_all, *rest)


def gather_full(shard):
    return lax.all_gather(shard, ALL_AXES, axis=0, tiled=True)


def swap_seq(parts):
    return lax.all_to_all(parts, 'sp', 0, 0, tiled=True)


def swap_all(parts):
    return lax.all_to_all(parts, ALL_AXES, 0, 0, tiled=True)


def from_sp(value, bits):
    return lax.ppermute(value, 'sp', [(s, s ^ bits) for s in range(SP)])


def from_dp(value):
    return lax.ppermute(value, 'dp', [(0, 1), (1, 0)])


def gather_chip_then_core(value):
    far = from_sp(value, 2)
    return value, from_sp(value, 1), far, from_sp(far, 1)


def gather_chips(value):
    across = from_dp(value)
    along = from_sp(value, 2)
    far = from_dp(along)
    return value, along, across, far


def reduce_chips(part):
    return lax.psum_scatter(part, ALL_AXES, scatter_dimension=0, tiled=True, axis_index_groups=CORE_GROUPS)


def layer_step(hidden, positions, grad_out, gain_attn, gain_mlp, w_query, w_key, w_value, w_out, w_gate, w_up, w_down):
    tokens = hidden[0]
    d_layer = grad_out[0]
    dp = lax.axis_index('dp')
    sp = lax.axis_index('sp')
    core = sp % 2
    chip = dp * PAIRS + sp // PAIRS
    f32, bf16 = jnp.float32, jnp.bfloat16
    sp_arr, dp_arr, core_arr = (t.astype(jnp.int32)[None] for t in (sp, dp, core))
    chip_arr = chip.astype(jnp.int32)[None]

    xs = gather_chip_then_core(tokens)
    w_cols, w_send, a1, b1, a3, b3 = pack_call(core_arr, w_query, w_key, w_value, w_gate, w_up, gain_attn[None], gain_mlp[None])
    w_mine = swap_seq(w_send)
    w_got = from_dp(w_mine)
    w_own, gain1, gain2 = join_qkv_call(dp_arr, w_mine, w_got)
    gain1, gain2 = gain1[0:1], gain2[0:1]
    pos = gather_chip_then_core(positions[0].reshape(8, HEAD_DIM))
    pos_all = jnp.concatenate(pos).reshape(SEQ)
    w1_rows, w3_rows = join_call(core_arr, (a1, from_sp(b1, 1)), (a3, from_sp(b3, 1)))
    wo_full = gather_full(w_out)
    w2, w1, w3 = (gather_chips(t) for t in (w_down, w1_rows, w3_rows))
    w_all = gather_full(w_cols)
    dy_pair = from_sp(d_layer, 1)

    lane = jnp.arange(HEAD_DIM)
    half = HEAD_DIM // 2
    inv_freq = ROPE_BASE ** (-((lane % half).astype(f32) * (2.0 / HEAD_DIM)))
    angles = pos_all.astype(f32)[:, None] * inv_freq
    cos = jnp.cos(angles)
    sin = jnp.sin(angles) * jnp.where(lane < half, -1.0, 1.0)

    near = qkv_call(sp_arr, xs[0], xs[1], 0, gain1, w_own, cos, sin, ())
    u_all, q0, k0, v0, q1, k1, v1 = qkv_call(sp_arr, xs[2], xs[3], 2, gain1, w_own, cos, sin, near)
    o0, lse0 = fwd_call(q0, k0, v0)
    got0 = swap_seq(o0)
    o1, lse1 = fwd_call(q1, k1, v1)
    got1 = swap_seq(o1)
    residual, u_mlp = oproj_call(got0, got1, wo_full, tokens, gain2)

    u_pair = from_sp(u_mlp, 1)
    z_a, da_a, dc_a, y_a, d_a = mlp_call(chip_arr, u_mlp, d_layer, w1, w3, w2)
    z_b, da_b, dc_b, y_b, d_b = mlp_call(chip_arr, u_pair, dy_pair, w1, w3, w2)
    d_umlp = d_a + from_sp(d_b, 1)
    h32 = residual.astype(f32)
    layer_out = (h32 + (y_a + from_sp(y_b, 1))).astype(bf16)
    inv_rms2 = lax.rsqrt(jnp.mean(h32 * h32, axis=-1, keepdims=True) + NORM_EPS)
    normed2 = h32 * inv_rms2
    d_normed2 = d_umlp * gain2.astype(f32)
    d_gain2 = jnp.sum(d_umlp * normed2, axis=0)
    d_resid = d_layer.astype(f32) + inv_rms2 * (d_normed2 - normed2 * jnp.mean(d_normed2 * normed2, axis=-1, keepdims=True))
    dhs = gather_chip_then_core(d_resid.astype(bf16))
    order = jnp.stack([chip ^ 3, chip ^ 2, chip ^ 1, chip]).astype(jnp.int32)
    down_send, down_keep = dw_split_call(order, z_a, z_b, d_layer, dy_pair)
    down_got = from_dp(down_send)

    part = reduce_chips(dw_call(u_mlp, u_pair, da_a, da_b, dc_a, dc_b))

    do0, do1, dwo = dout_call(sp_arr, dhs, o0, o1, wo_full)
    down_far, down_near = down_keep[0] + down_got[0], down_keep[1] + down_got[1]
    down_last = from_sp(down_far, 2)
    o_seq = (o0.reshape(SEQ, PAIR), o1.reshape(SEQ, PAIR))
    d0 = bwd_call(sp_arr, q0, k0, v0, o_seq[0], do0, lse0, cos, sin)
    back0 = [d0[0]] + [from_sp(d0[n], n) for n in (1, 2, 3)]
    part0 = dw_qkv_call(u_all, d0).reshape(8, HEAD_DIM, GRP)
    dw0 = swap_all(part0)
    d1 = bwd_call(sp_arr, q1, k1, v1, o_seq[1], do1, lse1, cos, sin)
    back1 = [d1[0]] + [from_sp(d1[n], n) for n in (1, 2, 3)]
    part1 = dw_qkv_call(u_all, d1).reshape(8, HEAD_DIM, GRP)
    part1, _ = lax.optimization_barrier((part1, dw0))
    dw1 = swap_all(part1)
    grad_w_out = lax.dynamic_index_in_dim(dwo, dp, 0, keepdims=False) + from_dp(lax.dynamic_index_in_dim(dwo, 1 - dp, 0, keepdims=False))
    part, _ = lax.optimization_barrier((part, part1))
    send = lax.dynamic_slice(part, ((1 - core) * HEAD_DIM, 0), (HEAD_DIM, 2 * HALF))
    grad_w_gate, grad_w_up = unpack_cols_call(core_arr, part, from_sp(send, 1))
    grad_w_down = down_near + down_last
    du0 = dx_call(sp_arr, 0, back0, w_all)
    grad_hidden, d_gain1 = dx_call(sp_arr, 1, back1, w_all, du0, tokens, d_resid, gain1)
    grad_w_query, grad_w_key, grad_w_value = unpack_qkv_call(dw0, dw1)
    gain_parts = jnp.stack([d_gain1.reshape(8, HEAD_DIM), d_gain2.reshape(8, HEAD_DIM)], axis=1)
    gain_parts, _ = lax.optimization_barrier((gain_parts, dw1))
    gain_sums = jnp.sum(swap_all(gain_parts), axis=0)
    return (layer_out[None], grad_hidden[None], gain_sums[0], gain_sums[1], grad_w_query, grad_w_key, grad_w_value,
            grad_w_out, grad_w_gate, grad_w_up, grad_w_down)


def solution(mesh):
    act_spec = P('dp', 'sp', None)
    pos_spec = P('dp', 'sp')
    vec_spec = P(ALL_AXES)
    mat_spec = P(ALL_AXES, None)
    in_specs = (act_spec, pos_spec, act_spec, vec_spec, vec_spec) + (mat_spec,) * 7
    out_specs = (act_spec, act_spec, vec_spec, vec_spec) + (mat_spec,) * 7

    return jax.shard_map(layer_step, mesh=mesh, in_specs=in_specs, out_specs=out_specs, check_vma=False)
```

```python
import math

import jax
import jax.numpy as jnp
from jax import lax
from jax.experimental import pallas as pl
from jax.experimental.pallas import tpu as pltpu
from jax.sharding import PartitionSpec as P


HEAD_DIM = 128
ROPE_BASE = 10000.0
NORM_EPS = 1e-5
ATTN_SCALE = HEAD_DIM ** -0.5
LOG2E = math.log2(math.e)
SCALE2 = ATTN_SCALE * LOG2E
ALL_AXES = ('dp', 'sp')
BLK = 512
QSUB = 256
SEQ = 4096
TOK = 1024
DIM = 1024
HALF = 1536
SEND = 144
CORE_GROUPS = [[0, 2, 4, 6], [1, 3, 5, 7]]
PAIR = 256
TINY = 10 ** 8
SP = 4
PAIRS = 2
GRP = 512
OWN = 384
NEG = -1e30
VMEM_LIMIT = 60 * 1024 * 1024


def dot_nt(left, right):
    return lax.dot_general(left, right, (((1,), (1,)), ((), ())), preferred_element_type=jnp.float32)


def dot_nn(left, right):
    return lax.dot_general(left, right, (((1,), (0,)), ((), ())), preferred_element_type=jnp.float32)


def dot_tn(left, right):
    return lax.dot_general(left, right, (((0,), (0,)), ((), ())), preferred_element_type=jnp.float32)


def fixed(shape):
    return pl.BlockSpec(shape, lambda *_: tuple(0 for _ in shape))


def row_block(width):
    return pl.BlockSpec((PAIR, width), lambda i, *_: (i, 0))


def pick(values, index):
    return lax.dynamic_index_in_dim(values, index, 0, keepdims=False)


def row_mean(values):
    return jnp.mean(values, axis=-1, keepdims=True)


def normalize(values):
    inv_rms = lax.rsqrt(row_mean(values * values) + NORM_EPS)
    return values * inv_rms, inv_rms


def normalize_grad(d_normed, normed, inv_rms):
    return inv_rms * (d_normed - normed * row_mean(d_normed * normed))


def accumulate(ref, value):
    @pl.when(pl.program_id(0) == 0)
    def _():
        ref[...] = jnp.zeros_like(ref)

    ref[...] += value


def col_sum(values):
    return jnp.sum(values, axis=0, keepdims=True)


def params(**kw):
    return pltpu.CompilerParams(vmem_limit_bytes=VMEM_LIMIT, dimension_semantics=('arbitrary',), **kw)


def cost(flops, mib):
    return pl.CostEstimate(flops=flops, bytes_accessed=mib << 20, transcendentals=0)


def pack_kernel(core_ref, wq_ref, wk_ref, wv_ref, w1_ref, w3_ref, g1_ref, g2_ref, all_ref, send_ref, a1_ref, b1_ref, a3_ref, b3_ref):
    for g in range(PAIRS):
        for n in range(SP):
            m = g * 4 + n
            piece = jnp.concatenate([wq_ref[:, m * PAIR:(m + 1) * PAIR], wk_ref[:, m * HEAD_DIM:(m + 1) * HEAD_DIM], wv_ref[:, m * HEAD_DIM:(m + 1) * HEAD_DIM]], axis=1)
            all_ref[:, m * GRP:(m + 1) * GRP] = piece
            send_ref[n * SEND:n * SEND + HEAD_DIM, g * GRP:(g + 1) * GRP] = piece
    tail = jnp.concatenate([g1_ref[...], g2_ref[...], jnp.zeros((1, DIM - PAIR), jnp.bfloat16)], axis=1)
    for n in range(SP):
        send_ref[n * SEND + HEAD_DIM:(n + 1) * SEND, :] = jnp.broadcast_to(tail, (SEND - HEAD_DIM, DIM))
    core = core_ref[0]
    for ref, own_ref, other_ref in ((w1_ref, a1_ref, b1_ref), (w3_ref, a3_ref, b3_ref)):
        for n in range(SP):
            cols = slice(n * OWN, (n + 1) * OWN)
            own_ref[:, cols] = ref[:, pl.ds(pl.multiple_of((n * 2 + core) * OWN, HEAD_DIM), OWN)]
            other_ref[:, cols] = ref[:, pl.ds(pl.multiple_of((n * 2 + 1 - core) * OWN, HEAD_DIM), OWN)]


def pack_call(core_arr, *weights):
    out = lambda *shape: jax.ShapeDtypeStruct(shape, jnp.bfloat16)
    return pl.pallas_call(
        pack_kernel,
        in_specs=[pl.BlockSpec(memory_space=pltpu.SMEM)] + [pl.BlockSpec(memory_space=pltpu.VMEM)] * 7,
        out_shape=[out(HEAD_DIM, SEQ), out(4 * SEND, DIM)] + [out(HEAD_DIM, HALF)] * 4,
        cost_estimate=cost(TINY, 6),
        name='pack',
    )(core_arr, *weights)


def join_kernel(pos_ref, *refs):
    count = len(refs) // 3
    for n in range(count):
        own_ref, got_ref, out_ref = refs[2 * n], refs[2 * n + 1], refs[2 * count + n]
        rows = own_ref.shape[0]
        out_ref[pl.ds(pl.multiple_of(pos_ref[0] * rows, HEAD_DIM), rows), :] = own_ref[...]
        out_ref[pl.ds(pl.multiple_of((1 - pos_ref[0]) * rows, HEAD_DIM), rows), :] = got_ref[...]


def join_call(pos_arr, *pairs):
    flat = [t for pair in pairs for t in pair]
    return pl.pallas_call(
        join_kernel,
        in_specs=[pl.BlockSpec(memory_space=pltpu.SMEM)] + [pl.BlockSpec(memory_space=pltpu.VMEM)] * len(flat),
        out_shape=[jax.ShapeDtypeStruct((2 * a.shape[0], a.shape[1]), a.dtype) for a, _ in pairs],
        cost_estimate=cost(TINY, 4),
        name='join',
    )(pos_arr, *flat)


def join_qkv_kernel(dp_ref, own_ref, got_ref, w_ref, g1_ref, g2_ref):
    for ref, part in ((own_ref, dp_ref[0]), (got_ref, 1 - dp_ref[0])):
        for n in range(SP):
            rows = pl.ds(pl.multiple_of((part * 4 + n) * HEAD_DIM, HEAD_DIM), HEAD_DIM)
            w_ref[rows, :] = ref[n * SEND:n * SEND + HEAD_DIM, :]
            tail = ref[n * SEND + HEAD_DIM:(n + 1) * SEND, 0:PAIR]
            g1_ref[:, rows] = tail[:, 0:HEAD_DIM]
            g2_ref[:, rows] = tail[:, HEAD_DIM:PAIR]


def join_qkv_call(dp_arr, own, got):
    out = lambda rows: jax.ShapeDtypeStruct((rows, DIM), jnp.bfloat16)
    return pl.pallas_call(
        join_qkv_kernel,
        in_specs=[pl.BlockSpec(memory_space=pltpu.SMEM)] + [pl.BlockSpec(memory_space=pltpu.VMEM)] * 2,
        out_shape=[out(DIM), out(SEND - HEAD_DIM), out(SEND - HEAD_DIM)],
        cost_estimate=cost(TINY, 4),
        name='join_qkv',
    )(dp_arr, own, got)


def unpack_qkv_kernel(p0_ref, p1_ref, wq_ref, wk_ref, wv_ref):
    for g, ref in enumerate((p0_ref, p1_ref)):
        for n in range(SP):
            m = g * 4 + n
            total = ref[n] + ref[4 + n]
            wq_ref[:, m * PAIR:(m + 1) * PAIR] = total[:, 0:PAIR]
            wk_ref[:, m * HEAD_DIM:(m + 1) * HEAD_DIM] = total[:, PAIR:OWN]
            wv_ref[:, m * HEAD_DIM:(m + 1) * HEAD_DIM] = total[:, OWN:GRP]


def unpack_qkv_call(p0, p1):
    out = lambda cols: jax.ShapeDtypeStruct((HEAD_DIM, cols), jnp.float32)
    return pl.pallas_call(unpack_qkv_kernel, out_shape=[out(2048), out(DIM), out(DIM)], cost_estimate=cost(TINY, 6), name='unpack_qkv')(p0, p1)


def unpack_cols_kernel(core_ref, own_ref, got_ref, gate_ref, up_ref):
    core = core_ref[0]
    mine = own_ref[pl.ds(pl.multiple_of(core * HEAD_DIM, HEAD_DIM), HEAD_DIM), :]
    for w, ref in enumerate((gate_ref, up_ref)):
        for n in range(SP):
            cols = slice(w * HALF + n * OWN, w * HALF + (n + 1) * OWN)
            ref[:, pl.ds(pl.multiple_of((n * 2 + core) * OWN, HEAD_DIM), OWN)] = mine[:, cols]
            ref[:, pl.ds(pl.multiple_of((n * 2 + 1 - core) * OWN, HEAD_DIM), OWN)] = got_ref[:, cols]


def unpack_cols_call(core_arr, own, got):
    return pl.pallas_call(
        unpack_cols_kernel,
        in_specs=[pl.BlockSpec(memory_space=pltpu.SMEM)] + [pl.BlockSpec(memory_space=pltpu.VMEM)] * 2,
        out_shape=[jax.ShapeDtypeStruct((HEAD_DIM, 2 * HALF), jnp.float32)] * 2,
        cost_estimate=cost(TINY, 4),
        name='unpack_cols',
    )(core_arr, own, got)


def qkv_kernel(sp_ref, xa_ref, xb_ref, g_ref, w_ref, cos_ref, sin_ref, *rest):
    u_ref, q0_ref, k0_ref, v0_ref, q1_ref, k1_ref, v1_ref, x_scr = rest[-8:]
    i = pl.program_id(0)

    @pl.when(i < 2)
    def _():
        x_scr[...] = xa_ref[...]

    @pl.when(i >= 2)
    def _():
        x_scr[...] = xb_ref[...]

    u = (normalize(x_scr[...].astype(jnp.float32))[0] * g_ref[...].astype(jnp.float32)).astype(jnp.bfloat16)
    u_ref[...] = u
    cos, sin = cos_ref[...], sin_ref[...]

    def rope(t):
        return (t * cos + pltpu.roll(t, 64, 1) * sin).astype(jnp.bfloat16)

    for g, (q_ref, k_ref, v_ref) in enumerate(((q0_ref, k0_ref, v0_ref), (q1_ref, k1_ref, v1_ref))):
        y = dot_nn(u, w_ref[:, g * GRP:(g + 1) * GRP])
        q_ref[:, 0:HEAD_DIM] = rope(y[:, 0:HEAD_DIM])
        q_ref[:, HEAD_DIM:PAIR] = rope(y[:, HEAD_DIM:PAIR])
        k_ref[...] = rope(y[:, PAIR:OWN])
        v_ref[...] = y[:, OWN:GRP].astype(jnp.bfloat16)


def qkv_call(sp_arr, xa, xb, first, gain, w_own, cos, sin, prev):
    place = lambda width: pl.BlockSpec((BLK, width), lambda i, s: ((s[0] ^ (first + i // PAIRS)) * PAIRS + i % PAIRS, 0))
    local = lambda width: pl.BlockSpec((BLK, width), lambda i, s: (first * PAIRS + i, 0))
    out = lambda width: jax.ShapeDtypeStruct((SEQ, width), jnp.bfloat16)
    xa_spec = pl.BlockSpec((BLK, DIM), lambda i, s: (jnp.minimum(i, 1), 0))
    xb_spec = pl.BlockSpec((BLK, DIM), lambda i, s: (jnp.maximum(i - 2, 0), 0))
    widths = (DIM, PAIR, HEAD_DIM, HEAD_DIM, PAIR, HEAD_DIM, HEAD_DIM)
    return pl.pallas_call(
        qkv_kernel,
        grid_spec=pltpu.PrefetchScalarGridSpec(
            num_scalar_prefetch=1,
            grid=(4,),
            in_specs=[xa_spec, xb_spec, fixed((1, DIM)), fixed((DIM, DIM)), local(HEAD_DIM), local(HEAD_DIM)]
            + [pl.BlockSpec(memory_space=pl.ANY)] * len(prev),
            out_specs=[local(DIM)] + [place(w) for w in widths[1:]],
            scratch_shapes=[pltpu.VMEM((BLK, DIM), jnp.bfloat16)],
        ),
        out_shape=[out(w) for w in widths],
        input_output_aliases={7 + n: n for n in range(len(prev))},
        compiler_params=params(),
        cost_estimate=cost(2 * 2048 * DIM * DIM, 20),
        name='qkv',
    )(sp_arr, xa, xb, gain, w_own, cos, sin, *prev)


def fwd_kernel(q_ref, k_ref, v_ref, o_ref, lse_ref, acc_ref, q_scr):
    i = pl.program_id(0)
    for h in range(PAIRS):
        q_scr[h * BLK:(h + 1) * BLK, :] = q_ref[:, h * HEAD_DIM:(h + 1) * HEAD_DIM]

    chunks = [(h, n) for h in range(PAIRS) for n in range(BLK // QSUB)]

    def step(j, carry, masked):
        start = pl.multiple_of(j * BLK, BLK)
        k = k_ref[pl.ds(start, BLK), :]
        v = v_ref[pl.ds(start, BLK), :]

        def scores(c):
            h, n = chunks[c]
            s = dot_nt(k, q_scr[h * BLK + n * QSUB:h * BLK + (n + 1) * QSUB, :])
            if masked:
                kv_idx = lax.broadcasted_iota(jnp.int32, (BLK, QSUB), 0)
                q_idx = lax.broadcasted_iota(jnp.int32, (BLK, QSUB), 1) + n * QSUB
                s = jnp.where(q_idx >= kv_idx, s, NEG)
            return s

        out = []
        s_next = scores(0)
        for c in range(len(chunks)):
            s = s_next
            if c + 1 < len(chunks):
                s_next = scores(c + 1)
            m, l = carry[c]
            m_new = jnp.maximum(m, jnp.max(s, axis=0, keepdims=True))
            p = jnp.exp2(s * SCALE2 - m_new * SCALE2)
            alpha = jnp.exp2((m - m_new) * SCALE2)
            l_new = alpha * l + jnp.sum(p, axis=0, keepdims=True)
            acc_ref[c] = acc_ref[c] * alpha + dot_tn(v, p.astype(jnp.bfloat16))
            out.append((m_new, l_new))
        return tuple(out)

    acc_ref[...] = jnp.zeros_like(acc_ref)
    init = tuple((jnp.full((1, QSUB), NEG, jnp.float32), jnp.zeros((1, QSUB), jnp.float32)) for _ in chunks)
    carry = lax.fori_loop(0, i, lambda j, c: step(j, c, False), init)
    carry = step(i, carry, True)
    for c, (h, n) in enumerate(chunks):
        m, l = carry[c]
        rows = slice(n * QSUB, (n + 1) * QSUB)
        o_ref[0, rows, h * HEAD_DIM:(h + 1) * HEAD_DIM] = (acc_ref[c] / l).T.astype(jnp.bfloat16)
        lse_ref[h, :, rows] = jnp.broadcast_to(m * SCALE2 + jnp.log2(l), (8, QSUB))


def fwd_call(q, k, v):
    whole = fixed((SEQ, HEAD_DIM))
    per = TOK // BLK
    return pl.pallas_call(
        fwd_kernel,
        grid=(SEQ // BLK,),
        in_specs=[pl.BlockSpec((BLK, PAIR), lambda i: (i, 0)), whole, whole],
        out_specs=[pl.BlockSpec((1, BLK, PAIR), lambda i: (i // per, i % per, 0)), pl.BlockSpec((2, 8, BLK), lambda i: (0, 0, i))],
        out_shape=[jax.ShapeDtypeStruct((SEQ // TOK, TOK, PAIR), jnp.bfloat16), jax.ShapeDtypeStruct((2, 8, SEQ), jnp.float32)],
        scratch_shapes=[pltpu.VMEM((2 * BLK // QSUB, HEAD_DIM, QSUB), jnp.float32), pltpu.VMEM((2 * BLK, HEAD_DIM), jnp.bfloat16)],
        compiler_params=params(),
        cost_estimate=cost(24 * 10 ** 9, 8),
        name='attn_fwd',
    )(q, k, v)


def bwd_kernel(sp_ref, q_ref, k_ref, v_ref, o_ref, do_ref, lse_ref, cos_ref, sin_ref, out0_ref, out1_ref, out2_ref, out3_ref, dq_acc, dk_acc, dv_acc, delta):
    j = pl.program_id(0)
    n_blk = SEQ // BLK

    @pl.when(j == 0)
    def _():
        dq_acc[...] = jnp.zeros_like(dq_acc)

        def rows(i, _):
            start = pl.multiple_of(i * BLK, BLK)
            prod = o_ref[pl.ds(start, BLK), :].astype(jnp.float32) * do_ref[pl.ds(start, BLK), :].astype(jnp.float32)
            for h in range(PAIRS):
                tot = jnp.sum(prod[:, h * HEAD_DIM:(h + 1) * HEAD_DIM], axis=1, keepdims=True)
                delta[h, :, pl.ds(start, BLK)] = jnp.broadcast_to(tot, (BLK, HEAD_DIM)).T[0:8, :]
            return 0

        lax.fori_loop(0, n_blk, rows, 0)

    k = k_ref[...]
    v = v_ref[...]
    dk_acc[...] = jnp.zeros_like(dk_acc)
    dv_acc[...] = jnp.zeros_like(dv_acc)

    def step(i, masked):
        start = pl.multiple_of(i * BLK, BLK)
        rows = pl.ds(start, BLK)
        for h in range(PAIRS):
            cols = slice(h * HEAD_DIM, (h + 1) * HEAD_DIM)
            q = q_ref[rows, cols]
            do = do_ref[rows, cols]
            s = dot_nt(k, q)
            p = jnp.exp2(s * SCALE2 - lse_ref[h, 0:1, rows])
            if masked:
                kv_idx = lax.broadcasted_iota(jnp.int32, (BLK, BLK), 0)
                q_idx = lax.broadcasted_iota(jnp.int32, (BLK, BLK), 1)
                p = jnp.where(q_idx >= kv_idx, p, 0.0)
            dp = dot_nt(v, do)
            dv_acc[...] += dot_nn(p.astype(jnp.bfloat16), do)
            ds = (p * (dp - delta[h, 0:1, rows]) * ATTN_SCALE).astype(jnp.bfloat16)
            dk_acc[...] += dot_nn(ds, q)
            dq_acc[rows, cols] += dot_tn(ds, k)

    step(j, True)

    def body(i, _):
        step(i, False)
        return 0

    lax.fori_loop(j + 1, n_blk, body, 0)

    cos, sin = cos_ref[...], sin_ref[...]

    def rope_back(t):
        t = t.astype(jnp.bfloat16).astype(jnp.float32)
        return (t * cos - pltpu.roll(t, 64, 1) * sin).astype(jnp.bfloat16)

    mine = pl.ds(pl.multiple_of(j * BLK, BLK), BLK)
    result = jnp.concatenate(
        [rope_back(dq_acc[mine, h * HEAD_DIM:(h + 1) * HEAD_DIM]) for h in range(PAIRS)] + [rope_back(dk_acc[...]), dv_acc[...].astype(jnp.bfloat16)], axis=1)
    for n, ref in enumerate((out0_ref, out1_ref, out2_ref, out3_ref)):
        @pl.when((j * BLK // TOK) ^ sp_ref[0] == n)
        def _(ref=ref):
            ref[...] = result


def bwd_call(sp_arr, q, k, v, o, do, lse, cos, sin):
    whole = lambda width: fixed((SEQ, width))
    block = pl.BlockSpec((BLK, HEAD_DIM), lambda j, s: (j, 0))
    per = TOK // BLK
    table = pl.BlockSpec((BLK, HEAD_DIM), lambda j, s: (((j // per) ^ s[0]) * per + j % per, 0))
    piece = lambda n: pl.BlockSpec((BLK, GRP), lambda j, s: (jnp.clip(j - per * (s[0] ^ n), 0, per - 1), 0))
    return pl.pallas_call(
        bwd_kernel,
        grid_spec=pltpu.PrefetchScalarGridSpec(
            num_scalar_prefetch=1,
            grid=(SEQ // BLK,),
            in_specs=[whole(PAIR), block, block, whole(PAIR), whole(PAIR), fixed((2, 8, SEQ)), table, table],
            out_specs=[piece(n) for n in range(SP)],
            scratch_shapes=[
                pltpu.VMEM((SEQ, PAIR), jnp.float32),
                pltpu.VMEM((BLK, HEAD_DIM), jnp.float32),
                pltpu.VMEM((BLK, HEAD_DIM), jnp.float32),
                pltpu.VMEM((2, 8, SEQ), jnp.float32),
            ],
        ),
        out_shape=[jax.ShapeDtypeStruct((TOK, GRP), jnp.bfloat16)] * 4,
        compiler_params=params(),
        cost_estimate=cost(60 * 10 ** 9, 16),
        name='attn_bwd',
    )(sp_arr, q, k, v, o, do, lse, cos, sin)


def oproj_kernel(a0_ref, a1_ref, w_ref, x_ref, g_ref, h_ref, u_ref):
    total = x_ref[...].astype(jnp.float32)
    for g, a_ref in enumerate((a0_ref, a1_ref)):
        a = jnp.concatenate([a_ref[s] for s in range(SP)], axis=1)
        total += dot_nn(a, w_ref[g * DIM:(g + 1) * DIM, :])
    h = total.astype(jnp.bfloat16)
    h_ref[...] = h
    u_ref[...] = (normalize(h.astype(jnp.float32))[0] * g_ref[...].astype(jnp.float32)).astype(jnp.bfloat16)


def oproj_call(a0, a1, wo, x, gain):
    blk = PAIR
    row = row_block(DIM)
    part = pl.BlockSpec((4, blk, PAIR), lambda i: (0, i, 0))
    return pl.pallas_call(
        oproj_kernel,
        grid=(TOK // blk,),
        in_specs=[part, part, fixed((2048, DIM)), row, fixed((1, DIM))],
        out_specs=[row, row],
        out_shape=[jax.ShapeDtypeStruct((TOK, DIM), jnp.bfloat16)] * 2,
        compiler_params=params(),
        cost_estimate=cost(2 * TOK * DIM * 2048, 14),
        name='oproj',
    )(a0, a1, wo, x, gain)


def mlp_kernel(chip_ref, u_ref, dy_ref, *refs):
    z_ref, da_ref, dc_ref, y_ref, d_ref, w1_ref, w3_ref, w2_ref = refs[3 * SP:]

    @pl.when(pl.program_id(0) == 0)
    def _():
        for w, ref in enumerate((w1_ref, w3_ref, w2_ref)):
            for n in range(SP):
                piece = refs[w * SP + n]
                rows = piece.shape[0]
                ref[pl.ds(pl.multiple_of((chip_ref[0] ^ n) * rows, HEAD_DIM), rows), :] = piece[...]

    u, dy = u_ref[...], dy_ref[...]
    for n in range(HALF // GRP):
        cols = slice(n * GRP, (n + 1) * GRP)
        gate = dot_nn(u, w1_ref[:, cols])
        up = dot_nn(u, w3_ref[:, cols])
        e = dot_nt(dy, w2_ref[cols, :])
        sig = 1.0 / (1.0 + jnp.exp(-gate))
        silu = gate * sig
        z_ref[:, cols] = (silu * up).astype(jnp.bfloat16)
        da_ref[:, cols] = (e * up * sig * (1.0 + gate * (1.0 - sig))).astype(jnp.bfloat16)
        dc_ref[:, cols] = (e * silu).astype(jnp.bfloat16)
    d_ref[...] = dot_nt(da_ref[...], w1_ref[...]) + dot_nt(dc_ref[...], w3_ref[...])
    y_ref[...] = dot_nn(z_ref[...], w2_ref[...])


def mlp_call(chip_arr, u, dy, w1, w3, w2):
    row = row_block
    pieces = [*w1, *w3, *w2]
    bf16, f32 = jnp.bfloat16, jnp.float32
    return pl.pallas_call(
        mlp_kernel,
        grid_spec=pltpu.PrefetchScalarGridSpec(
            num_scalar_prefetch=1,
            grid=(TOK // PAIR,),
            in_specs=[row(DIM), row(DIM)] + [fixed(t.shape) for t in pieces],
            out_specs=[row(HALF), row(HALF), row(HALF), row(DIM), row(DIM)],
            scratch_shapes=[pltpu.VMEM((DIM, HALF), bf16), pltpu.VMEM((DIM, HALF), bf16), pltpu.VMEM((HALF, DIM), bf16)],
        ),
        out_shape=[jax.ShapeDtypeStruct((TOK, HALF), bf16)] * 3 + [jax.ShapeDtypeStruct((TOK, DIM), f32)] * PAIRS,
        compiler_params=params(),
        cost_estimate=cost(12 * TOK * DIM * HALF, 30),
        name='mlp',
    )(chip_arr, u, dy, *pieces)


def dw_kernel(la_ref, lb_ref, *refs):
    rights, out_ref = refs[:-1], refs[-1]
    for n in range(len(rights) // 2):
        ra_ref, rb_ref = rights[2 * n], rights[2 * n + 1]
        cols = ra_ref.shape[1]
        out_ref[:, n * cols:(n + 1) * cols] = dot_tn(la_ref[...], ra_ref[...]) + dot_tn(lb_ref[...], rb_ref[...])


def dw_call(la, lb, *rights):
    rows, cols = la.shape[1] // 4, rights[0].shape[1]
    total = cols * len(rights) // 2
    left = pl.BlockSpec((TOK, rows), lambda b: (0, b))
    right = fixed((TOK, cols))
    return pl.pallas_call(
        dw_kernel,
        grid=(4,),
        in_specs=[left, left] + [right] * len(rights),
        out_specs=pl.BlockSpec((rows, total), lambda b: (b, 0)),
        out_shape=jax.ShapeDtypeStruct((4 * rows, total), jnp.float32),
        compiler_params=params(),
        cost_estimate=cost(4 * TOK * rows * 4 * total, 20),
        name='dw',
    )(la, lb, *rights)


def dw_split_kernel(idx_ref, la_ref, lb_ref, ra_ref, rb_ref, send_ref, keep_ref):
    b = pl.program_id(0)
    total = dot_tn(la_ref[...], ra_ref[...]) + dot_tn(lb_ref[...], rb_ref[...])
    for n, ref in enumerate((send_ref, keep_ref)):
        @pl.when(b // PAIRS == n)
        def _(ref=ref):
            ref[0] = total


def dw_split_call(idx, la, lb, ra, rb):
    rows, cols = la.shape[1] // SP, ra.shape[1]
    left = pl.BlockSpec((TOK, rows), lambda b, s: (0, s[b]))
    right = fixed((TOK, cols))
    out = lambda n: pl.BlockSpec((1, rows, cols), lambda b, s: (jnp.clip(b - PAIRS * n, 0, 1), 0, 0))
    return pl.pallas_call(
        dw_split_kernel,
        grid_spec=pltpu.PrefetchScalarGridSpec(
            num_scalar_prefetch=1, grid=(SP,), in_specs=[left, left, right, right], out_specs=[out(0), out(1)]),
        out_shape=[jax.ShapeDtypeStruct((PAIRS, rows, cols), jnp.float32)] * PAIRS,
        compiler_params=params(),
        cost_estimate=cost(SP * TOK * rows * SP * cols, 20),
        name='dw_split',
    )(idx, la, lb, ra, rb)


def dw_qkv_kernel(u_ref, *refs):
    out_ref = refs[-1]
    total = dot_tn(u_ref[0:TOK, :], refs[0][...])
    for n in range(1, 4):
        total += dot_tn(u_ref[n * TOK:(n + 1) * TOK, :], refs[n][...])
    out_ref[...] = total


def dw_qkv_call(u, pieces):
    return pl.pallas_call(
        dw_qkv_kernel,
        grid=(4,),
        in_specs=[pl.BlockSpec((SEQ, PAIR), lambda b: (0, b))] + [fixed((TOK, GRP))] * 4,
        out_specs=pl.BlockSpec((PAIR, GRP), lambda b: (b, 0)),
        out_shape=jax.ShapeDtypeStruct((DIM, GRP), jnp.float32),
        compiler_params=params(),
        cost_estimate=cost(2 * SEQ * DIM * GRP, 14),
        name='dw_qkv',
    )(u, *pieces)


def dout_kernel(sp_ref, h0_ref, h1_ref, h2_ref, h3_ref, o0_ref, o1_ref, wa_ref, wb_ref, d0_ref, d1_ref, dwo_ref, scr):
    i = pl.program_id(0)
    for n, ref in enumerate((h0_ref, h1_ref, h2_ref, h3_ref)):
        @pl.when(i // 2 == n)
        def _(ref=ref):
            scr[...] = ref[...]
    dh = scr[...]
    d0_ref[...] = dot_nt(dh, wa_ref[...]).astype(jnp.bfloat16)
    d1_ref[...] = dot_nt(dh, wb_ref[...]).astype(jnp.bfloat16)

    @pl.when(i == 0)
    def _():
        dwo_ref[...] = jnp.zeros_like(dwo_ref)

    dwo_ref[0] += dot_tn(o0_ref[0], dh)
    dwo_ref[1] += dot_tn(o1_ref[0], dh)


def dout_call(sp_arr, dhs, o0, o1, wo):
    src = lambda n: pl.BlockSpec((BLK, DIM), lambda i, s: (jnp.clip(i - 2 * n, 0, 1), 0))
    o_spec = pl.BlockSpec((1, BLK, PAIR), lambda i, s: (s[0] ^ (i // 2), i % 2, 0))
    d_spec = pl.BlockSpec((BLK, PAIR), lambda i, s: ((s[0] ^ (i // 2)) * 2 + i % 2, 0))
    out = jax.ShapeDtypeStruct((SEQ, PAIR), jnp.bfloat16)
    return pl.pallas_call(
        dout_kernel,
        grid_spec=pltpu.PrefetchScalarGridSpec(
            num_scalar_prefetch=1,
            grid=(SEQ // BLK,),
            in_specs=[src(0), src(1), src(2), src(3), o_spec, o_spec,
                      pl.BlockSpec((PAIR, DIM), lambda i, s: (s[0], 0)), pl.BlockSpec((PAIR, DIM), lambda i, s: (4 + s[0], 0))],
            out_specs=[d_spec, d_spec, fixed((2, PAIR, DIM))],
            scratch_shapes=[pltpu.VMEM((BLK, DIM), jnp.bfloat16)],
        ),
        out_shape=[out, out, jax.ShapeDtypeStruct((2, PAIR, DIM), jnp.float32)],
        compiler_params=params(),
        cost_estimate=cost(4 * SEQ * DIM * GRP, 20),
        name='dout',
    )(sp_arr, *dhs, o0, o1, wo, wo)


def du_sum(sp_ref, pieces, w_ref):
    total = 0.0
    for n, piece in enumerate(pieces):
        cols = pl.ds(pl.multiple_of((sp_ref[0] ^ n) * GRP, GRP), GRP)
        total += dot_nt(piece[...], w_ref[:, cols])
    return total


def du_kernel(sp_ref, *refs):
    refs[-1][...] = du_sum(sp_ref, refs[:SP], refs[SP])


def dx_kernel(sp_ref, *refs):
    w_ref, du_ref, x_ref, dr_ref, g_ref, dx_ref, dg_ref = refs[SP:]
    d_u = du_ref[...] + du_sum(sp_ref, refs[:SP], w_ref)
    normed, inv_rms = normalize(x_ref[...].astype(jnp.float32))
    grad_in = normalize_grad(d_u * g_ref[...].astype(jnp.float32), normed, inv_rms)
    dx_ref[...] = (dr_ref[...] + grad_in).astype(jnp.bfloat16)
    accumulate(dg_ref, col_sum(d_u * normed))


def dh_kernel(da_ref, db_ref, h_ref, dy_ref, g_ref, dr_ref, dh_ref, dg_ref):
    d_u = da_ref[...] + db_ref[...]
    normed, inv_rms = normalize(h_ref[...].astype(jnp.float32))
    d_resid = dy_ref[...].astype(jnp.float32) + normalize_grad(d_u * g_ref[...].astype(jnp.float32), normed, inv_rms)
    dr_ref[...] = d_resid
    dh_ref[...] = d_resid.astype(jnp.bfloat16)
    accumulate(dg_ref, col_sum(d_u * normed))


def dh_call(d_a, d_b, h, dy, gain):
    row = row_block(DIM)
    out = lambda rows, dtype: jax.ShapeDtypeStruct((rows, DIM), dtype)
    return pl.pallas_call(
        dh_kernel,
        grid=(TOK // PAIR,),
        in_specs=[row] * SP + [fixed(gain.shape)],
        out_specs=[row, row, fixed(gain.shape)],
        out_shape=[out(TOK, jnp.float32), out(TOK, jnp.bfloat16), out(gain.shape[0], jnp.float32)],
        compiler_params=params(),
        cost_estimate=cost(TINY, 18),
        name='dh',
    )(d_a, d_b, h, dy, gain)


def dx_call(sp_arr, group, pieces, w_all, *rest):
    row = row_block
    one = fixed((1, DIM))
    du_shape = jax.ShapeDtypeStruct((TOK, DIM), jnp.float32)
    last = len(rest) > 0
    return pl.pallas_call(
        dx_kernel if last else du_kernel,
        grid_spec=pltpu.PrefetchScalarGridSpec(
            num_scalar_prefetch=1,
            grid=(TOK // PAIR,),
            in_specs=[row(GRP)] * SP + [pl.BlockSpec((DIM, SP * GRP), lambda i, s: (0, group))] + ([row(DIM)] * 3 + [one] if last else []),
            out_specs=[row(DIM), one] if last else row(DIM),
        ),
        out_shape=[jax.ShapeDtypeStruct((TOK, DIM), jnp.bfloat16), jax.ShapeDtypeStruct((1, DIM), jnp.float32)] if last else du_shape,
        compiler_params=params(),
        cost_estimate=cost(SP * TOK * DIM * DIM, 16),
        name='dx' if last else 'du',
    )(sp_arr, *pieces, w_all, *rest)


def gather_full(shard):
    return lax.all_gather(shard, ALL_AXES, axis=0, tiled=True)


def swap_seq(parts):
    return lax.all_to_all(parts, 'sp', 0, 0, tiled=True)


def swap_all(parts):
    return lax.all_to_all(parts, ALL_AXES, 0, 0, tiled=True)


def from_sp(value, bits):
    return lax.ppermute(value, 'sp', [(s, s ^ bits) for s in range(SP)])


def from_dp(value):
    return lax.ppermute(value, 'dp', [(0, 1), (1, 0)])


def gather_chip_then_core(value):
    far = from_sp(value, 2)
    near = from_sp(value, 1)
    return value, near, far, from_sp(far, 1)


def gather_chips(value, by_x):
    across = from_dp(value)
    along = from_sp(value, 2)
    if by_x:
        return value, along, across, from_dp(along)
    return value, along, across, from_sp(across, 2)


def reduce_chips(part):
    return lax.psum_scatter(part, ALL_AXES, scatter_dimension=0, tiled=True, axis_index_groups=CORE_GROUPS)


def layer_step(hidden, positions, grad_out, gain_attn, gain_mlp, w_query, w_key, w_value, w_out, w_gate, w_up, w_down):
    tokens = hidden[0]
    d_layer = grad_out[0]
    dp = lax.axis_index('dp')
    sp = lax.axis_index('sp')
    core = sp % 2
    chip = dp * PAIRS + sp // PAIRS
    f32, bf16 = jnp.float32, jnp.bfloat16
    sp_arr, dp_arr, core_arr = (t.astype(jnp.int32)[None] for t in (sp, dp, core))
    chip_arr = chip.astype(jnp.int32)[None]

    xs = gather_chip_then_core(tokens)
    w_cols, w_send, a1, b1, a3, b3 = pack_call(core_arr, w_query, w_key, w_value, w_gate, w_up, gain_attn[None], gain_mlp[None])
    w_mine = swap_seq(w_send)
    w_got = from_dp(w_mine)
    w_own, gain1, gain2 = join_qkv_call(dp_arr, w_mine, w_got)
    gain1, gain2 = gain1[0:1], gain2[0:1]
    pos = gather_chip_then_core(positions[0].reshape(8, HEAD_DIM))
    pos_all = jnp.concatenate(pos).reshape(SEQ)
    w1_rows, w3_rows = join_call(core_arr, (a1, from_sp(b1, 1)), (a3, from_sp(b3, 1)))
    wo_full = gather_full(w_out)
    w1, w3, w2 = gather_chips(w1_rows, True), gather_chips(w3_rows, True), gather_chips(w_down, False)
    w_all = gather_full(w_cols)
    dy_pair = from_sp(d_layer, 1)

    lane = jnp.arange(HEAD_DIM)
    half = HEAD_DIM // 2
    inv_freq = ROPE_BASE ** (-((lane % half).astype(f32) * (2.0 / HEAD_DIM)))
    angles = pos_all.astype(f32)[:, None] * inv_freq
    cos = jnp.cos(angles)
    sin = jnp.sin(angles) * jnp.where(lane < half, -1.0, 1.0)

    near = qkv_call(sp_arr, xs[0], xs[1], 0, gain1, w_own, cos, sin, ())
    u_all, q0, k0, v0, q1, k1, v1 = qkv_call(sp_arr, xs[2], xs[3], 2, gain1, w_own, cos, sin, near)
    o0, lse0 = fwd_call(q0, k0, v0)
    got0 = swap_seq(o0)
    o1, lse1 = fwd_call(q1, k1, v1)
    got1 = swap_seq(o1)
    residual, u_mlp = oproj_call(got0, got1, wo_full, tokens, gain2)

    u_pair = from_sp(u_mlp, 1)
    z_a, da_a, dc_a, y_a, d_a = mlp_call(chip_arr, u_mlp, d_layer, w1, w3, w2)
    z_b, da_b, dc_b, y_b, d_b = mlp_call(chip_arr, u_pair, dy_pair, w1, w3, w2)
    d_got = from_sp(d_b, 1)
    layout_parts = y_a + from_sp(y_b, 1)
    layer_out = (residual.astype(f32) + layout_parts).astype(bf16)
    d_resid, dh, d_gain2 = dh_call(d_a, d_got, residual, d_layer, gain2)
    dhs = gather_chip_then_core(dh)
    order = jnp.stack([chip ^ 3, chip ^ 2, chip ^ 1, chip]).astype(jnp.int32)
    down_send, down_keep = dw_split_call(order, z_a, z_b, d_layer, dy_pair)
    down_got = from_dp(down_send)

    part = reduce_chips(dw_call(u_mlp, u_pair, da_a, da_b, dc_a, dc_b))

    do0, do1, dwo = dout_call(sp_arr, dhs, o0, o1, wo_full)
    down_far, down_near = down_keep[0] + down_got[0], down_keep[1] + down_got[1]
    down_last = from_sp(down_far, 2)
    o_seq = (o0.reshape(SEQ, PAIR), o1.reshape(SEQ, PAIR))
    d0 = bwd_call(sp_arr, q0, k0, v0, o_seq[0], do0, lse0, cos, sin)
    back0 = [d0[0]] + [from_sp(d0[n], n) for n in (1, 2, 3)]
    part0 = dw_qkv_call(u_all, d0).reshape(8, HEAD_DIM, GRP)
    dw0 = swap_all(part0)
    d1 = bwd_call(sp_arr, q1, k1, v1, o_seq[1], do1, lse1, cos, sin)
    back1 = [d1[0]] + [from_sp(d1[n], n) for n in (1, 2, 3)]
    part1 = dw_qkv_call(u_all, d1).reshape(8, HEAD_DIM, GRP)
    part1, _ = lax.optimization_barrier((part1, dw0))
    dw1 = swap_all(part1)
    grad_w_out = pick(dwo, dp) + from_dp(pick(dwo, 1 - dp))
    part, _ = lax.optimization_barrier((part, part1))
    send = lax.dynamic_slice(part, ((1 - core) * HEAD_DIM, 0), (HEAD_DIM, 2 * HALF))
    grad_w_gate, grad_w_up = unpack_cols_call(core_arr, part, from_sp(send, 1))
    grad_w_down = down_near + down_last
    du0 = dx_call(sp_arr, 0, back0, w_all)
    grad_hidden, d_gain1 = dx_call(sp_arr, 1, back1, w_all, du0, tokens, d_resid, gain1)
    grad_w_query, grad_w_key, grad_w_value = unpack_qkv_call(dw0, dw1)
    gain_parts = jnp.stack([d_gain1.reshape(8, HEAD_DIM), d_gain2.reshape(8, HEAD_DIM)], axis=1)
    gain_parts, _ = lax.optimization_barrier((gain_parts, dw1))
    gain_sums = jnp.sum(swap_all(gain_parts), axis=0)
    return (layer_out[None], grad_hidden[None], gain_sums[0], gain_sums[1], grad_w_query, grad_w_key, grad_w_value,
            grad_w_out, grad_w_gate, grad_w_up, grad_w_down)


def solution(mesh):
    act_spec = P('dp', 'sp', None)
    pos_spec = P('dp', 'sp')
    vec_spec = P(ALL_AXES)
    mat_spec = P(ALL_AXES, None)
    in_specs = (act_spec, pos_spec, act_spec, vec_spec, vec_spec) + (mat_spec,) * 7
    out_specs = (act_spec, act_spec, vec_spec, vec_spec) + (mat_spec,) * 7

    return jax.shard_map(layer_step, mesh=mesh, in_specs=in_specs, out_specs=out_specs, check_vma=False)
```

```python
import math

import jax
import jax.numpy as jnp
from jax import lax
from jax.experimental import pallas as pl
from jax.experimental.pallas import tpu as pltpu
from jax.sharding import PartitionSpec as P


HEAD_DIM = 128
ROPE_BASE = 10000.0
NORM_EPS = 1e-5
ATTN_SCALE = HEAD_DIM ** -0.5
LOG2E = math.log2(math.e)
SCALE2 = ATTN_SCALE * LOG2E
ALL_AXES = ('dp', 'sp')
BLK = 512
QSUB = 256
SEQ = 4096
TOK = 1024
DIM = 1024
HALF = 1536
SEND = 144
CORE_GROUPS = [[0, 2, 4, 6], [1, 3, 5, 7]]
PAIR = 256
TINY = 10 ** 8
SP = 4
PAIRS = 2
GRP = 512
OWN = 384
NEG = -1e30
VMEM_LIMIT = 60 * 1024 * 1024


def dot_nt(left, right):
    return lax.dot_general(left, right, (((1,), (1,)), ((), ())), preferred_element_type=jnp.float32)


def dot_nn(left, right):
    return lax.dot_general(left, right, (((1,), (0,)), ((), ())), preferred_element_type=jnp.float32)


def dot_tn(left, right):
    return lax.dot_general(left, right, (((0,), (0,)), ((), ())), preferred_element_type=jnp.float32)


def fixed(shape):
    return pl.BlockSpec(shape, lambda *_: tuple(0 for _ in shape))


def row_block(width):
    return pl.BlockSpec((PAIR, width), lambda i, *_: (i, 0))


def pick(values, index):
    return lax.dynamic_index_in_dim(values, index, 0, keepdims=False)


def row_mean(values):
    return jnp.mean(values, axis=-1, keepdims=True)


def normalize(values):
    inv_rms = lax.rsqrt(row_mean(values * values) + NORM_EPS)
    return values * inv_rms, inv_rms


def normalize_grad(d_normed, normed, inv_rms):
    return inv_rms * (d_normed - normed * row_mean(d_normed * normed))


def accumulate(ref, value):
    @pl.when(pl.program_id(0) == 0)
    def _():
        ref[...] = jnp.zeros_like(ref)

    ref[...] += value


def col_sum(values):
    return jnp.sum(values, axis=0, keepdims=True)


def params(**kw):
    return pltpu.CompilerParams(vmem_limit_bytes=VMEM_LIMIT, dimension_semantics=('arbitrary',), **kw)


def cost(flops, mib):
    return pl.CostEstimate(flops=flops, bytes_accessed=mib << 20, transcendentals=0)


def pack_kernel(core_ref, wq_ref, wk_ref, wv_ref, w1_ref, w3_ref, g1_ref, g2_ref, all_ref, send_ref, a1_ref, b1_ref, a3_ref, b3_ref):
    for g in range(PAIRS):
        for n in range(SP):
            m = g * 4 + n
            piece = jnp.concatenate([wq_ref[:, m * PAIR:(m + 1) * PAIR], wk_ref[:, m * HEAD_DIM:(m + 1) * HEAD_DIM], wv_ref[:, m * HEAD_DIM:(m + 1) * HEAD_DIM]], axis=1)
            all_ref[:, m * GRP:(m + 1) * GRP] = piece
            send_ref[n * SEND:n * SEND + HEAD_DIM, g * GRP:(g + 1) * GRP] = piece
    tail = jnp.concatenate([g1_ref[...], g2_ref[...], jnp.zeros((1, DIM - PAIR), jnp.bfloat16)], axis=1)
    for n in range(SP):
        send_ref[n * SEND + HEAD_DIM:(n + 1) * SEND, :] = jnp.broadcast_to(tail, (SEND - HEAD_DIM, DIM))
    core = core_ref[0]
    for ref, own_ref, other_ref in ((w1_ref, a1_ref, b1_ref), (w3_ref, a3_ref, b3_ref)):
        for n in range(SP):
            cols = slice(n * OWN, (n + 1) * OWN)
            own_ref[:, cols] = ref[:, pl.ds(pl.multiple_of((n * 2 + core) * OWN, HEAD_DIM), OWN)]
            other_ref[:, cols] = ref[:, pl.ds(pl.multiple_of((n * 2 + 1 - core) * OWN, HEAD_DIM), OWN)]


def pack_call(core_arr, *weights):
    out = lambda *shape: jax.ShapeDtypeStruct(shape, jnp.bfloat16)
    return pl.pallas_call(
        pack_kernel,
        in_specs=[pl.BlockSpec(memory_space=pltpu.SMEM)] + [pl.BlockSpec(memory_space=pltpu.VMEM)] * 7,
        out_shape=[out(HEAD_DIM, SEQ), out(4 * SEND, DIM)] + [out(HEAD_DIM, HALF)] * 4,
        cost_estimate=cost(TINY, 6),
        name='pack',
    )(core_arr, *weights)


def join_kernel(pos_ref, *refs):
    count = len(refs) // 3
    for n in range(count):
        own_ref, got_ref, out_ref = refs[2 * n], refs[2 * n + 1], refs[2 * count + n]
        rows = own_ref.shape[0]
        out_ref[pl.ds(pl.multiple_of(pos_ref[0] * rows, HEAD_DIM), rows), :] = own_ref[...]
        out_ref[pl.ds(pl.multiple_of((1 - pos_ref[0]) * rows, HEAD_DIM), rows), :] = got_ref[...]


def join_call(pos_arr, *pairs):
    flat = [t for pair in pairs for t in pair]
    return pl.pallas_call(
        join_kernel,
        in_specs=[pl.BlockSpec(memory_space=pltpu.SMEM)] + [pl.BlockSpec(memory_space=pltpu.VMEM)] * len(flat),
        out_shape=[jax.ShapeDtypeStruct((2 * a.shape[0], a.shape[1]), a.dtype) for a, _ in pairs],
        cost_estimate=cost(TINY, 4),
        name='join',
    )(pos_arr, *flat)


def join_qkv_kernel(dp_ref, own_ref, got_ref, w_ref, g1_ref, g2_ref):
    for ref, part in ((own_ref, dp_ref[0]), (got_ref, 1 - dp_ref[0])):
        for n in range(SP):
            rows = pl.ds(pl.multiple_of((part * 4 + n) * HEAD_DIM, HEAD_DIM), HEAD_DIM)
            w_ref[rows, :] = ref[n * SEND:n * SEND + HEAD_DIM, :]
            tail = ref[n * SEND + HEAD_DIM:(n + 1) * SEND, 0:PAIR]
            g1_ref[:, rows] = tail[:, 0:HEAD_DIM]
            g2_ref[:, rows] = tail[:, HEAD_DIM:PAIR]


def join_qkv_call(dp_arr, own, got):
    out = lambda rows: jax.ShapeDtypeStruct((rows, DIM), jnp.bfloat16)
    return pl.pallas_call(
        join_qkv_kernel,
        in_specs=[pl.BlockSpec(memory_space=pltpu.SMEM)] + [pl.BlockSpec(memory_space=pltpu.VMEM)] * 2,
        out_shape=[out(DIM), out(SEND - HEAD_DIM), out(SEND - HEAD_DIM)],
        cost_estimate=cost(TINY, 4),
        name='join_qkv',
    )(dp_arr, own, got)


def unpack_qkv_kernel(p0_ref, p1_ref, wq_ref, wk_ref, wv_ref):
    for g, ref in enumerate((p0_ref, p1_ref)):
        for n in range(SP):
            m = g * 4 + n
            total = ref[n] + ref[4 + n]
            wq_ref[:, m * PAIR:(m + 1) * PAIR] = total[:, 0:PAIR]
            wk_ref[:, m * HEAD_DIM:(m + 1) * HEAD_DIM] = total[:, PAIR:OWN]
            wv_ref[:, m * HEAD_DIM:(m + 1) * HEAD_DIM] = total[:, OWN:GRP]


def unpack_qkv_call(p0, p1):
    out = lambda cols: jax.ShapeDtypeStruct((HEAD_DIM, cols), jnp.float32)
    return pl.pallas_call(unpack_qkv_kernel, out_shape=[out(2048), out(DIM), out(DIM)], cost_estimate=cost(TINY, 6), name='unpack_qkv')(p0, p1)


def unpack_cols_kernel(core_ref, own_ref, got_ref, gate_ref, up_ref):
    core = core_ref[0]
    mine = own_ref[pl.ds(pl.multiple_of(core * HEAD_DIM, HEAD_DIM), HEAD_DIM), :]
    for w, ref in enumerate((gate_ref, up_ref)):
        for n in range(SP):
            cols = slice(w * HALF + n * OWN, w * HALF + (n + 1) * OWN)
            ref[:, pl.ds(pl.multiple_of((n * 2 + core) * OWN, HEAD_DIM), OWN)] = mine[:, cols]
            ref[:, pl.ds(pl.multiple_of((n * 2 + 1 - core) * OWN, HEAD_DIM), OWN)] = got_ref[:, cols]


def unpack_cols_call(core_arr, own, got):
    return pl.pallas_call(
        unpack_cols_kernel,
        in_specs=[pl.BlockSpec(memory_space=pltpu.SMEM)] + [pl.BlockSpec(memory_space=pltpu.VMEM)] * 2,
        out_shape=[jax.ShapeDtypeStruct((HEAD_DIM, 2 * HALF), jnp.float32)] * 2,
        cost_estimate=cost(TINY, 4),
        name='unpack_cols',
    )(core_arr, own, got)


def qkv_kernel(sp_ref, xa_ref, xb_ref, g_ref, w_ref, cos_ref, sin_ref, *rest):
    u_ref, q0_ref, k0_ref, v0_ref, q1_ref, k1_ref, v1_ref, x_scr = rest[-8:]
    i = pl.program_id(0)

    @pl.when(i < 2)
    def _():
        x_scr[...] = xa_ref[...]

    @pl.when(i >= 2)
    def _():
        x_scr[...] = xb_ref[...]

    u = (normalize(x_scr[...].astype(jnp.float32))[0] * g_ref[...].astype(jnp.float32)).astype(jnp.bfloat16)
    u_ref[...] = u
    cos, sin = cos_ref[...], sin_ref[...]

    def rope(t):
        return (t * cos + pltpu.roll(t, 64, 1) * sin).astype(jnp.bfloat16)

    for g, (q_ref, k_ref, v_ref) in enumerate(((q0_ref, k0_ref, v0_ref), (q1_ref, k1_ref, v1_ref))):
        y = dot_nn(u, w_ref[:, g * GRP:(g + 1) * GRP])
        q_ref[:, 0:HEAD_DIM] = rope(y[:, 0:HEAD_DIM])
        q_ref[:, HEAD_DIM:PAIR] = rope(y[:, HEAD_DIM:PAIR])
        k_ref[...] = rope(y[:, PAIR:OWN])
        v_ref[...] = y[:, OWN:GRP].astype(jnp.bfloat16)


def qkv_call(sp_arr, xa, xb, first, gain, w_own, cos, sin, prev):
    place = lambda width: pl.BlockSpec((BLK, width), lambda i, s: ((s[0] ^ (first + i // PAIRS)) * PAIRS + i % PAIRS, 0))
    local = lambda width: pl.BlockSpec((BLK, width), lambda i, s: (first * PAIRS + i, 0))
    out = lambda width: jax.ShapeDtypeStruct((SEQ, width), jnp.bfloat16)
    xa_spec = pl.BlockSpec((BLK, DIM), lambda i, s: (jnp.minimum(i, 1), 0))
    xb_spec = pl.BlockSpec((BLK, DIM), lambda i, s: (jnp.maximum(i - 2, 0), 0))
    widths = (DIM, PAIR, HEAD_DIM, HEAD_DIM, PAIR, HEAD_DIM, HEAD_DIM)
    return pl.pallas_call(
        qkv_kernel,
        grid_spec=pltpu.PrefetchScalarGridSpec(
            num_scalar_prefetch=1,
            grid=(4,),
            in_specs=[xa_spec, xb_spec, fixed((1, DIM)), fixed((DIM, DIM)), local(HEAD_DIM), local(HEAD_DIM)]
            + [pl.BlockSpec(memory_space=pl.ANY)] * len(prev),
            out_specs=[local(DIM)] + [place(w) for w in widths[1:]],
            scratch_shapes=[pltpu.VMEM((BLK, DIM), jnp.bfloat16)],
        ),
        out_shape=[out(w) for w in widths],
        input_output_aliases={7 + n: n for n in range(len(prev))},
        compiler_params=params(),
        cost_estimate=cost(2 * 2048 * DIM * DIM, 20),
        name='qkv',
    )(sp_arr, xa, xb, gain, w_own, cos, sin, *prev)


def fwd_kernel(q_ref, k_ref, v_ref, o_ref, lse_ref, acc_ref, q_scr):
    i = pl.program_id(0)
    for h in range(PAIRS):
        q_scr[h * BLK:(h + 1) * BLK, :] = q_ref[:, h * HEAD_DIM:(h + 1) * HEAD_DIM]

    chunks = [(h, n) for h in range(PAIRS) for n in range(BLK // QSUB)]

    def step(j, carry, masked):
        start = pl.multiple_of(j * BLK, BLK)
        k = k_ref[pl.ds(start, BLK), :]
        v = v_ref[pl.ds(start, BLK), :]

        def scores(c):
            h, n = chunks[c]
            s = dot_nt(k, q_scr[h * BLK + n * QSUB:h * BLK + (n + 1) * QSUB, :])
            if masked:
                kv_idx = lax.broadcasted_iota(jnp.int32, (BLK, QSUB), 0)
                q_idx = lax.broadcasted_iota(jnp.int32, (BLK, QSUB), 1) + n * QSUB
                s = jnp.where(q_idx >= kv_idx, s, NEG)
            return s

        out = []
        s_next = scores(0)
        for c in range(len(chunks)):
            s = s_next
            if c + 1 < len(chunks):
                s_next = scores(c + 1)
            m, l = carry[c]
            m_new = jnp.maximum(m, jnp.max(s, axis=0, keepdims=True))
            p = jnp.exp2(s * SCALE2 - m_new * SCALE2)
            alpha = jnp.exp2((m - m_new) * SCALE2)
            l_new = alpha * l + jnp.sum(p, axis=0, keepdims=True)
            acc_ref[c] = acc_ref[c] * alpha + dot_tn(v, p.astype(jnp.bfloat16))
            out.append((m_new, l_new))
        return tuple(out)

    acc_ref[...] = jnp.zeros_like(acc_ref)
    init = tuple((jnp.full((1, QSUB), NEG, jnp.float32), jnp.zeros((1, QSUB), jnp.float32)) for _ in chunks)
    carry = lax.fori_loop(0, i, lambda j, c: step(j, c, False), init)
    carry = step(i, carry, True)
    for c, (h, n) in enumerate(chunks):
        m, l = carry[c]
        rows = slice(n * QSUB, (n + 1) * QSUB)
        o_ref[0, rows, h * HEAD_DIM:(h + 1) * HEAD_DIM] = (acc_ref[c] / l).T.astype(jnp.bfloat16)
        lse_ref[h, :, rows] = jnp.broadcast_to(m * SCALE2 + jnp.log2(l), (8, QSUB))


def fwd_call(q, k, v):
    whole = fixed((SEQ, HEAD_DIM))
    per = TOK // BLK
    return pl.pallas_call(
        fwd_kernel,
        grid=(SEQ // BLK,),
        in_specs=[pl.BlockSpec((BLK, PAIR), lambda i: (i, 0)), whole, whole],
        out_specs=[pl.BlockSpec((1, BLK, PAIR), lambda i: (i // per, i % per, 0)), pl.BlockSpec((2, 8, BLK), lambda i: (0, 0, i))],
        out_shape=[jax.ShapeDtypeStruct((SEQ // TOK, TOK, PAIR), jnp.bfloat16), jax.ShapeDtypeStruct((2, 8, SEQ), jnp.float32)],
        scratch_shapes=[pltpu.VMEM((2 * BLK // QSUB, HEAD_DIM, QSUB), jnp.float32), pltpu.VMEM((2 * BLK, HEAD_DIM), jnp.bfloat16)],
        compiler_params=params(),
        cost_estimate=cost(24 * 10 ** 9, 8),
        name='attn_fwd',
    )(q, k, v)


def bwd_kernel(sp_ref, q_ref, k_ref, v_ref, o_ref, do_ref, lse_ref, cos_ref, sin_ref, out0_ref, out1_ref, out2_ref, out3_ref, dq_acc, dk_acc, dv_acc, delta):
    j = pl.program_id(0)
    n_blk = SEQ // BLK

    @pl.when(j == 0)
    def _():
        dq_acc[...] = jnp.zeros_like(dq_acc)

        def rows(i, _):
            start = pl.multiple_of(i * BLK, BLK)
            prod = o_ref[pl.ds(start, BLK), :].astype(jnp.float32) * do_ref[pl.ds(start, BLK), :].astype(jnp.float32)
            for h in range(PAIRS):
                tot = jnp.sum(prod[:, h * HEAD_DIM:(h + 1) * HEAD_DIM], axis=1, keepdims=True)
                delta[h, :, pl.ds(start, BLK)] = jnp.broadcast_to(tot, (BLK, HEAD_DIM)).T[0:8, :]
            return 0

        lax.fori_loop(0, n_blk, rows, 0)

    k = k_ref[...]
    v = v_ref[...]
    dk_acc[...] = jnp.zeros_like(dk_acc)
    dv_acc[...] = jnp.zeros_like(dv_acc)

    def step(i, masked):
        start = pl.multiple_of(i * BLK, BLK)
        rows = pl.ds(start, BLK)
        for h in range(PAIRS):
            cols = slice(h * HEAD_DIM, (h + 1) * HEAD_DIM)
            q = q_ref[rows, cols]
            do = do_ref[rows, cols]
            s = dot_nt(k, q)
            p = jnp.exp2(s * SCALE2 - lse_ref[h, 0:1, rows])
            if masked:
                kv_idx = lax.broadcasted_iota(jnp.int32, (BLK, BLK), 0)
                q_idx = lax.broadcasted_iota(jnp.int32, (BLK, BLK), 1)
                p = jnp.where(q_idx >= kv_idx, p, 0.0)
            dp = dot_nt(v, do)
            dv_acc[...] += dot_nn(p.astype(jnp.bfloat16), do)
            ds = (p * (dp - delta[h, 0:1, rows]) * ATTN_SCALE).astype(jnp.bfloat16)
            dk_acc[...] += dot_nn(ds, q)
            dq_acc[rows, cols] += dot_tn(ds, k)

    step(j, True)

    def body(i, _):
        step(i, False)
        return 0

    lax.fori_loop(j + 1, n_blk, body, 0)

    cos, sin = cos_ref[...], sin_ref[...]

    def rope_back(t):
        t = t.astype(jnp.bfloat16).astype(jnp.float32)
        return (t * cos - pltpu.roll(t, 64, 1) * sin).astype(jnp.bfloat16)

    mine = pl.ds(pl.multiple_of(j * BLK, BLK), BLK)
    result = jnp.concatenate(
        [rope_back(dq_acc[mine, h * HEAD_DIM:(h + 1) * HEAD_DIM]) for h in range(PAIRS)] + [rope_back(dk_acc[...]), dv_acc[...].astype(jnp.bfloat16)], axis=1)
    for n, ref in enumerate((out0_ref, out1_ref, out2_ref, out3_ref)):
        @pl.when((j * BLK // TOK) ^ sp_ref[0] == n)
        def _(ref=ref):
            ref[...] = result


def bwd_call(sp_arr, q, k, v, o, do, lse, cos, sin):
    whole = lambda width: fixed((SEQ, width))
    block = pl.BlockSpec((BLK, HEAD_DIM), lambda j, s: (j, 0))
    per = TOK // BLK
    table = pl.BlockSpec((BLK, HEAD_DIM), lambda j, s: (((j // per) ^ s[0]) * per + j % per, 0))
    piece = lambda n: pl.BlockSpec((BLK, GRP), lambda j, s: (jnp.clip(j - per * (s[0] ^ n), 0, per - 1), 0))
    return pl.pallas_call(
        bwd_kernel,
        grid_spec=pltpu.PrefetchScalarGridSpec(
            num_scalar_prefetch=1,
            grid=(SEQ // BLK,),
            in_specs=[whole(PAIR), block, block, whole(PAIR), whole(PAIR), fixed((2, 8, SEQ)), table, table],
            out_specs=[piece(n) for n in range(SP)],
            scratch_shapes=[
                pltpu.VMEM((SEQ, PAIR), jnp.float32),
                pltpu.VMEM((BLK, HEAD_DIM), jnp.float32),
                pltpu.VMEM((BLK, HEAD_DIM), jnp.float32),
                pltpu.VMEM((2, 8, SEQ), jnp.float32),
            ],
        ),
        out_shape=[jax.ShapeDtypeStruct((TOK, GRP), jnp.bfloat16)] * 4,
        compiler_params=params(),
        cost_estimate=cost(60 * 10 ** 9, 16),
        name='attn_bwd',
    )(sp_arr, q, k, v, o, do, lse, cos, sin)


def oproj_kernel(a0_ref, a1_ref, w_ref, x_ref, g_ref, h_ref, u_ref):
    total = x_ref[...].astype(jnp.float32)
    for g, a_ref in enumerate((a0_ref, a1_ref)):
        a = jnp.concatenate([a_ref[s] for s in range(SP)], axis=1)
        total += dot_nn(a, w_ref[g * DIM:(g + 1) * DIM, :])
    h = total.astype(jnp.bfloat16)
    h_ref[...] = h
    u_ref[...] = (normalize(h.astype(jnp.float32))[0] * g_ref[...].astype(jnp.float32)).astype(jnp.bfloat16)


def oproj_call(a0, a1, wo, x, gain):
    blk = PAIR
    row = row_block(DIM)
    part = pl.BlockSpec((4, blk, PAIR), lambda i: (0, i, 0))
    return pl.pallas_call(
        oproj_kernel,
        grid=(TOK // blk,),
        in_specs=[part, part, fixed((2048, DIM)), row, fixed((1, DIM))],
        out_specs=[row, row],
        out_shape=[jax.ShapeDtypeStruct((TOK, DIM), jnp.bfloat16)] * 2,
        compiler_params=params(),
        cost_estimate=cost(2 * TOK * DIM * 2048, 14),
        name='oproj',
    )(a0, a1, wo, x, gain)


def mlp_kernel(chip_ref, u_ref, dy_ref, *refs):
    z_ref, da_ref, dc_ref, y_ref, d_ref, w1_ref, w3_ref, w2_ref = refs[3 * SP:]

    @pl.when(pl.program_id(0) == 0)
    def _():
        for w, ref in enumerate((w1_ref, w3_ref, w2_ref)):
            for n in range(SP):
                piece = refs[w * SP + n]
                rows = piece.shape[0]
                ref[pl.ds(pl.multiple_of((chip_ref[0] ^ n) * rows, HEAD_DIM), rows), :] = piece[...]

    u, dy = u_ref[...], dy_ref[...]
    for n in range(HALF // GRP):
        cols = slice(n * GRP, (n + 1) * GRP)
        gate = dot_nn(u, w1_ref[:, cols])
        up = dot_nn(u, w3_ref[:, cols])
        e = dot_nt(dy, w2_ref[cols, :])
        sig = 1.0 / (1.0 + jnp.exp(-gate))
        silu = gate * sig
        z_ref[:, cols] = (silu * up).astype(jnp.bfloat16)
        da_ref[:, cols] = (e * up * sig * (1.0 + gate * (1.0 - sig))).astype(jnp.bfloat16)
        dc_ref[:, cols] = (e * silu).astype(jnp.bfloat16)
    d_ref[...] = dot_nt(da_ref[...], w1_ref[...]) + dot_nt(dc_ref[...], w3_ref[...])
    y_ref[...] = dot_nn(z_ref[...], w2_ref[...])


def mlp_call(chip_arr, u, dy, w1, w3, w2):
    row = row_block
    pieces = [*w1, *w3, *w2]
    bf16, f32 = jnp.bfloat16, jnp.float32
    return pl.pallas_call(
        mlp_kernel,
        grid_spec=pltpu.PrefetchScalarGridSpec(
            num_scalar_prefetch=1,
            grid=(TOK // PAIR,),
            in_specs=[row(DIM), row(DIM)] + [fixed(t.shape) for t in pieces],
            out_specs=[row(HALF), row(HALF), row(HALF), row(DIM), row(DIM)],
            scratch_shapes=[pltpu.VMEM((DIM, HALF), bf16), pltpu.VMEM((DIM, HALF), bf16), pltpu.VMEM((HALF, DIM), bf16)],
        ),
        out_shape=[jax.ShapeDtypeStruct((TOK, HALF), bf16)] * 3 + [jax.ShapeDtypeStruct((TOK, DIM), f32)] * PAIRS,
        compiler_params=params(),
        cost_estimate=cost(12 * TOK * DIM * HALF, 30),
        name='mlp',
    )(chip_arr, u, dy, *pieces)


def dw_kernel(la_ref, lb_ref, *refs):
    rights, out_ref = refs[:-1], refs[-1]
    for n in range(len(rights) // 2):
        ra_ref, rb_ref = rights[2 * n], rights[2 * n + 1]
        cols = ra_ref.shape[1]
        out_ref[:, n * cols:(n + 1) * cols] = dot_tn(la_ref[...], ra_ref[...]) + dot_tn(lb_ref[...], rb_ref[...])


def dw_call(la, lb, *rights):
    rows, cols = la.shape[1] // 4, rights[0].shape[1]
    total = cols * len(rights) // 2
    left = pl.BlockSpec((TOK, rows), lambda b: (0, b))
    right = fixed((TOK, cols))
    return pl.pallas_call(
        dw_kernel,
        grid=(4,),
        in_specs=[left, left] + [right] * len(rights),
        out_specs=pl.BlockSpec((rows, total), lambda b: (b, 0)),
        out_shape=jax.ShapeDtypeStruct((4 * rows, total), jnp.float32),
        compiler_params=params(),
        cost_estimate=cost(4 * TOK * rows * 4 * total, 20),
        name='dw',
    )(la, lb, *rights)


def dw_split_kernel(idx_ref, la_ref, lb_ref, ra_ref, rb_ref, send_ref, keep_ref):
    b = pl.program_id(0)
    total = dot_tn(la_ref[...], ra_ref[...]) + dot_tn(lb_ref[...], rb_ref[...])
    for n, ref in enumerate((send_ref, keep_ref)):
        @pl.when(b // PAIRS == n)
        def _(ref=ref):
            ref[0] = total


def dw_split_call(idx, la, lb, ra, rb):
    rows, cols = la.shape[1] // SP, ra.shape[1]
    left = pl.BlockSpec((TOK, rows), lambda b, s: (0, s[b]))
    right = fixed((TOK, cols))
    out = lambda n: pl.BlockSpec((1, rows, cols), lambda b, s: (jnp.clip(b - PAIRS * n, 0, 1), 0, 0))
    return pl.pallas_call(
        dw_split_kernel,
        grid_spec=pltpu.PrefetchScalarGridSpec(
            num_scalar_prefetch=1, grid=(SP,), in_specs=[left, left, right, right], out_specs=[out(0), out(1)]),
        out_shape=[jax.ShapeDtypeStruct((PAIRS, rows, cols), jnp.float32)] * PAIRS,
        compiler_params=params(),
        cost_estimate=cost(SP * TOK * rows * SP * cols, 20),
        name='dw_split',
    )(idx, la, lb, ra, rb)


def dw_qkv_kernel(u_ref, *refs):
    out_ref = refs[-1]
    total = dot_tn(u_ref[0:TOK, :], refs[0][...])
    for n in range(1, 4):
        total += dot_tn(u_ref[n * TOK:(n + 1) * TOK, :], refs[n][...])
    out_ref[...] = total


def dw_qkv_call(u, pieces):
    return pl.pallas_call(
        dw_qkv_kernel,
        grid=(4,),
        in_specs=[pl.BlockSpec((SEQ, PAIR), lambda b: (0, b))] + [fixed((TOK, GRP))] * 4,
        out_specs=pl.BlockSpec((PAIR, GRP), lambda b: (b, 0)),
        out_shape=jax.ShapeDtypeStruct((DIM, GRP), jnp.float32),
        compiler_params=params(),
        cost_estimate=cost(2 * SEQ * DIM * GRP, 14),
        name='dw_qkv',
    )(u, *pieces)


def dout_kernel(sp_ref, h0_ref, h1_ref, h2_ref, h3_ref, o0_ref, o1_ref, wa_ref, wb_ref, d0_ref, d1_ref, dwo_ref, scr):
    i = pl.program_id(0)
    for n, ref in enumerate((h0_ref, h1_ref, h2_ref, h3_ref)):
        @pl.when(i // 2 == n)
        def _(ref=ref):
            scr[...] = ref[...]
    dh = scr[...]
    d0_ref[...] = dot_nt(dh, wa_ref[...]).astype(jnp.bfloat16)
    d1_ref[...] = dot_nt(dh, wb_ref[...]).astype(jnp.bfloat16)

    @pl.when(i == 0)
    def _():
        dwo_ref[...] = jnp.zeros_like(dwo_ref)

    dwo_ref[0] += dot_tn(o0_ref[0], dh)
    dwo_ref[1] += dot_tn(o1_ref[0], dh)


def dout_call(sp_arr, dhs, o0, o1, wo):
    src = lambda n: pl.BlockSpec((BLK, DIM), lambda i, s: (jnp.clip(i - 2 * n, 0, 1), 0))
    o_spec = pl.BlockSpec((1, BLK, PAIR), lambda i, s: (s[0] ^ (i // 2), i % 2, 0))
    d_spec = pl.BlockSpec((BLK, PAIR), lambda i, s: ((s[0] ^ (i // 2)) * 2 + i % 2, 0))
    out = jax.ShapeDtypeStruct((SEQ, PAIR), jnp.bfloat16)
    return pl.pallas_call(
        dout_kernel,
        grid_spec=pltpu.PrefetchScalarGridSpec(
            num_scalar_prefetch=1,
            grid=(SEQ // BLK,),
            in_specs=[src(0), src(1), src(2), src(3), o_spec, o_spec,
                      pl.BlockSpec((PAIR, DIM), lambda i, s: (s[0], 0)), pl.BlockSpec((PAIR, DIM), lambda i, s: (4 + s[0], 0))],
            out_specs=[d_spec, d_spec, fixed((2, PAIR, DIM))],
            scratch_shapes=[pltpu.VMEM((BLK, DIM), jnp.bfloat16)],
        ),
        out_shape=[out, out, jax.ShapeDtypeStruct((2, PAIR, DIM), jnp.float32)],
        compiler_params=params(),
        cost_estimate=cost(4 * SEQ * DIM * GRP, 20),
        name='dout',
    )(sp_arr, *dhs, o0, o1, wo, wo)


def du_sum(sp_ref, pieces, w_ref):
    total = 0.0
    for n, piece in enumerate(pieces):
        cols = pl.ds(pl.multiple_of((sp_ref[0] ^ n) * GRP, GRP), GRP)
        total += dot_nt(piece[...], w_ref[:, cols])
    return total


def du_kernel(sp_ref, *refs):
    refs[-1][...] = du_sum(sp_ref, refs[:SP], refs[SP])


def dx_kernel(sp_ref, *refs):
    w_ref, du_ref, x_ref, dr_ref, g_ref, dx_ref, dg_ref = refs[SP:]
    d_u = du_ref[...] + du_sum(sp_ref, refs[:SP], w_ref)
    normed, inv_rms = normalize(x_ref[...].astype(jnp.float32))
    grad_in = normalize_grad(d_u * g_ref[...].astype(jnp.float32), normed, inv_rms)
    dx_ref[...] = (dr_ref[...] + grad_in).astype(jnp.bfloat16)
    accumulate(dg_ref, col_sum(d_u * normed))


def dx_call(sp_arr, group, pieces, w_all, *rest):
    row = row_block
    one = fixed((1, DIM))
    du_shape = jax.ShapeDtypeStruct((TOK, DIM), jnp.float32)
    last = len(rest) > 0
    return pl.pallas_call(
        dx_kernel if last else du_kernel,
        grid_spec=pltpu.PrefetchScalarGridSpec(
            num_scalar_prefetch=1,
            grid=(TOK // PAIR,),
            in_specs=[row(GRP)] * SP + [pl.BlockSpec((DIM, SP * GRP), lambda i, s: (0, group))] + ([row(DIM)] * 3 + [one] if last else []),
            out_specs=[row(DIM), one] if last else row(DIM),
        ),
        out_shape=[jax.ShapeDtypeStruct((TOK, DIM), jnp.bfloat16), jax.ShapeDtypeStruct((1, DIM), jnp.float32)] if last else du_shape,
        compiler_params=params(),
        cost_estimate=cost(SP * TOK * DIM * DIM, 16),
        name='dx' if last else 'du',
    )(sp_arr, *pieces, w_all, *rest)


def gather_full(shard):
    return lax.all_gather(shard, ALL_AXES, axis=0, tiled=True)


def swap_seq(parts):
    return lax.all_to_all(parts, 'sp', 0, 0, tiled=True)


def swap_all(parts):
    return lax.all_to_all(parts, ALL_AXES, 0, 0, tiled=True)


def from_sp(value, bits):
    return lax.ppermute(value, 'sp', [(s, s ^ bits) for s in range(SP)])


def from_dp(value):
    return lax.ppermute(value, 'dp', [(0, 1), (1, 0)])


def gather_chip_then_core(value):
    far = from_sp(value, 2)
    near = from_sp(value, 1)
    return value, near, far, from_sp(far, 1)


def gather_chips(value, by_x):
    across = from_dp(value)
    along = from_sp(value, 2)
    if by_x:
        return value, along, across, from_dp(along)
    return value, along, across, from_sp(across, 2)


def reduce_chips(part):
    return lax.psum_scatter(part, ALL_AXES, scatter_dimension=0, tiled=True, axis_index_groups=CORE_GROUPS)


def layer_step(hidden, positions, grad_out, gain_attn, gain_mlp, w_query, w_key, w_value, w_out, w_gate, w_up, w_down):
    tokens = hidden[0]
    d_layer = grad_out[0]
    dp = lax.axis_index('dp')
    sp = lax.axis_index('sp')
    core = sp % 2
    chip = dp * PAIRS + sp // PAIRS
    f32, bf16 = jnp.float32, jnp.bfloat16
    sp_arr, dp_arr, core_arr = (t.astype(jnp.int32)[None] for t in (sp, dp, core))
    chip_arr = chip.astype(jnp.int32)[None]

    xs = gather_chip_then_core(tokens)
    w_cols, w_send, a1, b1, a3, b3 = pack_call(core_arr, w_query, w_key, w_value, w_gate, w_up, gain_attn[None], gain_mlp[None])
    w_mine = swap_seq(w_send)
    w_got = from_dp(w_mine)
    w_own, gain1, gain2 = join_qkv_call(dp_arr, w_mine, w_got)
    gain1, gain2 = gain1[0:1], gain2[0:1]
    pos = gather_chip_then_core(positions[0].reshape(8, HEAD_DIM))
    pos_all = jnp.concatenate(pos).reshape(SEQ)
    w1_rows, w3_rows = join_call(core_arr, (a1, from_sp(b1, 1)), (a3, from_sp(b3, 1)))
    wo_full = gather_full(w_out)
    w1, w3, w2 = gather_chips(w1_rows, True), gather_chips(w3_rows, True), gather_chips(w_down, False)
    w_all = gather_full(w_cols)
    dy_pair = from_sp(d_layer, 1)

    lane = jnp.arange(HEAD_DIM)
    half = HEAD_DIM // 2
    inv_freq = ROPE_BASE ** (-((lane % half).astype(f32) * (2.0 / HEAD_DIM)))
    angles = pos_all.astype(f32)[:, None] * inv_freq
    cos = jnp.cos(angles)
    sin = jnp.sin(angles) * jnp.where(lane < half, -1.0, 1.0)

    near = qkv_call(sp_arr, xs[0], xs[1], 0, gain1, w_own, cos, sin, ())
    u_all, q0, k0, v0, q1, k1, v1 = qkv_call(sp_arr, xs[2], xs[3], 2, gain1, w_own, cos, sin, near)
    o0, lse0 = fwd_call(q0, k0, v0)
    got0 = swap_seq(o0)
    o1, lse1 = fwd_call(q1, k1, v1)
    got1 = swap_seq(o1)
    residual, u_mlp = oproj_call(got0, got1, wo_full, tokens, gain2)

    u_pair = from_sp(u_mlp, 1)
    z_a, da_a, dc_a, y_a, d_a = mlp_call(chip_arr, u_mlp, d_layer, w1, w3, w2)
    z_b, da_b, dc_b, y_b, d_b = mlp_call(chip_arr, u_pair, dy_pair, w1, w3, w2)
    d_umlp = d_a + from_sp(d_b, 1)
    h32 = residual.astype(f32)
    layer_out = (h32 + (y_a + from_sp(y_b, 1))).astype(bf16)
    normed2, inv_rms2 = normalize(h32)
    d_gain2 = col_sum(d_umlp * normed2)
    d_resid = d_layer.astype(f32) + normalize_grad(d_umlp * gain2.astype(f32), normed2, inv_rms2)
    dhs = gather_chip_then_core(d_resid.astype(bf16))
    order = jnp.stack([chip ^ 3, chip ^ 2, chip ^ 1, chip]).astype(jnp.int32)
    down_send, down_keep = dw_split_call(order, z_a, z_b, d_layer, dy_pair)
    down_got = from_dp(down_send)

    part = reduce_chips(dw_call(u_mlp, u_pair, da_a, da_b, dc_a, dc_b))

    do0, do1, dwo = dout_call(sp_arr, dhs, o0, o1, wo_full)
    down_far, down_near = down_keep[0] + down_got[0], down_keep[1] + down_got[1]
    down_last = from_sp(down_far, 2)
    o_seq = (o0.reshape(SEQ, PAIR), o1.reshape(SEQ, PAIR))
    d0 = bwd_call(sp_arr, q0, k0, v0, o_seq[0], do0, lse0, cos, sin)
    back0 = [d0[0]] + [from_sp(d0[n], n) for n in (1, 2, 3)]
    part0 = dw_qkv_call(u_all, d0).reshape(8, HEAD_DIM, GRP)
    dw0 = swap_all(part0)
    d1 = bwd_call(sp_arr, q1, k1, v1, o_seq[1], do1, lse1, cos, sin)
    back1 = [d1[0]] + [from_sp(d1[n], n) for n in (1, 2, 3)]
    part1 = dw_qkv_call(u_all, d1).reshape(8, HEAD_DIM, GRP)
    part1, _ = lax.optimization_barrier((part1, dw0))
    dw1 = swap_all(part1)
    grad_w_out = pick(dwo, dp) + from_dp(pick(dwo, 1 - dp))
    part, _ = lax.optimization_barrier((part, part1))
    send = lax.dynamic_slice(part, ((1 - core) * HEAD_DIM, 0), (HEAD_DIM, 2 * HALF))
    cols_got = from_sp(send, 1)
    grad_w_gate, grad_w_up = unpack_cols_call(core_arr, part, cols_got)
    grad_w_down = down_near + down_last
    du0 = dx_call(sp_arr, 0, back0, w_all)
    grad_hidden, d_gain1 = dx_call(sp_arr, 1, back1, w_all, du0, tokens, d_resid, gain1)
    grad_w_query, grad_w_key, grad_w_value = unpack_qkv_call(dw0, dw1)
    gain_parts = jnp.stack([d_gain1.reshape(8, HEAD_DIM), d_gain2.reshape(8, HEAD_DIM)], axis=1)
    gain_parts, _ = lax.optimization_barrier((gain_parts, dw1))
    gain_sums = jnp.sum(swap_all(gain_parts), axis=0)
    return (layer_out[None], grad_hidden[None], gain_sums[0], gain_sums[1], grad_w_query, grad_w_key, grad_w_value,
            grad_w_out, grad_w_gate, grad_w_up, grad_w_down)


def solution(mesh):
    act_spec = P('dp', 'sp', None)
    pos_spec = P('dp', 'sp')
    vec_spec = P(ALL_AXES)
    mat_spec = P(ALL_AXES, None)
    in_specs = (act_spec, pos_spec, act_spec, vec_spec, vec_spec) + (mat_spec,) * 7
    out_specs = (act_spec, act_spec, vec_spec, vec_spec) + (mat_spec,) * 7

    return jax.shard_map(layer_step, mesh=mesh, in_specs=in_specs, out_specs=out_specs, check_vma=False)
```

```python
import math

import jax
import jax.numpy as jnp
from jax import lax
from jax.experimental import pallas as pl
from jax.experimental.pallas import tpu as pltpu
from jax.sharding import PartitionSpec as P


HEAD_DIM = 128
ROPE_BASE = 10000.0
NORM_EPS = 1e-5
ATTN_SCALE = HEAD_DIM ** -0.5
LOG2E = math.log2(math.e)
SCALE2 = ATTN_SCALE * LOG2E
ALL_AXES = ('dp', 'sp')
BLK = 512
QSUB = 256
SEQ = 4096
TOK = 1024
DIM = 1024
HALF = 1536
SEND = 144
CORE_GROUPS = [[0, 2, 4, 6], [1, 3, 5, 7]]
PAIR = 256
TINY = 10 ** 8
SP = 4
PAIRS = 2
GRP = 512
OWN = 384
NEG = -1e30
VMEM_LIMIT = 60 * 1024 * 1024


def dot_nt(left, right):
    return lax.dot_general(left, right, (((1,), (1,)), ((), ())), preferred_element_type=jnp.float32)


def dot_nn(left, right):
    return lax.dot_general(left, right, (((1,), (0,)), ((), ())), preferred_element_type=jnp.float32)


def dot_tn(left, right):
    return lax.dot_general(left, right, (((0,), (0,)), ((), ())), preferred_element_type=jnp.float32)


def fixed(shape):
    return pl.BlockSpec(shape, lambda *_: tuple(0 for _ in shape))


def row_block(width):
    return pl.BlockSpec((PAIR, width), lambda i, *_: (i, 0))


def pick(values, index):
    return lax.dynamic_index_in_dim(values, index, 0, keepdims=False)


def row_mean(values):
    return jnp.mean(values, axis=-1, keepdims=True)


def normalize(values):
    inv_rms = lax.rsqrt(row_mean(values * values) + NORM_EPS)
    return values * inv_rms, inv_rms


def normalize_grad(d_normed, normed, inv_rms):
    return inv_rms * (d_normed - normed * row_mean(d_normed * normed))


def accumulate(ref, value):
    @pl.when(pl.program_id(0) == 0)
    def _():
        ref[...] = jnp.zeros_like(ref)

    ref[...] += value


def col_sum(values):
    return jnp.sum(values, axis=0, keepdims=True)


def params(**kw):
    return pltpu.CompilerParams(vmem_limit_bytes=VMEM_LIMIT, dimension_semantics=('arbitrary',), **kw)


def cost(flops, mib):
    return pl.CostEstimate(flops=flops, bytes_accessed=mib << 20, transcendentals=0)


def pack_kernel(core_ref, wq_ref, wk_ref, wv_ref, w1_ref, w3_ref, g1_ref, g2_ref, all_ref, send_ref, a1_ref, b1_ref, a3_ref, b3_ref):
    for g in range(PAIRS):
        for n in range(SP):
            m = g * 4 + n
            piece = jnp.concatenate([wq_ref[:, m * PAIR:(m + 1) * PAIR], wk_ref[:, m * HEAD_DIM:(m + 1) * HEAD_DIM], wv_ref[:, m * HEAD_DIM:(m + 1) * HEAD_DIM]], axis=1)
            all_ref[:, m * GRP:(m + 1) * GRP] = piece
            send_ref[n * SEND:n * SEND + HEAD_DIM, g * GRP:(g + 1) * GRP] = piece
    tail = jnp.concatenate([g1_ref[...], g2_ref[...], jnp.zeros((1, DIM - PAIR), jnp.bfloat16)], axis=1)
    for n in range(SP):
        send_ref[n * SEND + HEAD_DIM:(n + 1) * SEND, :] = jnp.broadcast_to(tail, (SEND - HEAD_DIM, DIM))
    core = core_ref[0]
    for ref, own_ref, other_ref in ((w1_ref, a1_ref, b1_ref), (w3_ref, a3_ref, b3_ref)):
        for n in range(SP):
            cols = slice(n * OWN, (n + 1) * OWN)
            own_ref[:, cols] = ref[:, pl.ds(pl.multiple_of((n * 2 + core) * OWN, HEAD_DIM), OWN)]
            other_ref[:, cols] = ref[:, pl.ds(pl.multiple_of((n * 2 + 1 - core) * OWN, HEAD_DIM), OWN)]


def pack_call(core_arr, *weights):
    out = lambda *shape: jax.ShapeDtypeStruct(shape, jnp.bfloat16)
    return pl.pallas_call(
        pack_kernel,
        in_specs=[pl.BlockSpec(memory_space=pltpu.SMEM)] + [pl.BlockSpec(memory_space=pltpu.VMEM)] * 7,
        out_shape=[out(HEAD_DIM, SEQ), out(4 * SEND, DIM)] + [out(HEAD_DIM, HALF)] * 4,
        cost_estimate=cost(TINY, 6),
        name='pack',
    )(core_arr, *weights)


def join_kernel(pos_ref, *refs):
    count = len(refs) // 3
    for n in range(count):
        own_ref, got_ref, out_ref = refs[2 * n], refs[2 * n + 1], refs[2 * count + n]
        rows = own_ref.shape[0]
        out_ref[pl.ds(pl.multiple_of(pos_ref[0] * rows, HEAD_DIM), rows), :] = own_ref[...]
        out_ref[pl.ds(pl.multiple_of((1 - pos_ref[0]) * rows, HEAD_DIM), rows), :] = got_ref[...]


def join_call(pos_arr, *pairs):
    flat = [t for pair in pairs for t in pair]
    return pl.pallas_call(
        join_kernel,
        in_specs=[pl.BlockSpec(memory_space=pltpu.SMEM)] + [pl.BlockSpec(memory_space=pltpu.VMEM)] * len(flat),
        out_shape=[jax.ShapeDtypeStruct((2 * a.shape[0], a.shape[1]), a.dtype) for a, _ in pairs],
        cost_estimate=cost(TINY, 4),
        name='join',
    )(pos_arr, *flat)


def join_qkv_kernel(dp_ref, own_ref, got_ref, w_ref, g1_ref, g2_ref):
    for ref, part in ((own_ref, dp_ref[0]), (got_ref, 1 - dp_ref[0])):
        for n in range(SP):
            rows = pl.ds(pl.multiple_of((part * 4 + n) * HEAD_DIM, HEAD_DIM), HEAD_DIM)
            w_ref[rows, :] = ref[n * SEND:n * SEND + HEAD_DIM, :]
            tail = ref[n * SEND + HEAD_DIM:(n + 1) * SEND, 0:PAIR]
            g1_ref[:, rows] = tail[:, 0:HEAD_DIM]
            g2_ref[:, rows] = tail[:, HEAD_DIM:PAIR]


def join_qkv_call(dp_arr, own, got):
    out = lambda rows: jax.ShapeDtypeStruct((rows, DIM), jnp.bfloat16)
    return pl.pallas_call(
        join_qkv_kernel,
        in_specs=[pl.BlockSpec(memory_space=pltpu.SMEM)] + [pl.BlockSpec(memory_space=pltpu.VMEM)] * 2,
        out_shape=[out(DIM), out(SEND - HEAD_DIM), out(SEND - HEAD_DIM)],
        cost_estimate=cost(TINY, 4),
        name='join_qkv',
    )(dp_arr, own, got)


def unpack_qkv_kernel(p_ref, wq_ref, wk_ref, wv_ref):
    for g in range(PAIRS):
        for n in range(SP):
            m = g * SP + n
            total = p_ref[n, :, g * GRP:(g + 1) * GRP]
            wq_ref[:, m * PAIR:(m + 1) * PAIR] = total[:, :PAIR]
            wk_ref[:, m * HEAD_DIM:(m + 1) * HEAD_DIM] = total[:, PAIR:OWN]
            wv_ref[:, m * HEAD_DIM:(m + 1) * HEAD_DIM] = total[:, OWN:]


def unpack_qkv_call(parts):
    out = lambda cols: jax.ShapeDtypeStruct((HEAD_DIM, cols), jnp.float32)
    return pl.pallas_call(unpack_qkv_kernel, out_shape=[out(PAIRS * DIM), out(DIM), out(DIM)], cost_estimate=cost(TINY, 6), name='unpack_qkv')(parts)


def unpack_cols_kernel(core_ref, own_ref, got_ref, gate_ref, up_ref):
    core = core_ref[0]
    mine = own_ref[pl.ds(pl.multiple_of(core * HEAD_DIM, HEAD_DIM), HEAD_DIM), :]
    for w, ref in enumerate((gate_ref, up_ref)):
        for n in range(SP):
            cols = slice(w * HALF + n * OWN, w * HALF + (n + 1) * OWN)
            ref[:, pl.ds(pl.multiple_of((n * 2 + core) * OWN, HEAD_DIM), OWN)] = mine[:, cols]
            ref[:, pl.ds(pl.multiple_of((n * 2 + 1 - core) * OWN, HEAD_DIM), OWN)] = got_ref[:, cols]


def unpack_cols_call(core_arr, own, got):
    return pl.pallas_call(
        unpack_cols_kernel,
        in_specs=[pl.BlockSpec(memory_space=pltpu.SMEM)] + [pl.BlockSpec(memory_space=pltpu.VMEM)] * 2,
        out_shape=[jax.ShapeDtypeStruct((HEAD_DIM, 2 * HALF), jnp.float32)] * 2,
        cost_estimate=cost(TINY, 4),
        name='unpack_cols',
    )(core_arr, own, got)


def qkv_kernel(sp_ref, xa_ref, xb_ref, g_ref, w_ref, cos_ref, sin_ref, *rest):
    u_ref, q0_ref, k0_ref, v0_ref, q1_ref, k1_ref, v1_ref, x_scr = rest[-8:]
    i = pl.program_id(0)

    @pl.when(i < 2)
    def _():
        x_scr[...] = xa_ref[...]

    @pl.when(i >= 2)
    def _():
        x_scr[...] = xb_ref[...]

    u = (normalize(x_scr[...].astype(jnp.float32))[0] * g_ref[...].astype(jnp.float32)).astype(jnp.bfloat16)
    u_ref[...] = u
    cos, sin = cos_ref[...], sin_ref[...]

    def rope(t):
        return (t * cos + pltpu.roll(t, 64, 1) * sin).astype(jnp.bfloat16)

    for g, (q_ref, k_ref, v_ref) in enumerate(((q0_ref, k0_ref, v0_ref), (q1_ref, k1_ref, v1_ref))):
        y = dot_nn(u, w_ref[:, g * GRP:(g + 1) * GRP])
        q_ref[:, 0:HEAD_DIM] = rope(y[:, 0:HEAD_DIM])
        q_ref[:, HEAD_DIM:PAIR] = rope(y[:, HEAD_DIM:PAIR])
        k_ref[...] = rope(y[:, PAIR:OWN])
        v_ref[...] = y[:, OWN:GRP].astype(jnp.bfloat16)


def qkv_call(sp_arr, xa, xb, first, gain, w_own, cos, sin, prev):
    place = lambda width: pl.BlockSpec((BLK, width), lambda i, s: ((s[0] ^ (first + i // PAIRS)) * PAIRS + i % PAIRS, 0))
    local = lambda width: pl.BlockSpec((BLK, width), lambda i, s: (first * PAIRS + i, 0))
    out = lambda width: jax.ShapeDtypeStruct((SEQ, width), jnp.bfloat16)
    xa_spec = pl.BlockSpec((BLK, DIM), lambda i, s: (jnp.minimum(i, 1), 0))
    xb_spec = pl.BlockSpec((BLK, DIM), lambda i, s: (jnp.maximum(i - 2, 0), 0))
    widths = (DIM, PAIR, HEAD_DIM, HEAD_DIM, PAIR, HEAD_DIM, HEAD_DIM)
    return pl.pallas_call(
        qkv_kernel,
        grid_spec=pltpu.PrefetchScalarGridSpec(
            num_scalar_prefetch=1,
            grid=(4,),
            in_specs=[xa_spec, xb_spec, fixed((1, DIM)), fixed((DIM, DIM)), local(HEAD_DIM), local(HEAD_DIM)]
            + [pl.BlockSpec(memory_space=pl.ANY)] * len(prev),
            out_specs=[local(DIM)] + [place(w) for w in widths[1:]],
            scratch_shapes=[pltpu.VMEM((BLK, DIM), jnp.bfloat16)],
        ),
        out_shape=[out(w) for w in widths],
        input_output_aliases={7 + n: n for n in range(len(prev))},
        compiler_params=params(),
        cost_estimate=cost(2 * 2048 * DIM * DIM, 20),
        name='qkv',
    )(sp_arr, xa, xb, gain, w_own, cos, sin, *prev)


def fwd_kernel(q_ref, k_ref, v_ref, o_ref, lse_ref, acc_ref, q_scr):
    i = pl.program_id(0)
    for h in range(PAIRS):
        q_scr[h * BLK:(h + 1) * BLK, :] = q_ref[:, h * HEAD_DIM:(h + 1) * HEAD_DIM]

    chunks = [(h, n) for h in range(PAIRS) for n in range(BLK // QSUB)]

    def step(j, carry, masked):
        start = pl.multiple_of(j * BLK, BLK)
        k = k_ref[pl.ds(start, BLK), :]
        v = v_ref[pl.ds(start, BLK), :]

        def scores(c):
            h, n = chunks[c]
            s = dot_nt(k, q_scr[h * BLK + n * QSUB:h * BLK + (n + 1) * QSUB, :])
            if masked:
                kv_idx = lax.broadcasted_iota(jnp.int32, (BLK, QSUB), 0)
                q_idx = lax.broadcasted_iota(jnp.int32, (BLK, QSUB), 1) + n * QSUB
                s = jnp.where(q_idx >= kv_idx, s, NEG)
            return s

        out = []
        s_next = scores(0)
        for c in range(len(chunks)):
            s = s_next
            if c + 1 < len(chunks):
                s_next = scores(c + 1)
            m, l = carry[c]
            m_new = jnp.maximum(m, jnp.max(s, axis=0, keepdims=True))
            p = jnp.exp2(s * SCALE2 - m_new * SCALE2)
            alpha = jnp.exp2((m - m_new) * SCALE2)
            l_new = alpha * l + jnp.sum(p, axis=0, keepdims=True)
            acc_ref[c] = acc_ref[c] * alpha + dot_tn(v, p.astype(jnp.bfloat16))
            out.append((m_new, l_new))
        return tuple(out)

    acc_ref[...] = jnp.zeros_like(acc_ref)
    init = tuple((jnp.full((1, QSUB), NEG, jnp.float32), jnp.zeros((1, QSUB), jnp.float32)) for _ in chunks)
    carry = lax.fori_loop(0, i, lambda j, c: step(j, c, False), init)
    carry = step(i, carry, True)
    for c, (h, n) in enumerate(chunks):
        m, l = carry[c]
        rows = slice(n * QSUB, (n + 1) * QSUB)
        o_ref[0, rows, h * HEAD_DIM:(h + 1) * HEAD_DIM] = (acc_ref[c] / l).T.astype(jnp.bfloat16)
        lse_ref[h, :, rows] = jnp.broadcast_to(m * SCALE2 + jnp.log2(l), (8, QSUB))


def fwd_call(q, k, v):
    whole = fixed((SEQ, HEAD_DIM))
    per = TOK // BLK
    return pl.pallas_call(
        fwd_kernel,
        grid=(SEQ // BLK,),
        in_specs=[pl.BlockSpec((BLK, PAIR), lambda i: (i, 0)), whole, whole],
        out_specs=[pl.BlockSpec((1, BLK, PAIR), lambda i: (i // per, i % per, 0)), pl.BlockSpec((2, 8, BLK), lambda i: (0, 0, i))],
        out_shape=[jax.ShapeDtypeStruct((SEQ // TOK, TOK, PAIR), jnp.bfloat16), jax.ShapeDtypeStruct((2, 8, SEQ), jnp.float32)],
        scratch_shapes=[pltpu.VMEM((2 * BLK // QSUB, HEAD_DIM, QSUB), jnp.float32), pltpu.VMEM((2 * BLK, HEAD_DIM), jnp.bfloat16)],
        compiler_params=params(),
        cost_estimate=cost(24 * 10 ** 9, 8),
        name='attn_fwd',
    )(q, k, v)


def bwd_kernel(sp_ref, q_ref, k_ref, v_ref, o_ref, do_ref, lse_ref, cos_ref, sin_ref, out0_ref, out1_ref, out2_ref, out3_ref, dq_acc, dk_acc, dv_acc, delta):
    j = pl.program_id(0)
    n_blk = SEQ // BLK

    @pl.when(j == 0)
    def _():
        dq_acc[...] = jnp.zeros_like(dq_acc)

        def rows(i, _):
            start = pl.multiple_of(i * BLK, BLK)
            prod = o_ref[pl.ds(start, BLK), :].astype(jnp.float32) * do_ref[pl.ds(start, BLK), :].astype(jnp.float32)
            for h in range(PAIRS):
                tot = jnp.sum(prod[:, h * HEAD_DIM:(h + 1) * HEAD_DIM], axis=1, keepdims=True)
                delta[h, :, pl.ds(start, BLK)] = jnp.broadcast_to(tot, (BLK, HEAD_DIM)).T[0:8, :]
            return 0

        lax.fori_loop(0, n_blk, rows, 0)

    k = k_ref[...]
    v = v_ref[...]
    dk_acc[...] = jnp.zeros_like(dk_acc)
    dv_acc[...] = jnp.zeros_like(dv_acc)

    def step(i, masked):
        start = pl.multiple_of(i * BLK, BLK)
        rows = pl.ds(start, BLK)
        for h in range(PAIRS):
            cols = slice(h * HEAD_DIM, (h + 1) * HEAD_DIM)
            q = q_ref[rows, cols]
            do = do_ref[rows, cols]
            s = dot_nt(k, q)
            p = jnp.exp2(s * SCALE2 - lse_ref[h, 0:1, rows])
            if masked:
                kv_idx = lax.broadcasted_iota(jnp.int32, (BLK, BLK), 0)
                q_idx = lax.broadcasted_iota(jnp.int32, (BLK, BLK), 1)
                p = jnp.where(q_idx >= kv_idx, p, 0.0)
            dp = dot_nt(v, do)
            dv_acc[...] += dot_nn(p.astype(jnp.bfloat16), do)
            ds = (p * (dp - delta[h, 0:1, rows]) * ATTN_SCALE).astype(jnp.bfloat16)
            dk_acc[...] += dot_nn(ds, q)
            dq_acc[rows, cols] += dot_tn(ds, k)

    step(j, True)

    def body(i, _):
        step(i, False)
        return 0

    lax.fori_loop(j + 1, n_blk, body, 0)

    cos, sin = cos_ref[...], sin_ref[...]

    def rope_back(t):
        t = t.astype(jnp.bfloat16).astype(jnp.float32)
        return (t * cos - pltpu.roll(t, 64, 1) * sin).astype(jnp.bfloat16)

    mine = pl.ds(pl.multiple_of(j * BLK, BLK), BLK)
    result = jnp.concatenate(
        [rope_back(dq_acc[mine, h * HEAD_DIM:(h + 1) * HEAD_DIM]) for h in range(PAIRS)] + [rope_back(dk_acc[...]), dv_acc[...].astype(jnp.bfloat16)], axis=1)
    for n, ref in enumerate((out0_ref, out1_ref, out2_ref, out3_ref)):
        @pl.when((j * BLK // TOK) ^ sp_ref[0] == n)
        def _(ref=ref):
            ref[...] = result


def bwd_call(sp_arr, q, k, v, o, do, lse, cos, sin):
    whole = lambda width: fixed((SEQ, width))
    block = pl.BlockSpec((BLK, HEAD_DIM), lambda j, s: (j, 0))
    per = TOK // BLK
    table = pl.BlockSpec((BLK, HEAD_DIM), lambda j, s: (((j // per) ^ s[0]) * per + j % per, 0))
    piece = lambda n: pl.BlockSpec((BLK, GRP), lambda j, s: (jnp.clip(j - per * (s[0] ^ n), 0, per - 1), 0))
    return pl.pallas_call(
        bwd_kernel,
        grid_spec=pltpu.PrefetchScalarGridSpec(
            num_scalar_prefetch=1,
            grid=(SEQ // BLK,),
            in_specs=[whole(PAIR), block, block, whole(PAIR), whole(PAIR), fixed((2, 8, SEQ)), table, table],
            out_specs=[piece(n) for n in range(SP)],
            scratch_shapes=[
                pltpu.VMEM((SEQ, PAIR), jnp.float32),
                pltpu.VMEM((BLK, HEAD_DIM), jnp.float32),
                pltpu.VMEM((BLK, HEAD_DIM), jnp.float32),
                pltpu.VMEM((2, 8, SEQ), jnp.float32),
            ],
        ),
        out_shape=[jax.ShapeDtypeStruct((TOK, GRP), jnp.bfloat16)] * 4,
        compiler_params=params(),
        cost_estimate=cost(60 * 10 ** 9, 16),
        name='attn_bwd',
    )(sp_arr, q, k, v, o, do, lse, cos, sin)


def oproj_kernel(a0_ref, a1_ref, w_ref, x_ref, g_ref, h_ref, u_ref):
    total = x_ref[...].astype(jnp.float32)
    for g, a_ref in enumerate((a0_ref, a1_ref)):
        a = jnp.concatenate([a_ref[s] for s in range(SP)], axis=1)
        total += dot_nn(a, w_ref[g * DIM:(g + 1) * DIM, :])
    h = total.astype(jnp.bfloat16)
    h_ref[...] = h
    u_ref[...] = (normalize(h.astype(jnp.float32))[0] * g_ref[...].astype(jnp.float32)).astype(jnp.bfloat16)


def oproj_call(a0, a1, wo, x, gain):
    blk = PAIR
    row = row_block(DIM)
    part = pl.BlockSpec((4, blk, PAIR), lambda i: (0, i, 0))
    return pl.pallas_call(
        oproj_kernel,
        grid=(TOK // blk,),
        in_specs=[part, part, fixed((2048, DIM)), row, fixed((1, DIM))],
        out_specs=[row, row],
        out_shape=[jax.ShapeDtypeStruct((TOK, DIM), jnp.bfloat16)] * 2,
        compiler_params=params(),
        cost_estimate=cost(2 * TOK * DIM * 2048, 14),
        name='oproj',
    )(a0, a1, wo, x, gain)


def mlp_kernel(chip_ref, u_ref, dy_ref, *refs):
    z_ref, da_ref, dc_ref, y_ref, d_ref, w1_ref, w3_ref, w2_ref = refs[3 * SP:]

    @pl.when(pl.program_id(0) == 0)
    def _():
        for w, ref in enumerate((w1_ref, w3_ref, w2_ref)):
            for n in range(SP):
                piece = refs[w * SP + n]
                rows = piece.shape[0]
                ref[pl.ds(pl.multiple_of((chip_ref[0] ^ n) * rows, HEAD_DIM), rows), :] = piece[...]

    u, dy = u_ref[...], dy_ref[...]
    for n in range(HALF // GRP):
        cols = slice(n * GRP, (n + 1) * GRP)
        gate = dot_nn(u, w1_ref[:, cols])
        up = dot_nn(u, w3_ref[:, cols])
        e = dot_nt(dy, w2_ref[cols, :])
        sig = 1.0 / (1.0 + jnp.exp(-gate))
        silu = gate * sig
        z_ref[:, cols] = (silu * up).astype(jnp.bfloat16)
        da_ref[:, cols] = (e * up * sig * (1.0 + gate * (1.0 - sig))).astype(jnp.bfloat16)
        dc_ref[:, cols] = (e * silu).astype(jnp.bfloat16)
    d_ref[...] = dot_nt(da_ref[...], w1_ref[...]) + dot_nt(dc_ref[...], w3_ref[...])
    y_ref[...] = dot_nn(z_ref[...], w2_ref[...])


def mlp_call(chip_arr, u, dy, w1, w3, w2):
    row = row_block
    pieces = [*w1, *w3, *w2]
    bf16, f32 = jnp.bfloat16, jnp.float32
    return pl.pallas_call(
        mlp_kernel,
        grid_spec=pltpu.PrefetchScalarGridSpec(
            num_scalar_prefetch=1,
            grid=(TOK // PAIR,),
            in_specs=[row(DIM), row(DIM)] + [fixed(t.shape) for t in pieces],
            out_specs=[row(HALF), row(HALF), row(HALF), row(DIM), row(DIM)],
            scratch_shapes=[pltpu.VMEM((DIM, HALF), bf16), pltpu.VMEM((DIM, HALF), bf16), pltpu.VMEM((HALF, DIM), bf16)],
        ),
        out_shape=[jax.ShapeDtypeStruct((TOK, HALF), bf16)] * 3 + [jax.ShapeDtypeStruct((TOK, DIM), f32)] * PAIRS,
        compiler_params=params(),
        cost_estimate=cost(12 * TOK * DIM * HALF, 30),
        name='mlp',
    )(chip_arr, u, dy, *pieces)


def dw_kernel(la_ref, lb_ref, *refs):
    rights, out_ref = refs[:-1], refs[-1]
    for n in range(len(rights) // 2):
        ra_ref, rb_ref = rights[2 * n], rights[2 * n + 1]
        cols = ra_ref.shape[1]
        out_ref[:, n * cols:(n + 1) * cols] = dot_tn(la_ref[...], ra_ref[...]) + dot_tn(lb_ref[...], rb_ref[...])


def dw_call(la, lb, *rights):
    rows, cols = la.shape[1] // 4, rights[0].shape[1]
    total = cols * len(rights) // 2
    left = pl.BlockSpec((TOK, rows), lambda b: (0, b))
    right = fixed((TOK, cols))
    return pl.pallas_call(
        dw_kernel,
        grid=(4,),
        in_specs=[left, left] + [right] * len(rights),
        out_specs=pl.BlockSpec((rows, total), lambda b: (b, 0)),
        out_shape=jax.ShapeDtypeStruct((4 * rows, total), jnp.float32),
        compiler_params=params(),
        cost_estimate=cost(4 * TOK * rows * 4 * total, 20),
        name='dw',
    )(la, lb, *rights)


def dw_split_kernel(idx_ref, la_ref, lb_ref, ra_ref, rb_ref, send_ref, keep_ref):
    b = pl.program_id(0)
    total = dot_tn(la_ref[...], ra_ref[...]) + dot_tn(lb_ref[...], rb_ref[...])
    for n, ref in enumerate((send_ref, keep_ref)):
        @pl.when(b // PAIRS == n)
        def _(ref=ref):
            ref[0] = total


def dw_split_call(idx, la, lb, ra, rb):
    rows, cols = la.shape[1] // SP, ra.shape[1]
    left = pl.BlockSpec((TOK, rows), lambda b, s: (0, s[b]))
    right = fixed((TOK, cols))
    out = lambda n: pl.BlockSpec((1, rows, cols), lambda b, s: (jnp.clip(b - PAIRS * n, 0, 1), 0, 0))
    return pl.pallas_call(
        dw_split_kernel,
        grid_spec=pltpu.PrefetchScalarGridSpec(
            num_scalar_prefetch=1, grid=(SP,), in_specs=[left, left, right, right], out_specs=[out(0), out(1)]),
        out_shape=[jax.ShapeDtypeStruct((PAIRS, rows, cols), jnp.float32)] * PAIRS,
        compiler_params=params(),
        cost_estimate=cost(SP * TOK * rows * SP * cols, 20),
        name='dw_split',
    )(idx, la, lb, ra, rb)


def dw_qkv_kernel(u_ref, *refs):
    out_ref = refs[-1]
    total = dot_tn(u_ref[0:TOK, :], refs[0][...])
    for n in range(1, 4):
        total += dot_tn(u_ref[n * TOK:(n + 1) * TOK, :], refs[n][...])
    out_ref[...] = total


def dw_qkv_call(u, pieces):
    return pl.pallas_call(
        dw_qkv_kernel,
        grid=(4,),
        in_specs=[pl.BlockSpec((SEQ, PAIR), lambda b: (0, b))] + [fixed((TOK, GRP))] * 4,
        out_specs=pl.BlockSpec((PAIR, GRP), lambda b: (b, 0)),
        out_shape=jax.ShapeDtypeStruct((DIM, GRP), jnp.float32),
        compiler_params=params(),
        cost_estimate=cost(2 * SEQ * DIM * GRP, 14),
        name='dw_qkv',
    )(u, *pieces)


def dout_kernel(sp_ref, h0_ref, h1_ref, h2_ref, h3_ref, o0_ref, o1_ref, wa_ref, wb_ref, d0_ref, d1_ref, dwo_ref, scr):
    i = pl.program_id(0)
    for n, ref in enumerate((h0_ref, h1_ref, h2_ref, h3_ref)):
        @pl.when(i // 2 == n)
        def _(ref=ref):
            scr[...] = ref[...]
    dh = scr[...]
    d0_ref[...] = dot_nt(dh, wa_ref[...]).astype(jnp.bfloat16)
    d1_ref[...] = dot_nt(dh, wb_ref[...]).astype(jnp.bfloat16)

    @pl.when(i == 0)
    def _():
        dwo_ref[...] = jnp.zeros_like(dwo_ref)

    dwo_ref[0] += dot_tn(o0_ref[0], dh)
    dwo_ref[1] += dot_tn(o1_ref[0], dh)


def dout_call(sp_arr, dhs, o0, o1, wo):
    src = lambda n: pl.BlockSpec((BLK, DIM), lambda i, s: (jnp.clip(i - 2 * n, 0, 1), 0))
    o_spec = pl.BlockSpec((1, BLK, PAIR), lambda i, s: (s[0] ^ (i // 2), i % 2, 0))
    d_spec = pl.BlockSpec((BLK, PAIR), lambda i, s: ((s[0] ^ (i // 2)) * 2 + i % 2, 0))
    out = jax.ShapeDtypeStruct((SEQ, PAIR), jnp.bfloat16)
    return pl.pallas_call(
        dout_kernel,
        grid_spec=pltpu.PrefetchScalarGridSpec(
            num_scalar_prefetch=1,
            grid=(SEQ // BLK,),
            in_specs=[src(0), src(1), src(2), src(3), o_spec, o_spec,
                      pl.BlockSpec((PAIR, DIM), lambda i, s: (s[0], 0)), pl.BlockSpec((PAIR, DIM), lambda i, s: (4 + s[0], 0))],
            out_specs=[d_spec, d_spec, fixed((2, PAIR, DIM))],
            scratch_shapes=[pltpu.VMEM((BLK, DIM), jnp.bfloat16)],
        ),
        out_shape=[out, out, jax.ShapeDtypeStruct((2, PAIR, DIM), jnp.float32)],
        compiler_params=params(),
        cost_estimate=cost(4 * SEQ * DIM * GRP, 20),
        name='dout',
    )(sp_arr, *dhs, o0, o1, wo, wo)


def du_sum(sp_ref, pieces, w_ref):
    total = 0.0
    for n, piece in enumerate(pieces):
        cols = pl.ds(pl.multiple_of((sp_ref[0] ^ n) * GRP, GRP), GRP)
        total += dot_nt(piece[...], w_ref[:, cols])
    return total


def du_kernel(sp_ref, *refs):
    refs[-1][...] = du_sum(sp_ref, refs[:SP], refs[SP])


def dx_kernel(sp_ref, *refs):
    w_ref, du_ref, x_ref, dr_ref, g_ref, dx_ref, dg_ref = refs[SP:]
    d_u = du_ref[...] + du_sum(sp_ref, refs[:SP], w_ref)
    normed, inv_rms = normalize(x_ref[...].astype(jnp.float32))
    grad_in = normalize_grad(d_u * g_ref[...].astype(jnp.float32), normed, inv_rms)
    dx_ref[...] = (dr_ref[...] + grad_in).astype(jnp.bfloat16)
    accumulate(dg_ref, col_sum(d_u * normed))


def dx_call(sp_arr, group, pieces, w_all, *rest):
    row = row_block
    one = fixed((1, DIM))
    du_shape = jax.ShapeDtypeStruct((TOK, DIM), jnp.float32)
    last = len(rest) > 0
    return pl.pallas_call(
        dx_kernel if last else du_kernel,
        grid_spec=pltpu.PrefetchScalarGridSpec(
            num_scalar_prefetch=1,
            grid=(TOK // PAIR,),
            in_specs=[row(GRP)] * SP + [pl.BlockSpec((DIM, SP * GRP), lambda i, s: (0, group))] + ([row(DIM)] * 3 + [one] if last else []),
            out_specs=[row(DIM), one] if last else row(DIM),
        ),
        out_shape=[jax.ShapeDtypeStruct((TOK, DIM), jnp.bfloat16), jax.ShapeDtypeStruct((1, DIM), jnp.float32)] if last else du_shape,
        compiler_params=params(),
        cost_estimate=cost(SP * TOK * DIM * DIM, 16),
        name='dx' if last else 'du',
    )(sp_arr, *pieces, w_all, *rest)


def gather_full(shard):
    return lax.all_gather(shard, ALL_AXES, axis=0, tiled=True)


def swap_seq(parts):
    return lax.all_to_all(parts, 'sp', 0, 0, tiled=True)


def swap_all(parts):
    return lax.all_to_all(parts, ALL_AXES, 0, 0, tiled=True)


def from_sp(value, bits):
    return lax.ppermute(value, 'sp', [(s, s ^ bits) for s in range(SP)])


def from_dp(value):
    return lax.ppermute(value, 'dp', [(0, 1), (1, 0)])


def gather_chip_then_core(value):
    far = from_sp(value, 2)
    near = from_sp(value, 1)
    return value, near, far, from_sp(far, 1)


def gather_chips(value, by_x):
    across = from_dp(value)
    along = from_sp(value, 2)
    if by_x:
        return value, along, across, from_dp(along)
    return value, along, across, from_sp(across, 2)


def reduce_chips(part):
    return lax.psum_scatter(part, ALL_AXES, scatter_dimension=0, tiled=True, axis_index_groups=CORE_GROUPS)


def layer_step(hidden, positions, grad_out, gain_attn, gain_mlp, w_query, w_key, w_value, w_out, w_gate, w_up, w_down):
    tokens = hidden[0]
    d_layer = grad_out[0]
    dp = lax.axis_index('dp')
    sp = lax.axis_index('sp')
    core = sp % 2
    chip = dp * PAIRS + sp // PAIRS
    f32, bf16 = jnp.float32, jnp.bfloat16
    sp_arr, dp_arr, core_arr = (t.astype(jnp.int32)[None] for t in (sp, dp, core))
    chip_arr = chip.astype(jnp.int32)[None]

    xs = gather_chip_then_core(tokens)
    w_cols, w_send, a1, b1, a3, b3 = pack_call(core_arr, w_query, w_key, w_value, w_gate, w_up, gain_attn[None], gain_mlp[None])
    w_mine = swap_seq(w_send)
    w_got = from_dp(w_mine)
    w_own, gain1, gain2 = join_qkv_call(dp_arr, w_mine, w_got)
    gain1, gain2 = gain1[0:1], gain2[0:1]
    pos = gather_chip_then_core(positions[0].reshape(8, HEAD_DIM))
    pos_all = jnp.concatenate(pos).reshape(SEQ)
    w1_rows, w3_rows = join_call(core_arr, (a1, from_sp(b1, 1)), (a3, from_sp(b3, 1)))
    wo_full = gather_full(w_out)
    w1, w3, w2 = gather_chips(w1_rows, True), gather_chips(w3_rows, True), gather_chips(w_down, False)
    w_all = gather_full(w_cols)
    dy_pair = from_sp(d_layer, 1)

    lane = jnp.arange(HEAD_DIM)
    half = HEAD_DIM // 2
    inv_freq = ROPE_BASE ** (-((lane % half).astype(f32) * (2.0 / HEAD_DIM)))
    angles = pos_all.astype(f32)[:, None] * inv_freq
    cos = jnp.cos(angles)
    sin = jnp.sin(angles) * jnp.where(lane < half, -1.0, 1.0)

    near = qkv_call(sp_arr, xs[0], xs[1], 0, gain1, w_own, cos, sin, ())
    u_all, q0, k0, v0, q1, k1, v1 = qkv_call(sp_arr, xs[2], xs[3], 2, gain1, w_own, cos, sin, near)
    o0, lse0 = fwd_call(q0, k0, v0)
    got0 = swap_seq(o0)
    o1, lse1 = fwd_call(q1, k1, v1)
    got1 = swap_seq(o1)
    residual, u_mlp = oproj_call(got0, got1, wo_full, tokens, gain2)

    u_pair = from_sp(u_mlp, 1)
    z_a, da_a, dc_a, y_a, d_a = mlp_call(chip_arr, u_mlp, d_layer, w1, w3, w2)
    z_b, da_b, dc_b, y_b, d_b = mlp_call(chip_arr, u_pair, dy_pair, w1, w3, w2)
    d_got = from_sp(d_b, 1)
    d_umlp = d_a + d_got
    h32 = residual.astype(f32)
    layer_out = (h32 + (y_a + from_sp(y_b, 1))).astype(bf16)
    normed2, inv_rms2 = normalize(h32)
    d_gain2 = col_sum(d_umlp * normed2)
    d_resid = d_layer.astype(f32) + normalize_grad(d_umlp * gain2.astype(f32), normed2, inv_rms2)
    dhs = gather_chip_then_core(d_resid.astype(bf16))
    order = jnp.stack([chip ^ 3, chip ^ 2, chip ^ 1, chip]).astype(jnp.int32)
    down_send, down_keep = dw_split_call(order, z_a, z_b, d_layer, dy_pair)
    down_got = from_dp(down_send)

    part = reduce_chips(dw_call(u_mlp, u_pair, da_a, da_b, dc_a, dc_b))

    do0, do1, dwo = dout_call(sp_arr, dhs, o0, o1, wo_full)
    down_far, down_near = down_keep[0] + down_got[0], down_keep[1] + down_got[1]
    down_last = from_sp(down_far, 2)
    o_seq = (o0.reshape(SEQ, PAIR), o1.reshape(SEQ, PAIR))
    d0 = bwd_call(sp_arr, q0, k0, v0, o_seq[0], do0, lse0, cos, sin)
    back0 = [d0[0]] + [from_sp(d0[n], n) for n in (1, 2, 3)]
    part0 = dw_qkv_call(u_all, d0).reshape(PAIRS, GRP, GRP)
    dw_got0 = from_dp(pick(part0, 1 - dp))
    d1 = bwd_call(sp_arr, q1, k1, v1, o_seq[1], do1, lse1, cos, sin)
    back1 = [d1[0]] + [from_sp(d1[n], n) for n in (1, 2, 3)]
    part1 = dw_qkv_call(u_all, d1).reshape(PAIRS, GRP, GRP)
    dw_got1 = from_dp(pick(part1, 1 - dp))
    dw_rows = jnp.concatenate([pick(part0, dp) + dw_got0, pick(part1, dp) + dw_got1], axis=1)
    dw_cols = swap_seq(dw_rows.reshape(SP, HEAD_DIM, DIM))

    grad_w_out = pick(dwo, dp) + from_dp(pick(dwo, 1 - dp))
    part, _ = lax.optimization_barrier((part, part1))
    send = lax.dynamic_slice(part, ((1 - core) * HEAD_DIM, 0), (HEAD_DIM, 2 * HALF))
    cols_got = from_sp(send, 1)
    grad_w_gate, grad_w_up = unpack_cols_call(core_arr, part, cols_got)
    grad_w_down = down_near + down_last
    du0 = dx_call(sp_arr, 0, back0, w_all)
    grad_hidden, d_gain1 = dx_call(sp_arr, 1, back1, w_all, du0, tokens, d_resid, gain1)
    grad_w_query, grad_w_key, grad_w_value = unpack_qkv_call(dw_cols)
    gain_parts = jnp.stack([d_gain1.reshape(8, HEAD_DIM), d_gain2.reshape(8, HEAD_DIM)], axis=1)
    gain_parts, _ = lax.optimization_barrier((gain_parts, dw_cols))
    gain_sums = jnp.sum(swap_all(gain_parts), axis=0)
    return (layer_out[None], grad_hidden[None], gain_sums[0], gain_sums[1], grad_w_query, grad_w_key, grad_w_value,
            grad_w_out, grad_w_gate, grad_w_up, grad_w_down)


def solution(mesh):
    act_spec = P('dp', 'sp', None)
    pos_spec = P('dp', 'sp')
    vec_spec = P(ALL_AXES)
    mat_spec = P(ALL_AXES, None)
    in_specs = (act_spec, pos_spec, act_spec, vec_spec, vec_spec) + (mat_spec,) * 7
    out_specs = (act_spec, act_spec, vec_spec, vec_spec) + (mat_spec,) * 7

    return jax.shard_map(layer_step, mesh=mesh, in_specs=in_specs, out_specs=out_specs, check_vma=False)
```
